32 devices in a mesh: model: 4 (over z), data: 8 (over y, x, core).
Axes of the slice: x: 2, y: 2, z: 4, core: 2. Of those that a mesh axis runs over, the one named last changes fastest.
Arguments:
- x_tokens: bfloat16 [32768, 1024], P('data')
- dy_tokens: bfloat16 [32768, 1024], P('data')
- w_col: bfloat16 [2, 1024, 1024], P(None, None, 'model')
- w_row: bfloat16 [2, 1024, 1024], P(None, 'model')
- a_old_col: float32 [2, 1024, 1024], replicated
- s_old_col: float32 [2, 1024, 256], P(None, 'model')
- a_old_row: float32 [2, 1024, 256], P(None, 'model')
- s_old_row: float32 [2, 1024, 1024], replicated
- a_inv_col: float32 [2, 1024, 1024], replicated
- s_inv_col: float32 [2, 1024, 256], P(None, 'model')
- a_inv_row: float32 [2, 1024, 256], P(None, 'model')
- s_inv_row: float32 [2, 1024, 1024], replicated
Outputs:
- output 1: float32 [2, 1024, 1024], P(None, None, 'model')
- output 2: float32 [2, 1024, 1024], P(None, 'model')
- output 3: float32 [2, 1024, 1024], replicated
- output 4: float32 [2, 1024, 256], P(None, 'model')
- output 5: float32 [2, 1024, 256], P(None, 'model')
- output 6: float32 [2, 1024, 1024], replicated
All inputs are finite; a program needn't handle non-finite values.
Results may differ from the reference program's by a relative error of at most 0.00553995.
Values are sent between devices in bfloat16 or wider.
A program may use at most 1 GiB of HBM per device.

```python
import math
import jax
import jax.numpy as jnp
from jax import lax

HIDDEN = 1024
TOKENS_DEV = 4096
DATA_WAYS = 8
MODEL_WAYS = 4
BATCH_ROWS = TOKENS_DEV * DATA_WAYS
BLOCK_DIM = HIDDEN // MODEL_WAYS
FACTOR_DECAY = 0.8
GELU_SCALE = math.sqrt(2.0 / math.pi)
GELU_CUBIC = 0.044715
EXACT = lax.Precision.HIGHEST


def gelu_value(pre_act):
    tanh_arg = GELU_SCALE * (pre_act + GELU_CUBIC * pre_act * pre_act * pre_act)
    return 0.5 * pre_act * (1.0 + jnp.tanh(tanh_arg))


def gelu_slope(pre_act):
    tanh_arg = GELU_SCALE * (pre_act + GELU_CUBIC * pre_act * pre_act * pre_act)
    tanh_val = jnp.tanh(tanh_arg)
    return 0.5 * (1.0 + tanh_val) + 0.5 * pre_act * (1.0 - tanh_val * tanh_val) * GELU_SCALE * (1.0 + 3.0 * GELU_CUBIC * pre_act * pre_act)


def activate(pre_act):
    return gelu_value(pre_act.astype(jnp.float32)).astype(jnp.bfloat16)


def back_gate(grad_act, pre_act):
    return (grad_act.astype(jnp.float32) * gelu_slope(pre_act.astype(jnp.float32))).astype(jnp.bfloat16)


def sym_draw(rand_key, lead_count, mat_dim, spread):
    diag_key, noise_key = jax.random.split(rand_key)
    diag_vals = jax.random.uniform(diag_key, (lead_count, mat_dim), jnp.float32, 0.5, 1.5)
    sym_noise = jax.random.normal(noise_key, (lead_count, mat_dim, mat_dim), jnp.float32)
    sym_noise = (sym_noise + jnp.swapaxes(sym_noise, 1, 2)) * (spread / math.sqrt(2.0 * mat_dim))
    return sym_noise + diag_vals[:, :, None] * jnp.eye(mat_dim, dtype=jnp.float32)


def block_draw(rand_key, spread):
    return sym_draw(rand_key, 2 * MODEL_WAYS, BLOCK_DIM, spread).reshape(2, HIDDEN, BLOCK_DIM)


def token_draw(rand_key):
    mean_key, scale_key, base_key = jax.random.split(rand_key, 3)
    shard_mean = jax.random.normal(mean_key, (DATA_WAYS, 1, HIDDEN), jnp.float32) * (0.5 * HIDDEN ** -0.25)
    shard_scale = jnp.exp2(jax.random.uniform(scale_key, (DATA_WAYS, 1, 1), jnp.float32, -1.0, 1.0))
    base_vals = jax.random.normal(base_key, (DATA_WAYS, TOKENS_DEV, HIDDEN), jnp.float32)
    return (base_vals * shard_scale + shard_mean).reshape(BATCH_ROWS, HIDDEN).astype(jnp.bfloat16)


def setup_inputs(seed: int = 0) -> dict:
    key_list = jax.random.split(jax.random.key(seed), 12)
    weight_scale = HIDDEN ** -0.5
    return {
        'x_tokens': token_draw(key_list[0]),
        'dy_tokens': token_draw(key_list[1]),
        'w_col': (jax.random.normal(key_list[2], (2, HIDDEN, HIDDEN), jnp.float32) * weight_scale).astype(jnp.bfloat16),
        'w_row': (jax.random.normal(key_list[3], (2, HIDDEN, HIDDEN), jnp.float32) * weight_scale).astype(jnp.bfloat16),
        'a_old_col': sym_draw(key_list[4], 2, HIDDEN, 0.3),
        's_old_col': block_draw(key_list[5], 0.3),
        'a_old_row': block_draw(key_list[6], 0.3),
        's_old_row': sym_draw(key_list[7], 2, HIDDEN, 0.3),
        'a_inv_col': sym_draw(key_list[8], 2, HIDDEN, 0.2),
        's_inv_col': block_draw(key_list[9], 0.2),
        'a_inv_row': block_draw(key_list[10], 0.2),
        's_inv_row': sym_draw(key_list[11], 2, HIDDEN, 0.2),
    }


def gram_mat(left_mat, right_mat):
    return jnp.dot(left_mat.T, right_mat, preferred_element_type=jnp.float32) / BATCH_ROWS


def block_gram(left_mat, right_mat):
    left_blocks = jnp.swapaxes(left_mat.reshape(BATCH_ROWS, MODEL_WAYS, BLOCK_DIM), 0, 1)
    right_blocks = jnp.swapaxes(right_mat.reshape(BATCH_ROWS, MODEL_WAYS, BLOCK_DIM), 0, 1)
    blocks = lax.map(lambda block_pair: jnp.dot(block_pair[0].T, block_pair[1], preferred_element_type=jnp.float32), (left_blocks, right_blocks))
    return blocks.reshape(HIDDEN, BLOCK_DIM) / BATCH_ROWS


def precondition_col(a_inv, grad_mat, s_inv_blocks):
    left_done = jnp.dot(a_inv, grad_mat, precision=EXACT).reshape(HIDDEN, MODEL_WAYS, BLOCK_DIM)
    right_blocks = s_inv_blocks.reshape(MODEL_WAYS, BLOCK_DIM, BLOCK_DIM)
    return jnp.einsum('dmi,mij->dmj', left_done, right_blocks, precision=EXACT).reshape(HIDDEN, HIDDEN)


def precondition_row(a_inv_blocks, grad_mat, s_inv):
    left_blocks = a_inv_blocks.reshape(MODEL_WAYS, BLOCK_DIM, BLOCK_DIM)
    left_done = jnp.einsum('mij,mjk->mik', left_blocks, grad_mat.reshape(MODEL_WAYS, BLOCK_DIM, HIDDEN), precision=EXACT).reshape(HIDDEN, HIDDEN)
    return jnp.dot(left_done, s_inv, precision=EXACT)


def blend_factor(old_mats, first_new, second_new):
    return FACTOR_DECAY * old_mats + (1.0 - FACTOR_DECAY) * jnp.stack([first_new, second_new])


def reference(x_tokens, dy_tokens, w_col, w_row, a_old_col, s_old_col, a_old_row, s_old_row, a_inv_col, s_inv_col, a_inv_row, s_inv_row):
    z_one = jnp.dot(x_tokens, w_col[0], preferred_element_type=jnp.float32).astype(jnp.bfloat16)
    h_one = activate(z_one)
    z_two = jnp.dot(h_one, w_row[0], preferred_element_type=jnp.float32).astype(jnp.bfloat16)
    h_two = activate(z_two)
    z_three = jnp.dot(h_two, w_col[1], preferred_element_type=jnp.float32).astype(jnp.bfloat16)
    h_three = activate(z_three)
    g_three = back_gate(jnp.dot(dy_tokens, w_row[1].T, preferred_element_type=jnp.float32).astype(jnp.bfloat16), z_three)
    g_two = back_gate(jnp.dot(g_three, w_col[1].T, preferred_element_type=jnp.float32).astype(jnp.bfloat16), z_two)
    g_one = back_gate(jnp.dot(g_two, w_row[0].T, preferred_element_type=jnp.float32).astype(jnp.bfloat16), z_one)
    u_col = jnp.stack([
        precondition_col(a_inv_col[0], gram_mat(x_tokens, g_one), s_inv_col[0]),
        precondition_col(a_inv_col[1], gram_mat(h_two, g_three), s_inv_col[1]),
    ])
    u_row = jnp.stack([
        precondition_row(a_inv_row[0], gram_mat(h_one, g_two), s_inv_row[0]),
        precondition_row(a_inv_row[1], gram_mat(h_three, dy_tokens), s_inv_row[1]),
    ])
    a_new_col = blend_factor(a_old_col, gram_mat(x_tokens, x_tokens), gram_mat(h_two, h_two))
    s_new_col = blend_factor(s_old_col, block_gram(g_one, g_one), block_gram(g_three, g_three))
    a_new_row = blend_factor(a_old_row, block_gram(h_one, h_one), block_gram(h_three, h_three))
    s_new_row = blend_factor(s_old_row, gram_mat(g_two, g_two), gram_mat(dy_tokens, dy_tokens))
    return (u_col, u_row, a_new_col, s_new_col, a_new_row, s_new_row)
```

```python
import math
import jax
import jax.numpy as jnp
from jax import lax
from jax.sharding import PartitionSpec as P
from jax.experimental import pallas as pl
from jax.experimental.pallas import tpu as pltpu

FACTOR_DECAY = 0.8
GELU_SCALE = math.sqrt(2.0 / math.pi)
GELU_CUBIC = 0.044715
EXACT = lax.Precision.HIGHEST
TN_DIMS = (((0,), (0,)), ((), ()))
NT_DIMS = (((1,), (1,)), ((), ()))
BOTH = ('model', 'data')


def gelu_value(pre_act):
    tanh_arg = GELU_SCALE * (pre_act + GELU_CUBIC * pre_act * pre_act * pre_act)
    return 0.5 * pre_act * (1.0 + jnp.tanh(tanh_arg))


def gelu_slope(pre_act):
    tanh_arg = GELU_SCALE * (pre_act + GELU_CUBIC * pre_act * pre_act * pre_act)
    tanh_val = jnp.tanh(tanh_arg)
    return 0.5 * (1.0 + tanh_val) + 0.5 * pre_act * (1.0 - tanh_val * tanh_val) * GELU_SCALE * (1.0 + 3.0 * GELU_CUBIC * pre_act * pre_act)


def activate(pre_act):
    return gelu_value(pre_act.astype(jnp.float32)).astype(jnp.bfloat16)


def back_gate(grad_act, pre_act):
    return (grad_act.astype(jnp.float32) * gelu_slope(pre_act.astype(jnp.float32))).astype(jnp.bfloat16)


def matmul(left_mat, right_mat):
    return jnp.dot(left_mat, right_mat, preferred_element_type=jnp.float32)


def matmul_tn(left_mat, right_mat):
    return lax.dot_general(left_mat, right_mat, TN_DIMS, preferred_element_type=jnp.float32)


def matmul_nt(left_mat, right_mat):
    return lax.dot_general(left_mat, right_mat, NT_DIMS, preferred_element_type=jnp.float32)


def exact_dot(left_mat, right_mat):
    return jnp.dot(left_mat, right_mat, precision=EXACT, preferred_element_type=jnp.float32)


D_ROWS = 512
FULL_BASE = 512
BLOCK_BASE = 768
SHARE_ROWS = 896


def gram_kernel(x_ref, g1_ref, g2_ref, h1_ref, h2_ref, g3_ref, dy_ref, h3_ref, out_ref,
                act, stage, bstage, in_sem, out_sem, b_sem):
    sources = [dy_ref, h3_ref, h2_ref, g3_ref, g2_ref, h1_ref, x_ref, g1_ref]
    slots = [3, 7, 2, 6, 1, 5, 0, 4]
    loads = [pltpu.make_async_copy(src, act.at[slot], in_sem.at[slot]) for src, slot in zip(sources, slots)]
    for load in loads:
        load.start()
    started = [0]
    pend = {}

    def out_copy(slot, dst):
        return pltpu.make_async_copy(stage.at[slot], dst, out_sem.at[slot])

    for layer in (3, 2, 1, 0):
        pltpu.make_async_copy(x_ref, act.at[layer], in_sem.at[layer]).wait()
        pltpu.make_async_copy(x_ref, act.at[4 + layer], in_sem.at[4 + layer]).wait()

        def d_body(m, carry, layer=layer):
            slot = lax.rem(m, 2)
            cols = pl.ds(pl.multiple_of(m * 256, 256), 256)
            right = act[4 + layer, :, cols]
            dst = out_ref.at[pl.ds(m * 8 + 2 * layer, 2), pl.ds(0, D_ROWS)]

            if layer == 3:
                @pl.when(m >= 2)
                def _():
                    out_copy(slot, dst).wait()
                    pltpu.make_async_copy(bstage.at[slot], out_ref.at[pl.ds(0, 8), pl.ds(BLOCK_BASE, 32)], b_sem.at[slot]).wait()
            else:
                out_copy(slot, dst).wait()
                pltpu.make_async_copy(bstage.at[slot], out_ref.at[pl.ds(0, 8), pl.ds(BLOCK_BASE, 32)], b_sem.at[slot]).wait()
            prod = lax.dot_general(act[layer], right, TN_DIMS, preferred_element_type=jnp.float32)
            stage[slot] = prod.reshape(2, D_ROWS, 256)
            out_copy(slot, dst).start()
            blk = lax.dot_general(right, right, TN_DIMS, preferred_element_type=jnp.float32)
            bstage[slot] = blk.reshape(8, 32, 256)
            pltpu.make_async_copy(bstage.at[slot], out_ref.at[pl.ds(m * 8, 8), pl.ds(BLOCK_BASE + 32 * layer, 32)], b_sem.at[slot]).start()
            return carry

        lax.fori_loop(0, 4, d_body, 0)

        if layer in (2, 1):
            which = 0 if layer == 2 else 1

            def f_body(n, carry, layer=layer, which=which):
                slot = lax.rem(n, 2)
                cols = pl.ds(pl.multiple_of(n * 256, 256), 256)
                dst = out_ref.at[:, pl.ds(FULL_BASE + which * 128 + 32 * n, 32)]
                pltpu.make_async_copy(stage.at[slot], out_ref.at[pl.ds(0, 2), pl.ds(0, D_ROWS)], out_sem.at[slot]).wait()
                prod = lax.dot_general(act[layer], act[layer, :, cols], TN_DIMS, preferred_element_type=jnp.float32)
                stage[slot] = prod.reshape(2, D_ROWS, 256)
                pltpu.make_async_copy(stage.at[slot].reshape(32, 32, 256), dst, out_sem.at[slot]).start()
                return carry

            lax.fori_loop(0, 4, f_body, 0)
    for slot in range(2):
        pltpu.make_async_copy(stage.at[slot], out_ref.at[pl.ds(0, 2), pl.ds(0, D_ROWS)], out_sem.at[slot]).wait()
        pltpu.make_async_copy(bstage.at[slot], out_ref.at[pl.ds(0, 8), pl.ds(BLOCK_BASE, 32)], b_sem.at[slot]).wait()


def gram_call(x_loc, g_one, g_two, h_one, h_two, g_three, dy_loc, h_three):
    any_spec = pl.BlockSpec(memory_space=pl.ANY)
    return pl.pallas_call(
        gram_kernel,
        out_shape=jax.ShapeDtypeStruct((32, SHARE_ROWS, 256), jnp.float32),
        in_specs=[any_spec] * 8,
        out_specs=any_spec,
        scratch_shapes=[
            pltpu.VMEM((8, 1024, 1024), jnp.bfloat16),
            pltpu.VMEM((2, 2, D_ROWS, 256), jnp.float32),
            pltpu.VMEM((2, 8, 32, 256), jnp.float32),
            pltpu.SemaphoreType.DMA((8,)),
            pltpu.SemaphoreType.DMA((2,)),
            pltpu.SemaphoreType.DMA((2,)),
        ],
        compiler_params=pltpu.CompilerParams(vmem_limit_bytes=48 * 1024 * 1024),
        cost_estimate=pl.CostEstimate(flops=15_000_000_000, bytes_accessed=46_000_000, transcendentals=0),
        name='gram',
    )(x_loc, g_one, g_two, h_one, h_two, g_three, dy_loc, h_three)


def solution(mesh):
    data_ways = mesh.shape['data']
    model_ways = mesh.shape['model']
    n_dev = data_ways * model_ways

    def shard_body(x_tokens, dy_tokens, w_col, w_row, a_old_col, s_old_col, a_old_row, s_old_row, a_inv_col, s_inv_col, a_inv_row, s_inv_row):
        model_id = lax.axis_index('model')
        data_id = lax.axis_index('data')
        dev_id = model_id * data_ways + data_id
        inv_rows = 1.0 / (x_tokens.shape[0] * data_ways)
        col_part = lax.dynamic_slice(w_col, (0, 128 * data_id, 0), (2, 128, 256))
        row_part = lax.dynamic_slice(w_row, (0, 32 * data_id, 0), (2, 32, 1024))
        col_all = lax.all_gather(col_part, BOTH)
        row_all = lax.all_gather(row_part, BOTH)
        w_c = [jnp.swapaxes(col_all[:, layer].reshape(4, 1024, 256), 0, 1).reshape(1024, 1024) for layer in range(2)]
        w_r = [row_all[:, layer].reshape(1024, 1024) for layer in range(2)]
        x_cols = lax.dynamic_slice(x_tokens, (0, 256 * model_id), (x_tokens.shape[0], 256))
        dy_cols = lax.dynamic_slice(dy_tokens, (0, 256 * model_id), (x_tokens.shape[0], 256))
        ends = jnp.stack([matmul_tn(x_cols, x_tokens), matmul_tn(dy_cols, dy_tokens)]).reshape(2, 8, 32, 1024)
        ends = lax.psum_scatter(jnp.swapaxes(ends, 0, 1), 'data', scatter_dimension=0, tiled=False)
        rows_dev = x_tokens.shape[0] // model_ways
        x_loc = lax.dynamic_slice(x_tokens, (rows_dev * model_id, 0), (rows_dev, 1024))
        dy_loc = lax.dynamic_slice(dy_tokens, (rows_dev * model_id, 0), (rows_dev, 1024))
        z_one = matmul(x_loc, w_c[0]).astype(jnp.bfloat16)
        h_one = activate(z_one)
        z_two = matmul(h_one, w_r[0]).astype(jnp.bfloat16)
        h_two = activate(z_two)
        z_three = matmul(h_two, w_c[1]).astype(jnp.bfloat16)
        h_three = activate(z_three)
        g_three = back_gate(matmul_nt(dy_loc, w_r[1]).astype(jnp.bfloat16), z_three)
        g_two = back_gate(matmul_nt(g_three, w_c[1]).astype(jnp.bfloat16), z_two)
        g_one = back_gate(matmul_nt(g_two, w_r[0]).astype(jnp.bfloat16), z_one)
        parts = gram_call(x_loc, g_one, g_two, h_one, h_two, g_three, dy_loc, h_three)
        share = lax.psum_scatter(parts, BOTH, scatter_dimension=0, tiled=False)
        row_at = 32 * dev_id
        mids = jnp.swapaxes(share[FULL_BASE:BLOCK_BASE].reshape(2, 4, 32, 256), 1, 2).reshape(2, 32, 1024)
        old_a = lax.dynamic_slice(a_old_col, (0, row_at, 0), (2, 32, 1024))
        old_s = lax.dynamic_slice(s_old_row, (0, row_at, 0), (2, 32, 1024))
        keep = 1.0 - FACTOR_DECAY
        new_a = FACTOR_DECAY * old_a + keep * inv_rows * jnp.stack([ends[0], mids[0]])
        new_s = FACTOR_DECAY * old_s + keep * inv_rows * jnp.stack([mids[1], ends[1]])
        a_new_col = lax.all_gather(new_a, BOTH, axis=1, tiled=True)
        s_new_row = lax.all_gather(new_s, BOTH, axis=1, tiled=True)
        pair = [[2 * j, 2 * j + 1] for j in range(data_ways // 2)]
        grad_mat = lax.all_gather(share[:D_ROWS], 'data', axis_index_groups=pair, tiled=True) * inv_rows
        layer_id = data_id // 2
        stack_id = layer_id // 2
        is_col = lax.rem(layer_id, 2) == 0
        half_at = lax.rem(data_id, 2) * D_ROWS
        full_inv = jnp.where(is_col, lax.dynamic_slice(a_inv_col, (stack_id, half_at, 0), (1, D_ROWS, 1024))[0],
                             lax.dynamic_slice(s_inv_row, (stack_id, half_at, 0), (1, D_ROWS, 1024))[0])
        block_inv = jnp.where(is_col, lax.dynamic_slice(s_inv_col, (stack_id, 0, 0), (1, 256, 256))[0],
                              lax.dynamic_slice(a_inv_row, (stack_id, 0, 0), (1, 256, 256))[0])
        u_half = exact_dot(exact_dot(full_inv, grad_mat), block_inv)
        blk_at = 32 * data_id
        old_sc = lax.dynamic_slice(s_old_col, (0, blk_at, 0), (2, 32, 256))
        old_ar = lax.dynamic_slice(a_old_row, (0, blk_at, 0), (2, 32, 256))
        blks = share[BLOCK_BASE:].reshape(2, 2, 32, 256)
        new_sc = FACTOR_DECAY * old_sc + keep * inv_rows * blks[:, 0]
        new_ar = FACTOR_DECAY * old_ar + keep * inv_rows * blks[:, 1]
        small = jnp.concatenate([u_half, new_sc.reshape(64, 256), new_ar.reshape(64, 256)], axis=0)
        small_all = lax.all_gather(small, 'data')
        u_all = small_all[:, :D_ROWS].reshape(2, 2, 1024, 256)
        u_col = u_all[:, 0]
        u_row = jnp.swapaxes(u_all[:, 1], 1, 2)
        blk_all = jnp.swapaxes(small_all[:, D_ROWS:].reshape(8, 4, 32, 256), 0, 1).reshape(4, 256, 256)
        return (u_col, u_row, a_new_col, blk_all[:2], blk_all[2:], s_new_row)

    batch_split = P('data', None)
    col_split = P(None, None, 'model')
    row_split = P(None, 'model', None)
    replicated = P()
    return jax.shard_map(
        shard_body,
        mesh=mesh,
        in_specs=(batch_split, batch_split, col_split, row_split, replicated, row_split, row_split, replicated, replicated, row_split, row_split, replicated),
        out_specs=(col_split, row_split, replicated, row_split, row_split, replicated),
        check_vma=False,
    )
```

```python
import functools
import math
import jax
import jax.numpy as jnp
from jax import lax
from jax.sharding import PartitionSpec as P
from jax.experimental import pallas as pl
from jax.experimental.pallas import tpu as pltpu

FACTOR_DECAY = 0.8
GELU_SCALE = math.sqrt(2.0 / math.pi)
GELU_CUBIC = 0.044715
EXACT = lax.Precision.HIGHEST
TN_DIMS = (((0,), (0,)), ((), ()))
NT_DIMS = (((1,), (1,)), ((), ()))
BOTH = ('model', 'data')


def gelu_value(pre_act):
    tanh_arg = GELU_SCALE * (pre_act + GELU_CUBIC * pre_act * pre_act * pre_act)
    return 0.5 * pre_act * (1.0 + jnp.tanh(tanh_arg))


def gelu_slope(pre_act):
    tanh_arg = GELU_SCALE * (pre_act + GELU_CUBIC * pre_act * pre_act * pre_act)
    tanh_val = jnp.tanh(tanh_arg)
    return 0.5 * (1.0 + tanh_val) + 0.5 * pre_act * (1.0 - tanh_val * tanh_val) * GELU_SCALE * (1.0 + 3.0 * GELU_CUBIC * pre_act * pre_act)


def activate(pre_act):
    return gelu_value(pre_act.astype(jnp.float32)).astype(jnp.bfloat16)


def back_gate(grad_act, pre_act):
    return (grad_act.astype(jnp.float32) * gelu_slope(pre_act.astype(jnp.float32))).astype(jnp.bfloat16)


def matmul(left_mat, right_mat):
    return jnp.dot(left_mat, right_mat, preferred_element_type=jnp.float32)


def matmul_tn(left_mat, right_mat):
    return lax.dot_general(left_mat, right_mat, TN_DIMS, preferred_element_type=jnp.float32)


def matmul_nt(left_mat, right_mat):
    return lax.dot_general(left_mat, right_mat, NT_DIMS, preferred_element_type=jnp.float32)


def exact_dot(left_mat, right_mat):
    return jnp.dot(left_mat, right_mat, precision=EXACT, preferred_element_type=jnp.float32)


D_ROWS = 512
FULL_BASE = 512
BLOCK_BASE = 768
SHARE_ROWS = 896


def gram_kernel(x_ref, g1_ref, g2_ref, h1_ref, h2_ref, g3_ref, dy_ref, h3_ref, out_ref,
                act, stage, bstage, in_sem, out_sem, b_sem):
    sources = [dy_ref, h3_ref, h2_ref, g3_ref, g2_ref, h1_ref, x_ref, g1_ref]
    slots = [3, 7, 2, 6, 1, 5, 0, 4]
    loads = [pltpu.make_async_copy(src, act.at[slot], in_sem.at[slot]) for src, slot in zip(sources, slots)]
    for load in loads:
        load.start()
    started = [0]
    pend = {}

    def out_copy(slot, dst):
        return pltpu.make_async_copy(stage.at[slot], dst, out_sem.at[slot])

    for layer in (3, 2, 1, 0):
        pltpu.make_async_copy(x_ref, act.at[layer], in_sem.at[layer]).wait()
        pltpu.make_async_copy(x_ref, act.at[4 + layer], in_sem.at[4 + layer]).wait()

        def d_body(m, carry, layer=layer):
            slot = lax.rem(m, 2)
            cols = pl.ds(pl.multiple_of(m * 256, 256), 256)
            right = act[4 + layer, :, cols]
            dst = out_ref.at[pl.ds(m * 8 + 2 * layer, 2), pl.ds(0, D_ROWS)]

            if layer == 3:
                @pl.when(m >= 2)
                def _():
                    out_copy(slot, dst).wait()
                    pltpu.make_async_copy(bstage.at[slot], out_ref.at[pl.ds(0, 8), pl.ds(BLOCK_BASE, 32)], b_sem.at[slot]).wait()
            else:
                out_copy(slot, dst).wait()
                pltpu.make_async_copy(bstage.at[slot], out_ref.at[pl.ds(0, 8), pl.ds(BLOCK_BASE, 32)], b_sem.at[slot]).wait()
            prod = lax.dot_general(act[layer], right, TN_DIMS, preferred_element_type=jnp.float32)
            stage[slot] = prod.reshape(2, D_ROWS, 256)
            out_copy(slot, dst).start()
            blk = lax.dot_general(right, right, TN_DIMS, preferred_element_type=jnp.float32)
            bstage[slot] = blk.reshape(8, 32, 256)
            pltpu.make_async_copy(bstage.at[slot], out_ref.at[pl.ds(m * 8, 8), pl.ds(BLOCK_BASE + 32 * layer, 32)], b_sem.at[slot]).start()
            return carry

        lax.fori_loop(0, 4, d_body, 0)

        if layer in (2, 1):
            which = 0 if layer == 2 else 1

            def f_body(n, carry, layer=layer, which=which):
                slot = lax.rem(n, 2)
                cols = pl.ds(pl.multiple_of(n * 256, 256), 256)
                dst = out_ref.at[:, pl.ds(FULL_BASE + which * 128 + 32 * n, 32)]
                pltpu.make_async_copy(stage.at[slot], out_ref.at[pl.ds(0, 2), pl.ds(0, D_ROWS)], out_sem.at[slot]).wait()
                prod = lax.dot_general(act[layer], act[layer, :, cols], TN_DIMS, preferred_element_type=jnp.float32)
                stage[slot] = prod.reshape(2, D_ROWS, 256)
                pltpu.make_async_copy(stage.at[slot].reshape(32, 32, 256), dst, out_sem.at[slot]).start()
                return carry

            lax.fori_loop(0, 4, f_body, 0)
    for slot in range(2):
        pltpu.make_async_copy(stage.at[slot], out_ref.at[pl.ds(0, 2), pl.ds(0, D_ROWS)], out_sem.at[slot]).wait()
        pltpu.make_async_copy(bstage.at[slot], out_ref.at[pl.ds(0, 8), pl.ds(BLOCK_BASE, 32)], b_sem.at[slot]).wait()


def gram_call(x_loc, g_one, g_two, h_one, h_two, g_three, dy_loc, h_three):
    any_spec = pl.BlockSpec(memory_space=pl.ANY)
    return pl.pallas_call(
        gram_kernel,
        out_shape=jax.ShapeDtypeStruct((32, SHARE_ROWS, 256), jnp.float32),
        in_specs=[any_spec] * 8,
        out_specs=any_spec,
        scratch_shapes=[
            pltpu.VMEM((8, 1024, 1024), jnp.bfloat16),
            pltpu.VMEM((2, 2, D_ROWS, 256), jnp.float32),
            pltpu.VMEM((2, 8, 32, 256), jnp.float32),
            pltpu.SemaphoreType.DMA((8,)),
            pltpu.SemaphoreType.DMA((2,)),
            pltpu.SemaphoreType.DMA((2,)),
        ],
        compiler_params=pltpu.CompilerParams(vmem_limit_bytes=48 * 1024 * 1024),
        cost_estimate=pl.CostEstimate(flops=15_000_000_000, bytes_accessed=46_000_000, transcendentals=0),
        name='gram',
    )(x_loc, g_one, g_two, h_one, h_two, g_three, dy_loc, h_three)


MESH_ID = pl.DeviceIdType.MESH
CHUNK_ORDER = ((0, 0), (3, 0), (0, 1), (3, 1), (1, 0), (2, 0), (1, 1), (2, 1))


def torus_place():
    z = lax.axis_index('model')
    d = lax.axis_index('data')
    y = d // 4
    x = (d // 2) % 2
    c = d % 2
    near = {'x': (z, d + 2 - 4 * x), 'y': (z, d + 4 - 8 * y), 'c': (z, d + 1 - 2 * c), 'up': (z + 1, d), 'dn': (z - 1, d)}
    return z, y, x, c, near


def meet_neighbours(z, near):
    barrier = pltpu.get_barrier_semaphore()
    for side in ('x', 'y', 'c'):
        pl.semaphore_signal(barrier, inc=1, device_id=near[side], device_id_type=MESH_ID)

    @pl.when(z < 3)
    def _():
        pl.semaphore_signal(barrier, inc=1, device_id=near['up'], device_id_type=MESH_ID)

    @pl.when(z > 0)
    def _():
        pl.semaphore_signal(barrier, inc=1, device_id=near['dn'], device_id_type=MESH_ID)
    pl.semaphore_wait(barrier, 3 + (z + 3) // 4 + (6 - z) // 4)


def remote(src, dst, send_sem, recv_sem, where):
    return pltpu.make_async_remote_copy(src_ref=src, dst_ref=dst, send_sem=send_sem, recv_sem=recv_sem, device_id=where, device_id_type=MESH_ID)


def gather_kernel(n_plane, *refs):
    if n_plane:
        piece_ref, plane_ref, out_ref, pout_ref = refs[:4]
        sems = refs[4:]
    else:
        piece_ref, out_ref = refs[:2]
        sems = refs[2:]
    load_sem, z_recv, x_recv, y_recv, d_recv, c_recv, up_send, dn_send, x_send, y_send, dy_send, dx_send, c_send = sems
    z, y, x, c, near = torus_place()
    half = piece_ref.shape[0] // 2
    load = pltpu.make_async_copy(piece_ref, out_ref.at[z, y, x, c], load_sem.at[0])
    load.start()
    if n_plane:
        pload = pltpu.make_async_copy(plane_ref, pout_ref.at[y, x, c], load_sem.at[1])
        pload.start()
        phalf = plane_ref.shape[0] // 2
    meet_neighbours(z, near)

    def view(zs, yy, xx, cc):
        return pout_ref.at[yy, xx, cc] if zs is None else out_ref.at[zs, yy, xx, cc]

    def part(zs, yy, xx, cc, which):
        size = phalf if zs is None else half
        return view(zs, yy, xx, cc).at[pl.ds(which * size, size)]

    def at(zs):
        return 4 if zs is None else zs

    def x_copy(zs):
        return remote(view(zs, y, x, c), view(zs, y, x, c), x_send.at[at(zs)], x_recv.at[at(zs)], near['x'])

    def y_copy(zs):
        return remote(view(zs, y, x, c), view(zs, y, x, c), y_send.at[at(zs)], y_recv.at[at(zs)], near['y'])

    def dy_copy(zs):
        return remote(part(zs, y, 1 - x, c, 0), part(zs, y, 1 - x, c, 0), dy_send.at[at(zs)], d_recv.at[at(zs), 0], near['y'])

    def dx_copy(zs):
        return remote(part(zs, 1 - y, x, c, 1), part(zs, 1 - y, x, c, 1), dx_send.at[at(zs)], d_recv.at[at(zs), 1], near['x'])

    def c_copy(zs, kind):
        yy = y if kind in (0, 1) else 1 - y
        xx = x if kind in (0, 2) else 1 - x
        return remote(view(zs, yy, xx, c), view(zs, yy, xx, c), c_send.at[at(zs), kind], c_recv.at[at(zs), kind], near['c'])

    def up_copy(zs):
        return remote(view(zs, y, x, c), view(zs, y, x, c), up_send.at[at(zs)], z_recv.at[at(zs)], near['up'])

    def dn_copy(zs):
        return remote(view(zs, y, x, c), view(zs, y, x, c), dn_send.at[at(zs)], z_recv.at[at(zs)], near['dn'])

    def guard(off, body):
        if off is None:
            body(None)
        elif off == 0:
            body(z)
        elif off < 0:
            pl.when(z >= -off)(lambda: body(z + off))
        else:
            pl.when(z <= 3 - off)(lambda: body(z + off))

    def z_step(off):
        def body(zs):
            if off is None:
                pload.wait()
            elif off == 0:
                load.wait()
            else:
                up_copy(zs).wait_recv()
            if off is not None and off <= 0:
                pl.when(z < 3)(lambda: up_copy(zs).start())
            if off is not None and off >= 0:
                pl.when(z > 0)(lambda: dn_copy(zs).start())
            x_copy(zs).start()
            y_copy(zs).start()
            c_copy(zs, 0).start()
        guard(off, body)

    def xy_step(off):
        def body(zs):
            remote(view(zs, y, 1 - x, c), view(zs, y, 1 - x, c), x_send.at[at(zs)], x_recv.at[at(zs)], near['x']).wait_recv()
            dy_copy(zs).start()
            c_copy(zs, 1).start()
            remote(view(zs, 1 - y, x, c), view(zs, 1 - y, x, c), y_send.at[at(zs)], y_recv.at[at(zs)], near['y']).wait_recv()
            dx_copy(zs).start()
            c_copy(zs, 2).start()
        guard(off, body)

    def diag_step(off):
        def body(zs):
            for which in range(2):
                remote(part(zs, 1 - y, 1 - x, c, which), part(zs, 1 - y, 1 - x, c, which), dy_send.at[at(zs)], d_recv.at[at(zs), which], near['y']).wait_recv()
            c_copy(zs, 3).start()
        guard(off, body)

    def last_step(off):
        def body(zs):
            for kind in range(4):
                yy = y if kind in (0, 1) else 1 - y
                xx = x if kind in (0, 2) else 1 - x
                remote(view(zs, yy, xx, 1 - c), view(zs, yy, xx, 1 - c), c_send.at[at(zs), kind], c_recv.at[at(zs), kind], near['c']).wait_recv()
                c_copy(zs, kind).wait_send()
            x_copy(zs).wait_send()
            y_copy(zs).wait_send()
            dy_copy(zs).wait_send()
            dx_copy(zs).wait_send()
            if off is not None and off <= 0:
                pl.when(z < 3)(lambda: up_copy(zs).wait_send())
            if off is not None and off >= 0:
                pl.when(z > 0)(lambda: dn_copy(zs).wait_send())
        guard(off, body)

    lead = [None] if n_plane else []
    waves = [lead + [0], [-1, 1], [-2, 2], [-3, 3]]
    for step in range(6):
        for func, lag in ((z_step, 0), (xy_step, 1), (diag_step, 2)):
            if 0 <= step - lag < 4:
                for off in waves[step - lag]:
                    func(off)
    for wave in waves:
        for off in wave:
            last_step(off)


def gather_call(piece, plane, collective_id, name):
    dtype = piece.dtype
    out_shape = [jax.ShapeDtypeStruct((4, 2, 2, 2) + piece.shape, dtype)]
    args = [piece]
    if plane is not None:
        out_shape.append(jax.ShapeDtypeStruct((2, 2, 2) + plane.shape, plane.dtype))
        args.append(plane)
    dma = pltpu.SemaphoreType.DMA
    size = sum(math_prod(o.shape) * o.dtype.itemsize for o in out_shape)
    out = pl.pallas_call(
        functools.partial(gather_kernel, 0 if plane is None else 1),
        out_shape=out_shape,
        in_specs=[pl.BlockSpec(memory_space=pltpu.HBM)] * len(args),
        out_specs=[pl.BlockSpec(memory_space=pltpu.VMEM)] * len(out_shape),
        scratch_shapes=[dma((2,)), dma((5,)), dma((5,)), dma((5,)), dma((5, 2)), dma((5, 4)), dma((5,)), dma((5,)), dma((5,)), dma((5,)), dma((5,)), dma((5,)), dma((5, 4))],
        compiler_params=pltpu.CompilerParams(collective_id=collective_id, has_side_effects=True, vmem_limit_bytes=size + 8 * 1024 * 1024),
        cost_estimate=pl.CostEstimate(flops=50_000_000_000, bytes_accessed=size, transcendentals=0),
        name=name,
    )(*args)
    return out


def math_prod(shape):
    n = 1
    for s in shape:
        n *= s
    return n


def add_into(dst, src, rows):
    step = 32 if rows % 32 == 0 else 16 if rows % 16 == 0 else 8

    def body(i, carry):
        span = pl.ds(pl.multiple_of(i * step, 8), step)
        dst[span, :] = dst[span, :] + src[span, :]
        return carry

    lax.fori_loop(0, rows // step, body, 0)


def scatter_kernel(rows, parts_ref, share_ref, own, mate, one_x, one_y, two_x, two_y, up_buf, dn_buf,
                   own_sem, mate_send, mate_recv, x1_send, x1_recv, y1_send, y1_recv, x2_send, x2_recv, y2_send, y2_recv,
                   up_send, up_recv, dn_send, dn_recv, out_sem):
    z, y, x, c, near = torus_place()
    sub = rows // 4
    loads = {}
    for k, (zd, h) in enumerate(CHUNK_ORDER):
        loads[k] = []
        for col in range(2):
            span = pl.ds(col * 2 * sub + h * sub, sub)
            load = pltpu.make_async_copy(parts_ref.at[zd, :, :, c, span], own.at[zd, :, :, span], own_sem.at[k, col])
            load.start()
            loads[k].append(load)
    meet_neighbours(z, near)
    mates = {}
    for k, (zd, h) in enumerate(CHUNK_ORDER):
        mates[k] = []
        for col in range(2):
            span = pl.ds(col * 2 * sub + h * sub, sub)
            copy = remote(parts_ref.at[zd, :, :, 1 - c, span], mate.at[zd, :, :, span], mate_send.at[k, col], mate_recv.at[k, col], near['c'])
            copy.start()
            mates[k].append(copy)

    def spans(h):
        return pl.ds(h * sub, sub), pl.ds(2 * sub + h * sub, sub)

    def one_copies(k):
        zd, h = CHUNK_ORDER[k]
        first, second = spans(h)
        piece = pl.ds(h * sub, sub)
        return (remote(own.at[zd, :, 1 - x, first], one_x.at[zd, :, piece], x1_send.at[k], x1_recv.at[k], near['x']),
                remote(own.at[zd, 1 - y, :, second], one_y.at[zd, :, piece], y1_send.at[k], y1_recv.at[k], near['y']))

    def two_copies(k):
        zd, h = CHUNK_ORDER[k]
        first, second = spans(h)
        piece = pl.ds(h * sub, sub)
        return (remote(own.at[zd, 1 - y, x, first], two_y.at[zd, piece], y2_send.at[k], y2_recv.at[k], near['y']),
                remote(own.at[zd, y, 1 - x, second], two_x.at[zd, piece], x2_send.at[k], x2_recv.at[k], near['x']))

    def z_copies(k):
        zd, h = CHUNK_ORDER[k]
        out = []
        for col, span in enumerate(spans(h)):
            out.append((remote(own.at[zd, y, x, span], up_buf.at[zd, span], dn_send.at[k, col], up_recv.at[k, col], near['dn']),
                        remote(own.at[zd, y, x, span], dn_buf.at[zd, span], up_send.at[k, col], dn_recv.at[k, col], near['up'])))
        return out

    def step_a(k):
        zd, h = CHUNK_ORDER[k]
        first, second = spans(h)
        ones = one_copies(k)
        loads[k][0].wait()
        mates[k][0].wait_recv()
        for yy in range(2):
            add_into(own.at[zd, yy, 1 - x, first], mate.at[zd, yy, 1 - x, first], sub)
        ones[0].start()
        loads[k][1].wait()
        mates[k][1].wait_recv()
        for xx in range(2):
            add_into(own.at[zd, 1 - y, xx, second], mate.at[zd, 1 - y, xx, second], sub)
        ones[1].start()
        for yy in range(2):
            add_into(own.at[zd, yy, x, first], mate.at[zd, yy, x, first], sub)
        for xx in range(2):
            add_into(own.at[zd, y, xx, second], mate.at[zd, y, xx, second], sub)

    def step_b(k):
        zd, h = CHUNK_ORDER[k]
        first, second = spans(h)
        piece = pl.ds(h * sub, sub)
        ones, twos = one_copies(k), two_copies(k)
        ones[0].wait_recv()
        add_into(own.at[zd, 1 - y, x, first], one_x.at[zd, 1 - y, piece], sub)
        twos[0].start()
        ones[1].wait_recv()
        add_into(own.at[zd, y, 1 - x, second], one_y.at[zd, 1 - x, piece], sub)
        twos[1].start()
        add_into(own.at[zd, y, x, first], one_x.at[zd, y, piece], sub)
        add_into(own.at[zd, y, x, second], one_y.at[zd, x, piece], sub)

    def step_c(k):
        zd, h = CHUNK_ORDER[k]
        first, second = spans(h)
        piece = pl.ds(h * sub, sub)
        twos = two_copies(k)
        zcs = z_copies(k)
        for col, (copy, buf, span) in enumerate(((twos[0], two_y, first), (twos[1], two_x, second))):
            copy.wait_recv()
            add_into(own.at[zd, y, x, span], buf.at[zd, piece], sub)

            @pl.when((z < 3) & (z >= zd))
            def _(col=col, span=span):
                zcs[col][0].wait_recv()
                add_into(own.at[zd, y, x, span], up_buf.at[zd, span], sub)

            @pl.when((z > 0) & (z <= zd))
            def _(col=col, span=span):
                zcs[col][1].wait_recv()
                add_into(own.at[zd, y, x, span], dn_buf.at[zd, span], sub)
            pl.when(z > zd)(lambda: zcs[col][0].start())
            pl.when(z < zd)(lambda: zcs[col][1].start())

            @pl.when(z == zd)
            def _(col=col, span=span):
                pltpu.make_async_copy(own.at[zd, y, x, span], share_ref.at[span], out_sem.at[h, col]).start()

    n = len(CHUNK_ORDER)
    for step in range(n + 3):
        if step < n:
            step_a(step)
        if 0 <= step - 1 < n:
            step_b(step - 1)
        if 0 <= step - 3 < n:
            step_c(step - 3)
    for k, (zd, h) in enumerate(CHUNK_ORDER):
        for copy in mates[k] + list(one_copies(k)) + list(two_copies(k)):
            copy.wait_send()
        for col, (down, up) in enumerate(z_copies(k)):
            pl.when(z > zd)(lambda: down.wait_send())
            pl.when(z < zd)(lambda: up.wait_send())
    for h in range(2):
        for col in range(2):
            span = spans(h)[col]
            pltpu.make_async_copy(own.at[0, y, x, span], share_ref.at[span], out_sem.at[h, col]).wait()


def scatter_call(parts, collective_id, name):
    rows = parts.shape[-2]
    half = rows // 2
    f32 = jnp.float32
    dma = pltpu.SemaphoreType.DMA
    n = len(CHUNK_ORDER)
    one = (n,)
    two = (n, 2)
    return pl.pallas_call(
        functools.partial(scatter_kernel, rows),
        out_shape=jax.ShapeDtypeStruct((rows, 256), f32),
        in_specs=[pl.BlockSpec(memory_space=pltpu.HBM)],
        out_specs=pl.BlockSpec(memory_space=pltpu.HBM),
        scratch_shapes=[
            pltpu.VMEM((4, 2, 2, rows, 256), f32), pltpu.VMEM((4, 2, 2, rows, 256), f32),
            pltpu.VMEM((4, 2, half, 256), f32), pltpu.VMEM((4, 2, half, 256), f32),
            pltpu.VMEM((4, half, 256), f32), pltpu.VMEM((4, half, 256), f32),
            pltpu.VMEM((4, rows, 256), f32), pltpu.VMEM((4, rows, 256), f32),
            dma(two), dma(two), dma(two), dma(one), dma(one), dma(one), dma(one), dma(one), dma(one), dma(one), dma(one),
            dma(two), dma(two), dma(two), dma(two), dma((2, 2)),
        ],
        compiler_params=pltpu.CompilerParams(collective_id=collective_id, has_side_effects=True, vmem_limit_bytes=60 * 1024 * 1024),
        cost_estimate=pl.CostEstimate(flops=120_000_000_000, bytes_accessed=60_000_000, transcendentals=0),
        name=name,
    )(parts.reshape(4, 2, 2, 2, rows, 256))


def solution(mesh):
    data_ways = mesh.shape['data']
    model_ways = mesh.shape['model']
    n_dev = data_ways * model_ways

    def shard_body(x_tokens, dy_tokens, w_col, w_row, a_old_col, s_old_col, a_old_row, s_old_row, a_inv_col, s_inv_col, a_inv_row, s_inv_row):
        model_id = lax.axis_index('model')
        data_id = lax.axis_index('data')
        dev_id = model_id * data_ways + data_id
        inv_rows = 1.0 / (x_tokens.shape[0] * data_ways)
        col_part = lax.dynamic_slice(w_col, (0, 128 * data_id, 0), (2, 128, 256))
        row_part = lax.dynamic_slice(w_row, (0, 32 * data_id, 0), (2, 32, 1024))
        row_part = jnp.swapaxes(row_part.reshape(2, 32, 4, 256), 1, 2).reshape(256, 256)
        (w_all,) = gather_call(jnp.concatenate([col_part.reshape(256, 256), row_part], axis=0), None, 1, 'weights')
        w_all = w_all.reshape(4, 8, 4, 128, 256)
        w_c = [jnp.transpose(w_all[:, :, layer].reshape(4, 1024, 256), (1, 0, 2)).reshape(1024, 1024) for layer in range(2)]
        w_r = [jnp.swapaxes(w_all[:, :, 2 + layer].reshape(32, 4, 32, 256), 1, 2).reshape(1024, 1024) for layer in range(2)]
        x_cols = lax.dynamic_slice(x_tokens, (0, 256 * model_id), (x_tokens.shape[0], 256))
        dy_cols = lax.dynamic_slice(dy_tokens, (0, 256 * model_id), (x_tokens.shape[0], 256))
        ends = jnp.stack([matmul_tn(x_cols, x_tokens), matmul_tn(dy_cols, dy_tokens)]).reshape(2, 8, 32, 1024)
        ends = lax.psum_scatter(jnp.swapaxes(ends, 0, 1), 'data', scatter_dimension=0, tiled=False)
        rows_dev = x_tokens.shape[0] // model_ways
        x_loc = lax.dynamic_slice(x_tokens, (rows_dev * model_id, 0), (rows_dev, 1024))
        dy_loc = lax.dynamic_slice(dy_tokens, (rows_dev * model_id, 0), (rows_dev, 1024))
        z_one = matmul(x_loc, w_c[0]).astype(jnp.bfloat16)
        h_one = activate(z_one)
        z_two = matmul(h_one, w_r[0]).astype(jnp.bfloat16)
        h_two = activate(z_two)
        z_three = matmul(h_two, w_c[1]).astype(jnp.bfloat16)
        h_three = activate(z_three)
        g_three = back_gate(matmul_nt(dy_loc, w_r[1]).astype(jnp.bfloat16), z_three)
        g_two = back_gate(matmul_nt(g_three, w_c[1]).astype(jnp.bfloat16), z_two)
        g_one = back_gate(matmul_nt(g_two, w_r[0]).astype(jnp.bfloat16), z_one)
        parts = gram_call(x_loc, g_one, g_two, h_one, h_two, g_three, dy_loc, h_three)
        share = scatter_call(parts, 2, 'sums')
        row_at = 32 * dev_id
        mids = jnp.swapaxes(share[FULL_BASE:BLOCK_BASE].reshape(2, 4, 32, 256), 1, 2).reshape(2, 32, 1024)
        old_a = lax.dynamic_slice(a_old_col, (0, row_at, 0), (2, 32, 1024))
        old_s = lax.dynamic_slice(s_old_row, (0, row_at, 0), (2, 32, 1024))
        keep = 1.0 - FACTOR_DECAY
        new_a = FACTOR_DECAY * old_a + keep * inv_rows * jnp.stack([ends[0], mids[0]])
        new_s = FACTOR_DECAY * old_s + keep * inv_rows * jnp.stack([mids[1], ends[1]])
        pair = [[2 * j, 2 * j + 1] for j in range(data_ways // 2)]
        grad_mat = lax.all_gather(share[:D_ROWS], 'data', axis_index_groups=pair, tiled=True) * inv_rows
        layer_id = data_id // 2
        stack_id = layer_id // 2
        is_col = lax.rem(layer_id, 2) == 0
        half_at = lax.rem(data_id, 2) * D_ROWS
        full_inv = jnp.where(is_col, lax.dynamic_slice(a_inv_col, (stack_id, half_at, 0), (1, D_ROWS, 1024))[0],
                             lax.dynamic_slice(s_inv_row, (stack_id, half_at, 0), (1, D_ROWS, 1024))[0])
        block_inv = jnp.where(is_col, lax.dynamic_slice(s_inv_col, (stack_id, 0, 0), (1, 256, 256))[0],
                              lax.dynamic_slice(a_inv_row, (stack_id, 0, 0), (1, 256, 256))[0])
        u_half = exact_dot(exact_dot(full_inv, grad_mat), block_inv)
        blk_at = 32 * data_id
        old_sc = lax.dynamic_slice(s_old_col, (0, blk_at, 0), (2, 32, 256))
        old_ar = lax.dynamic_slice(a_old_row, (0, blk_at, 0), (2, 32, 256))
        blks = share[BLOCK_BASE:].reshape(2, 2, 32, 256)
        new_sc = FACTOR_DECAY * old_sc + keep * inv_rows * blks[:, 0]
        new_ar = FACTOR_DECAY * old_ar + keep * inv_rows * blks[:, 1]
        small = jnp.concatenate([u_half, new_sc.reshape(64, 256), new_ar.reshape(64, 256)], axis=0)
        fact_all, small_all = gather_call(jnp.concatenate([new_a, new_s], axis=0).reshape(128, 1024), small, 3, 'results')
        fact_all = jnp.swapaxes(fact_all.reshape(32, 4, 32, 1024), 0, 1).reshape(4, 1024, 1024)
        a_new_col, s_new_row = fact_all[:2], fact_all[2:]
        small_all = small_all.reshape(8, 640, 256)
        u_all = small_all[:, :D_ROWS].reshape(2, 2, 1024, 256)
        u_col = u_all[:, 0]
        u_row = jnp.swapaxes(u_all[:, 1], 1, 2)
        blk_all = jnp.swapaxes(small_all[:, D_ROWS:].reshape(8, 4, 32, 256), 0, 1).reshape(4, 256, 256)
        return (u_col, u_row, a_new_col, blk_all[:2], blk_all[2:], s_new_row)

    batch_split = P('data', None)
    col_split = P(None, None, 'model')
    row_split = P(None, 'model', None)
    replicated = P()
    return jax.shard_map(
        shard_body,
        mesh=mesh,
        in_specs=(batch_split, batch_split, col_split, row_split, replicated, row_split, row_split, replicated, replicated, row_split, row_split, replicated),
        out_specs=(col_split, row_split, replicated, row_split, row_split, replicated),
        check_vma=False,
    )
```

```python
import functools
import math
import jax
import jax.numpy as jnp
from jax import lax
from jax.sharding import PartitionSpec as P
from jax.experimental import pallas as pl
from jax.experimental.pallas import tpu as pltpu

FACTOR_DECAY = 0.8
GELU_SCALE = math.sqrt(2.0 / math.pi)
GELU_CUBIC = 0.044715
EXACT = lax.Precision.HIGHEST
TN_DIMS = (((0,), (0,)), ((), ()))
NT_DIMS = (((1,), (1,)), ((), ()))
BOTH = ('model', 'data')


def gelu_value(pre_act):
    tanh_arg = GELU_SCALE * (pre_act + GELU_CUBIC * pre_act * pre_act * pre_act)
    return 0.5 * pre_act * (1.0 + jnp.tanh(tanh_arg))


def gelu_slope(pre_act):
    tanh_arg = GELU_SCALE * (pre_act + GELU_CUBIC * pre_act * pre_act * pre_act)
    tanh_val = jnp.tanh(tanh_arg)
    return 0.5 * (1.0 + tanh_val) + 0.5 * pre_act * (1.0 - tanh_val * tanh_val) * GELU_SCALE * (1.0 + 3.0 * GELU_CUBIC * pre_act * pre_act)


def activate(pre_act):
    return gelu_value(pre_act.astype(jnp.float32)).astype(jnp.bfloat16)


def back_gate(grad_act, pre_act):
    return (grad_act.astype(jnp.float32) * gelu_slope(pre_act.astype(jnp.float32))).astype(jnp.bfloat16)


def matmul(left_mat, right_mat):
    return jnp.dot(left_mat, right_mat, preferred_element_type=jnp.float32)


def matmul_tn(left_mat, right_mat):
    return lax.dot_general(left_mat, right_mat, TN_DIMS, preferred_element_type=jnp.float32)


def matmul_nt(left_mat, right_mat):
    return lax.dot_general(left_mat, right_mat, NT_DIMS, preferred_element_type=jnp.float32)


def exact_dot(left_mat, right_mat):
    return jnp.dot(left_mat, right_mat, precision=EXACT, preferred_element_type=jnp.float32)


MIB = 1024 * 1024
BLOCK = 256
HIDDEN = 1024
D_ROWS = 512
FULL_BASE = 512
BLOCK_BASE = 768
SHARE_ROWS = 896


def gram_kernel(x_ref, g1_ref, g2_ref, h1_ref, h2_ref, g3_ref, dy_ref, h3_ref, out_ref,
                act, stage, bstage, in_sem, out_sem, b_sem):
    sources = [dy_ref, h3_ref, h2_ref, g3_ref, g2_ref, h1_ref, x_ref, g1_ref]
    slots = [3, 7, 2, 6, 1, 5, 0, 4]
    loads = [pltpu.make_async_copy(src, act.at[slot], in_sem.at[slot]) for src, slot in zip(sources, slots)]
    for load in loads:
        load.start()
    started = [0]
    pend = {}

    def out_copy(slot, dst):
        return pltpu.make_async_copy(stage.at[slot], dst, out_sem.at[slot])

    for layer in (3, 2, 1, 0):
        pltpu.make_async_copy(x_ref, act.at[layer], in_sem.at[layer]).wait()
        pltpu.make_async_copy(x_ref, act.at[4 + layer], in_sem.at[4 + layer]).wait()

        def d_body(m, carry, layer=layer):
            slot = lax.rem(m, 2)
            cols = pl.ds(pl.multiple_of(m * BLOCK, BLOCK), BLOCK)
            right = act[4 + layer, :, cols]
            dst = out_ref.at[pl.ds(m * 8 + 2 * layer, 2), pl.ds(0, D_ROWS)]

            if layer == 3:
                @pl.when(m >= 2)
                def _():
                    out_copy(slot, dst).wait()
                    pltpu.make_async_copy(bstage.at[slot], out_ref.at[pl.ds(0, 8), pl.ds(BLOCK_BASE, 32)], b_sem.at[slot]).wait()
            else:
                out_copy(slot, dst).wait()
                pltpu.make_async_copy(bstage.at[slot], out_ref.at[pl.ds(0, 8), pl.ds(BLOCK_BASE, 32)], b_sem.at[slot]).wait()
            prod = lax.dot_general(act[layer], right, TN_DIMS, preferred_element_type=jnp.float32)
            stage[slot] = prod.reshape(2, D_ROWS, BLOCK)
            out_copy(slot, dst).start()
            blk = lax.dot_general(right, right, TN_DIMS, preferred_element_type=jnp.float32)
            bstage[slot] = blk.reshape(8, 32, BLOCK)
            pltpu.make_async_copy(bstage.at[slot], out_ref.at[pl.ds(m * 8, 8), pl.ds(BLOCK_BASE + 32 * layer, 32)], b_sem.at[slot]).start()
            return carry

        lax.fori_loop(0, 4, d_body, 0)

        if layer in (2, 1):
            which = 0 if layer == 2 else 1

            def f_body(n, carry, layer=layer, which=which):
                slot = lax.rem(n, 2)
                cols = pl.ds(pl.multiple_of(n * BLOCK, BLOCK), BLOCK)
                dst = out_ref.at[pl.ds(n * 8, 8), pl.ds(FULL_BASE + which * 128, 128)]
                pltpu.make_async_copy(stage.at[slot], out_ref.at[pl.ds(0, 2), pl.ds(0, D_ROWS)], out_sem.at[slot]).wait()
                prod = lax.dot_general(act[layer], act[layer, :, cols], TN_DIMS, preferred_element_type=jnp.float32)
                stage[slot] = prod.reshape(2, D_ROWS, BLOCK)
                pltpu.make_async_copy(stage.at[slot].reshape(8, 128, BLOCK), dst, out_sem.at[slot]).start()
                return carry

            lax.fori_loop(0, 4, f_body, 0)
    for slot in range(2):
        pltpu.make_async_copy(stage.at[slot], out_ref.at[pl.ds(0, 2), pl.ds(0, D_ROWS)], out_sem.at[slot]).wait()
        pltpu.make_async_copy(bstage.at[slot], out_ref.at[pl.ds(0, 8), pl.ds(BLOCK_BASE, 32)], b_sem.at[slot]).wait()


def gram_call(x_loc, g_one, g_two, h_one, h_two, g_three, dy_loc, h_three):
    any_spec = pl.BlockSpec(memory_space=pl.ANY)
    return pl.pallas_call(
        gram_kernel,
        out_shape=jax.ShapeDtypeStruct((32, SHARE_ROWS, BLOCK), jnp.float32),
        in_specs=[any_spec] * 8,
        out_specs=any_spec,
        scratch_shapes=[
            pltpu.VMEM((8, HIDDEN, HIDDEN), jnp.bfloat16),
            pltpu.VMEM((2, 2, D_ROWS, BLOCK), jnp.float32),
            pltpu.VMEM((2, 8, 32, BLOCK), jnp.float32),
            pltpu.SemaphoreType.DMA((8,)),
            pltpu.SemaphoreType.DMA((2,)),
            pltpu.SemaphoreType.DMA((2,)),
        ],
        compiler_params=pltpu.CompilerParams(vmem_limit_bytes=48 * HIDDEN * HIDDEN),
        cost_estimate=pl.CostEstimate(flops=15_000_000_000, bytes_accessed=46_000_000, transcendentals=0),
        name='gram',
    )(x_loc, g_one, g_two, h_one, h_two, g_three, dy_loc, h_three)


MESH_ID = pl.DeviceIdType.MESH
CHUNK_ORDER = ((0, 0), (3, 0), (0, 1), (3, 1), (1, 0), (2, 0), (1, 1), (2, 1))


def torus_place():
    z = lax.axis_index('model')
    d = lax.axis_index('data')
    y = d // 4
    x = (d // 2) % 2
    c = d % 2
    near = {'x': (z, d + 2 - 4 * x), 'y': (z, d + 4 - 8 * y), 'c': (z, d + 1 - 2 * c), 'up': (z + 1, d), 'dn': (z - 1, d)}
    return z, y, x, c, near


def meet_neighbours(z, near):
    barrier = pltpu.get_barrier_semaphore()
    for side in ('x', 'y', 'c'):
        pl.semaphore_signal(barrier, inc=1, device_id=near[side], device_id_type=MESH_ID)

    @pl.when(z < 3)
    def _():
        pl.semaphore_signal(barrier, inc=1, device_id=near['up'], device_id_type=MESH_ID)

    @pl.when(z > 0)
    def _():
        pl.semaphore_signal(barrier, inc=1, device_id=near['dn'], device_id_type=MESH_ID)
    pl.semaphore_wait(barrier, 3 + (z + 3) // 4 + (6 - z) // 4)


def remote(src, dst, send_sem, recv_sem, where):
    return pltpu.make_async_remote_copy(src_ref=src, dst_ref=dst, send_sem=send_sem, recv_sem=recv_sem, device_id=where, device_id_type=MESH_ID)


def gather_kernel(plan, *refs):
    n = len(plan.items)
    pieces, outs, lands = refs[:plan.n_in], refs[plan.n_in:plan.n_in + n], refs[plan.n_in + n:plan.n_in + 2 * n]
    load_sem, z_recv, x_recv, y_recv, d_recv, c_recv, up_send, dn_send, x_send, y_send, dy_send, dx_send, c_send, flush_sem = refs[plan.n_in + 2 * n:]
    z, y, x, c, near = torus_place()

    def slot(ref, j, zs, yy, xx, cc):
        return plan.items[j].slot(ref, zs, 4 * yy + 2 * xx + cc)

    def view(j, zs, yy, xx, cc):
        return slot(lands[j], j, zs, yy, xx, cc)

    def half(j, zs, yy, xx, cc, which):
        return plan.items[j].half(lands[j], zs, 4 * yy + 2 * xx + cc, which)

    def flush(j, zs, yy, xx, cc, index):
        return pltpu.make_async_copy(view(j, zs, yy, xx, cc), slot(outs[j], j, zs, yy, xx, cc), flush_sem.at[j, zs, index])

    loads = [pltpu.make_async_copy(item.piece(pieces, z, 4 * y + 2 * x + c), view(j, z, y, x, c), load_sem.at[j]) for j, item in enumerate(plan.items)]
    for load in loads:
        load.start()
    meet_neighbours(z, near)

    def side_copy(j, zs, side):
        send, recv = {'x': (x_send, x_recv), 'y': (y_send, y_recv), 'up': (up_send, z_recv), 'dn': (dn_send, z_recv)}[side]
        return remote(view(j, zs, y, x, c), view(j, zs, y, x, c), send.at[j, zs], recv.at[j, zs], near[side])

    def from_side(j, zs, side):
        yy, xx = (y, 1 - x) if side == 'x' else (1 - y, x)
        send, recv = {'x': (x_send, x_recv), 'y': (y_send, y_recv)}[side]
        return remote(view(j, zs, yy, xx, c), view(j, zs, yy, xx, c), send.at[j, zs], recv.at[j, zs], near[side])

    def dy_copy(j, zs):
        return remote(half(j, zs, y, 1 - x, c, 0), half(j, zs, y, 1 - x, c, 0), dy_send.at[j, zs], d_recv.at[j, zs, 0], near['y'])

    def dx_copy(j, zs):
        return remote(half(j, zs, 1 - y, x, c, 1), half(j, zs, 1 - y, x, c, 1), dx_send.at[j, zs], d_recv.at[j, zs, 1], near['x'])

    def kind_place(kind):
        return (y if kind < 2 else 1 - y), (x if kind % 2 == 0 else 1 - x)

    def c_copy(j, zs, kind):
        yy, xx = kind_place(kind)
        return remote(view(j, zs, yy, xx, c), view(j, zs, yy, xx, c), c_send.at[j, zs, kind], c_recv.at[j, zs, kind], near['c'])

    def share_core(j, zs, kind):
        yy, xx = kind_place(kind)
        c_copy(j, zs, kind).start()
        flush(j, zs, yy, xx, c, kind).start()

    def guard(off, body):
        if off == 0:
            body(z)
        elif off < 0:
            pl.when(z >= -off)(lambda: body(z + off))
        else:
            pl.when(z <= 3 - off)(lambda: body(z + off))

    def z_step(j, off):
        def body(zs):
            if off == 0:
                loads[j].wait()
            else:
                side_copy(j, zs, 'up').wait_recv()
            if off <= 0 and not plan.items[j].plane:
                pl.when(z < 3)(lambda: side_copy(j, zs, 'up').start())
            if off >= 0 and not plan.items[j].plane:
                pl.when(z > 0)(lambda: side_copy(j, zs, 'dn').start())
            side_copy(j, zs, 'x').start()
            side_copy(j, zs, 'y').start()
            share_core(j, zs, 0)
        guard(off, body)

    def xy_step(j, off):
        def body(zs):
            from_side(j, zs, 'x').wait_recv()
            dy_copy(j, zs).start()
            share_core(j, zs, 1)
            from_side(j, zs, 'y').wait_recv()
            dx_copy(j, zs).start()
            share_core(j, zs, 2)
        guard(off, body)

    def diag_step(j, off):
        def body(zs):
            for which in range(2):
                remote(half(j, zs, 1 - y, 1 - x, c, which), half(j, zs, 1 - y, 1 - x, c, which), dy_send.at[j, zs], d_recv.at[j, zs, which], near['y']).wait_recv()
            share_core(j, zs, 3)
        guard(off, body)

    def core_step(j, off):
        def body(zs):
            for kind in range(4):
                yy, xx = kind_place(kind)
                remote(view(j, zs, yy, xx, 1 - c), view(j, zs, yy, xx, 1 - c), c_send.at[j, zs, kind], c_recv.at[j, zs, kind], near['c']).wait_recv()
                flush(j, zs, yy, xx, 1 - c, 4 + kind).start()
        guard(off, body)

    def last_step(j, off):
        def body(zs):
            for kind in range(4):
                yy, xx = kind_place(kind)
                c_copy(j, zs, kind).wait_send()
                flush(j, zs, yy, xx, c, kind).wait()
                flush(j, zs, yy, xx, 1 - c, 4 + kind).wait()
            side_copy(j, zs, 'x').wait_send()
            side_copy(j, zs, 'y').wait_send()
            dy_copy(j, zs).wait_send()
            dx_copy(j, zs).wait_send()
            if off <= 0 and not plan.items[j].plane:
                pl.when(z < 3)(lambda: side_copy(j, zs, 'up').wait_send())
            if off >= 0 and not plan.items[j].plane:
                pl.when(z > 0)(lambda: side_copy(j, zs, 'dn').wait_send())
        guard(off, body)

    waves = [[(j, 0) for j in plan.order]]
    for far in range(1, 4):
        waves.append([(j, sign * far) for j in plan.order if not plan.items[j].plane for sign in (-1, 1)])
    for step in range(7):
        for func, lag in ((z_step, 0), (xy_step, 1), (diag_step, 2), (core_step, 3)):
            if 0 <= step - lag < 4:
                for j, off in waves[step - lag]:
                    func(j, off)
    for wave in waves:
        for j, off in wave:
            last_step(j, off)


class Item:
    def __init__(self, shape, dtype, piece, slot, half, plane=False):
        self.shape, self.dtype, self.piece, self.slot, self.half, self.plane = shape, dtype, piece, slot, half, plane


class Plan:
    def __init__(self, n_in, items, order):
        self.n_in, self.items, self.order = n_in, items, order


def gather_call(args, items, order, collective_id, name):
    n = len(items)
    dma = pltpu.SemaphoreType.DMA
    size = sum(math.prod(item.shape) * jnp.dtype(item.dtype).itemsize for item in items)
    hbm = pl.BlockSpec(memory_space=pltpu.HBM)
    flat = dma((n, 4))
    return pl.pallas_call(
        functools.partial(gather_kernel, Plan(len(args), items, order)),
        out_shape=[jax.ShapeDtypeStruct(item.shape, item.dtype) for item in items],
        in_specs=[hbm] * len(args),
        out_specs=[hbm] * n,
        scratch_shapes=[pltpu.VMEM(item.shape, item.dtype) for item in items]
        + [dma((n,)), flat, flat, flat, dma((n, 4, 2)), dma((n, 4, 4)), flat, flat, flat, flat, flat, flat, dma((n, 4, 4)), dma((n, 4, 8))],
        compiler_params=pltpu.CompilerParams(collective_id=collective_id, has_side_effects=True, vmem_limit_bytes=size + 8 * MIB),
        cost_estimate=pl.CostEstimate(flops=50_000_000_000, bytes_accessed=size, transcendentals=0),
        name=name,
    )(*args)


def col_slot(ref, zs, d):
    return ref.at[pl.ds(d * 128, 128), pl.ds(zs * BLOCK, BLOCK)]


def col_half(ref, zs, d, which):
    return ref.at[pl.ds(d * 128 + which * 64, 64), pl.ds(zs * BLOCK, BLOCK)]


def row_slot(ref, zs, d):
    return ref.at[pl.ds((zs * 8 + d) * 32, 32)]


def row_half(ref, zs, d, which):
    return ref.at[pl.ds((zs * 8 + d) * 32 + which * 16, 16)]


def gather_weights(w_col, w_row):
    shape = (HIDDEN, HIDDEN)
    items = [Item(shape, w_col.dtype, lambda refs, z, d, i=i: refs[0].at[i, pl.ds(d * 128, 128)], col_slot, col_half) for i in range(2)]
    items += [Item(shape, w_row.dtype, lambda refs, z, d, i=i: refs[1].at[i, pl.ds(d * 32, 32)], row_slot, row_half) for i in range(2)]
    return gather_call((w_col, w_row), items, (0, 3, 2, 1), 1, 'weights')


def gather_results(facts, u_half, blocks):
    items = [
        Item((4, HIDDEN, HIDDEN), facts.dtype, lambda refs, z, d: refs[0],
             lambda ref, zs, d: ref.at[:, pl.ds(d * 128, 128), pl.ds(zs * BLOCK, BLOCK)],
             lambda ref, zs, d, which: ref.at[pl.ds(2 * which, 2), pl.ds(d * 128, 128), pl.ds(zs * BLOCK, BLOCK)]),
        Item((8, D_ROWS, BLOCK), facts.dtype, lambda refs, z, d: refs[1],
             lambda ref, zs, d: ref.at[d], lambda ref, zs, d, which: ref.at[d, pl.ds(which * BLOCK, BLOCK)], True),
        Item((4, BLOCK, BLOCK), facts.dtype, lambda refs, z, d: refs[2],
             lambda ref, zs, d: ref.at[:, pl.ds(d * 32, 32)], lambda ref, zs, d, which: ref.at[pl.ds(2 * which, 2), pl.ds(d * 32, 32)], True),
    ]
    return gather_call((facts, u_half, blocks), items, (1, 2, 0), 3, 'results')


def add_into(dst, src, rows):
    step = 32 if rows % 32 == 0 else 16 if rows % 16 == 0 else 8

    def body(i, carry):
        span = pl.ds(pl.multiple_of(i * step, 8), step)
        dst[span, :] = dst[span, :] + src[span, :]
        return carry

    lax.fori_loop(0, rows // step, body, 0)


def scatter_kernel(rows, parts_ref, ends_ref, share_ref, eshare_ref, grad_ref, own, mate, one_x, one_y, two_x, two_y, up_buf, dn_buf,
                   eown, emate, eone, etwo, gland, e_sem, emate_sem, eone_sem, etwo_sem, g_sem, out2_sem,
                   own_sem, mate_send, mate_recv, x1_send, x1_recv, y1_send, y1_recv, x2_send, x2_recv, y2_send, y2_recv,
                   up_send, up_recv, dn_send, dn_recv, out_sem):
    z, y, x, c, near = torus_place()
    sub = rows // 4
    eload = pltpu.make_async_copy(ends_ref.at[:, :, :, c], eown, e_sem.at[0])
    eload.start()
    loads = {}
    for k, (zd, h) in enumerate(CHUNK_ORDER):
        loads[k] = []
        for col in range(2):
            span = pl.ds(col * 2 * sub + h * sub, sub)
            load = pltpu.make_async_copy(parts_ref.at[zd, :, :, c, span], own.at[zd, :, :, span], own_sem.at[k, col])
            load.start()
            loads[k].append(load)
    meet_neighbours(z, near)
    ematec = remote(ends_ref.at[:, :, :, 1 - c], emate, emate_sem.at[0], emate_sem.at[1], near['c'])
    ematec.start()
    eones = (remote(eown.at[0, :, 1 - x], eone.at[0], eone_sem.at[0], eone_sem.at[1], near['x']),
             remote(eown.at[1, 1 - y], eone.at[1], eone_sem.at[2], eone_sem.at[3], near['y']))
    etwos = (remote(eown.at[0, 1 - y, x], etwo.at[0], etwo_sem.at[0], etwo_sem.at[1], near['y']),
             remote(eown.at[1, y, 1 - x], etwo.at[1], etwo_sem.at[2], etwo_sem.at[3], near['x']))
    mates = {}
    for k, (zd, h) in enumerate(CHUNK_ORDER):
        mates[k] = []
        for col in range(2):
            span = pl.ds(col * 2 * sub + h * sub, sub)
            copy = remote(parts_ref.at[zd, :, :, 1 - c, span], mate.at[zd, :, :, span], mate_send.at[k, col], mate_recv.at[k, col], near['c'])
            copy.start()
            mates[k].append(copy)

    def spans(h):
        return pl.ds(h * sub, sub), pl.ds(2 * sub + h * sub, sub)

    def one_copies(k):
        zd, h = CHUNK_ORDER[k]
        first, second = spans(h)
        piece = pl.ds(h * sub, sub)
        return (remote(own.at[zd, :, 1 - x, first], one_x.at[zd, :, piece], x1_send.at[k], x1_recv.at[k], near['x']),
                remote(own.at[zd, 1 - y, :, second], one_y.at[zd, :, piece], y1_send.at[k], y1_recv.at[k], near['y']))

    def two_copies(k):
        zd, h = CHUNK_ORDER[k]
        first, second = spans(h)
        piece = pl.ds(h * sub, sub)
        return (remote(own.at[zd, 1 - y, x, first], two_y.at[zd, piece], y2_send.at[k], y2_recv.at[k], near['y']),
                remote(own.at[zd, y, 1 - x, second], two_x.at[zd, piece], x2_send.at[k], x2_recv.at[k], near['x']))

    def z_copies(k):
        zd, h = CHUNK_ORDER[k]
        out = []
        for col, span in enumerate(spans(h)):
            out.append((remote(own.at[zd, y, x, span], up_buf.at[zd, span], dn_send.at[k, col], up_recv.at[k, col], near['dn']),
                        remote(own.at[zd, y, x, span], dn_buf.at[zd, span], up_send.at[k, col], dn_recv.at[k, col], near['up'])))
        return out

    def step_a(k):
        zd, h = CHUNK_ORDER[k]
        first, second = spans(h)
        ones = one_copies(k)
        loads[k][0].wait()
        mates[k][0].wait_recv()
        for yy in range(2):
            add_into(own.at[zd, yy, 1 - x, first], mate.at[zd, yy, 1 - x, first], sub)
        ones[0].start()
        loads[k][1].wait()
        mates[k][1].wait_recv()
        for xx in range(2):
            add_into(own.at[zd, 1 - y, xx, second], mate.at[zd, 1 - y, xx, second], sub)
        ones[1].start()
        for yy in range(2):
            add_into(own.at[zd, yy, x, first], mate.at[zd, yy, x, first], sub)
        for xx in range(2):
            add_into(own.at[zd, y, xx, second], mate.at[zd, y, xx, second], sub)

    def step_b(k):
        zd, h = CHUNK_ORDER[k]
        first, second = spans(h)
        piece = pl.ds(h * sub, sub)
        ones, twos = one_copies(k), two_copies(k)
        ones[0].wait_recv()
        add_into(own.at[zd, 1 - y, x, first], one_x.at[zd, 1 - y, piece], sub)
        twos[0].start()
        ones[1].wait_recv()
        add_into(own.at[zd, y, 1 - x, second], one_y.at[zd, 1 - x, piece], sub)
        twos[1].start()
        add_into(own.at[zd, y, x, first], one_x.at[zd, y, piece], sub)
        add_into(own.at[zd, y, x, second], one_y.at[zd, x, piece], sub)

    def step_c(k):
        zd, h = CHUNK_ORDER[k]
        first, second = spans(h)
        piece = pl.ds(h * sub, sub)
        twos = two_copies(k)
        zcs = z_copies(k)
        for col, (copy, buf, span) in enumerate(((twos[0], two_y, first), (twos[1], two_x, second))):
            copy.wait_recv()
            add_into(own.at[zd, y, x, span], buf.at[zd, piece], sub)

            @pl.when((z < 3) & (z >= zd))
            def _(col=col, span=span):
                zcs[col][0].wait_recv()
                add_into(own.at[zd, y, x, span], up_buf.at[zd, span], sub)

            @pl.when((z > 0) & (z <= zd))
            def _(col=col, span=span):
                zcs[col][1].wait_recv()
                add_into(own.at[zd, y, x, span], dn_buf.at[zd, span], sub)
            pl.when(z > zd)(lambda: zcs[col][0].start())
            pl.when(z < zd)(lambda: zcs[col][1].start())

            @pl.when(z == zd)
            def _(col=col, span=span):
                pltpu.make_async_copy(own.at[zd, y, x, span], share_ref.at[span], out_sem.at[h, col]).start()

    def ends_a():
        eload.wait()
        ematec.wait_recv()
        for mat in range(2):
            for yy in range(2):
                for xx in range(2):
                    add_into(eown.at[mat, yy, xx], emate.at[mat, yy, xx], 128)
            eones[mat].start()

    def ends_b():
        eones[0].wait_recv()
        for yy in range(2):
            add_into(eown.at[0, yy, x], eone.at[0, yy], 128)
        etwos[0].start()
        eones[1].wait_recv()
        for xx in range(2):
            add_into(eown.at[1, y, xx], eone.at[1, xx], 128)
        etwos[1].start()

    def ends_c():
        for mat in range(2):
            etwos[mat].wait_recv()
            add_into(eown.at[mat, y, x], etwo.at[mat], 128)
            pltpu.make_async_copy(eown.at[mat, y, x], eshare_ref.at[mat], out2_sem.at[mat]).start()

    n = len(CHUNK_ORDER)
    ends_a()
    for step in range(n + 3):
        if step == 1:
            ends_b()
        if step == 2:
            ends_c()
        if step < n:
            step_a(step)
        if 0 <= step - 1 < n:
            step_b(step - 1)
        if 0 <= step - 3 < n:
            step_c(step - 3)
    mine = own.at[z, y, x, pl.ds(0, D_ROWS)]
    gcopy = remote(mine, gland, g_sem.at[0], g_sem.at[1], near['c'])
    gcopy.start()
    gout = pltpu.make_async_copy(mine, grad_ref.at[c], out2_sem.at[2])
    gout.start()
    gcopy.wait_recv()
    gmate = pltpu.make_async_copy(gland, grad_ref.at[1 - c], out2_sem.at[3])
    gmate.start()
    for copy in (ematec, gcopy) + eones + etwos:
        copy.wait_send()
    for k, (zd, h) in enumerate(CHUNK_ORDER):
        for copy in mates[k] + list(one_copies(k)) + list(two_copies(k)):
            copy.wait_send()
        for col, (down, up) in enumerate(z_copies(k)):
            pl.when(z > zd)(lambda: down.wait_send())
            pl.when(z < zd)(lambda: up.wait_send())
    for h in range(2):
        for col in range(2):
            span = spans(h)[col]
            pltpu.make_async_copy(own.at[0, y, x, span], share_ref.at[span], out_sem.at[h, col]).wait()
    for mat in range(2):
        pltpu.make_async_copy(eown.at[mat, y, x], eshare_ref.at[mat], out2_sem.at[mat]).wait()
    gout.wait()
    gmate.wait()


def scatter_call(parts, ends, collective_id, name):
    rows = parts.shape[-2]
    half = rows // 2
    f32 = jnp.float32
    dma = pltpu.SemaphoreType.DMA
    n = len(CHUNK_ORDER)
    whole = pltpu.VMEM((4, 2, 2, rows, BLOCK), f32)
    one_buf = pltpu.VMEM((4, 2, half, BLOCK), f32)
    two_buf = pltpu.VMEM((4, half, BLOCK), f32)
    z_buf = pltpu.VMEM((4, rows, BLOCK), f32)
    e_buf = pltpu.VMEM((2, 2, 2, 128, BLOCK), f32)
    hbm = pl.BlockSpec(memory_space=pltpu.HBM)
    return pl.pallas_call(
        functools.partial(scatter_kernel, rows),
        out_shape=[jax.ShapeDtypeStruct((rows, BLOCK), f32), jax.ShapeDtypeStruct((2, 128, BLOCK), f32), jax.ShapeDtypeStruct((2, D_ROWS, BLOCK), f32)],
        in_specs=[hbm] * 2,
        out_specs=[hbm] * 3,
        scratch_shapes=[whole, whole, one_buf, one_buf, two_buf, two_buf, z_buf, z_buf,
                        e_buf, e_buf, pltpu.VMEM((2, 2, 128, BLOCK), f32), pltpu.VMEM((2, 128, BLOCK), f32), pltpu.VMEM((D_ROWS, BLOCK), f32),
                        dma((1,)), dma((2,)), dma((4,)), dma((4,)), dma((2,)), dma((4,))]
        + [dma((n, 2))] * 3 + [dma((n,))] * 8 + [dma((n, 2))] * 4 + [dma((2, 2))],
        compiler_params=pltpu.CompilerParams(collective_id=collective_id, has_side_effects=True, vmem_limit_bytes=60 * MIB),
        cost_estimate=pl.CostEstimate(flops=120_000_000_000, bytes_accessed=60 * MIB, transcendentals=0),
        name=name,
    )(parts.reshape(4, 2, 2, 2, rows, BLOCK), ends.reshape(2, 2, 2, 2, 128, BLOCK))


def solution(mesh):
    data_ways = mesh.shape['data']
    model_ways = mesh.shape['model']

    def shard_body(x_tokens, dy_tokens, w_col, w_row, a_old_col, s_old_col, a_old_row, s_old_row, a_inv_col, s_inv_col, a_inv_row, s_inv_row):
        model_id = lax.axis_index('model')
        data_id = lax.axis_index('data')
        inv_rows = 1.0 / (x_tokens.shape[0] * data_ways)
        w_one, w_three, w_two, w_four = gather_weights(w_col, w_row)
        x_cols = lax.dynamic_slice(x_tokens, (0, BLOCK * model_id), (x_tokens.shape[0], BLOCK))
        dy_cols = lax.dynamic_slice(dy_tokens, (0, BLOCK * model_id), (x_tokens.shape[0], BLOCK))
        ends = jnp.stack([matmul_tn(x_tokens, x_cols), matmul_tn(dy_tokens, dy_cols)])
        rows_dev = x_tokens.shape[0] // model_ways
        x_loc = lax.dynamic_slice(x_tokens, (rows_dev * model_id, 0), (rows_dev, HIDDEN))
        dy_loc = lax.dynamic_slice(dy_tokens, (rows_dev * model_id, 0), (rows_dev, HIDDEN))
        z_one = matmul(x_loc, w_one).astype(jnp.bfloat16)
        h_one = activate(z_one)
        z_two = matmul(h_one, w_two).astype(jnp.bfloat16)
        h_two = activate(z_two)
        z_three = matmul(h_two, w_three).astype(jnp.bfloat16)
        h_three = activate(z_three)
        g_three = back_gate(matmul_nt(dy_loc, w_four).astype(jnp.bfloat16), z_three)
        g_two = back_gate(matmul_nt(g_three, w_three).astype(jnp.bfloat16), z_two)
        g_one = back_gate(matmul_nt(g_two, w_two).astype(jnp.bfloat16), z_one)
        parts = gram_call(x_loc, g_one, g_two, h_one, h_two, g_three, dy_loc, h_three)
        share, eshare, grad_mat = scatter_call(parts, ends, 2, 'sums')
        keep = 1.0 - FACTOR_DECAY
        spot = (0, 128 * data_id, BLOCK * model_id)
        mids = share[FULL_BASE:BLOCK_BASE].reshape(2, 128, BLOCK)
        sums = jnp.stack([eshare[0], mids[0], mids[1], eshare[1]])
        olds = jnp.concatenate([lax.dynamic_slice(old, spot, (2, 128, BLOCK)) for old in (a_old_col, s_old_row)])
        facts = FACTOR_DECAY * olds + keep * inv_rows * sums
        grad_mat = grad_mat.reshape(HIDDEN, BLOCK) * inv_rows
        layer_id = data_id // 2
        stack_id = layer_id // 2
        is_col = lax.rem(layer_id, 2) == 0
        half_at = lax.rem(data_id, 2) * D_ROWS
        full_inv = jnp.where(is_col, *[lax.dynamic_slice(inv, (stack_id, half_at, 0), (1, D_ROWS, HIDDEN))[0] for inv in (a_inv_col, s_inv_row)])
        block_inv = jnp.where(is_col, *[lax.dynamic_slice(inv, (stack_id, 0, 0), (1, BLOCK, BLOCK))[0] for inv in (s_inv_col, a_inv_row)])
        u_half = exact_dot(exact_dot(full_inv, grad_mat), block_inv)
        old_blocks = jnp.concatenate([lax.dynamic_slice(old, (0, 32 * data_id, 0), (2, 32, BLOCK)) for old in (s_old_col, a_old_row)])
        new_blocks = jnp.swapaxes(share[BLOCK_BASE:].reshape(2, 2, 32, BLOCK), 0, 1).reshape(4, 32, BLOCK)
        blocks = FACTOR_DECAY * old_blocks + keep * inv_rows * new_blocks
        fact_all, u_all, blk_all = gather_results(facts, u_half, blocks)
        u_all = u_all.reshape(2, 2, HIDDEN, BLOCK)
        u_col = u_all[:, 0]
        u_row = jnp.swapaxes(u_all[:, 1], 1, 2)
        return (u_col, u_row, fact_all[:2], blk_all[:2], blk_all[2:], fact_all[2:])

    batch_split = P('data', None)
    col_split = P(None, None, 'model')
    row_split = P(None, 'model', None)
    replicated = P()
    return jax.shard_map(
        shard_body,
        mesh=mesh,
        in_specs=(batch_split, batch_split, col_split, row_split, replicated, row_split, row_split, replicated, replicated, row_split, row_split, replicated),
        out_specs=(col_split, row_split, replicated, row_split, row_split, replicated),
        check_vma=False,
    )
```

```python
import functools
import math
import jax
import jax.numpy as jnp
from jax import lax
from jax.sharding import PartitionSpec as P
from jax.experimental import pallas as pl
from jax.experimental.pallas import tpu as pltpu

FACTOR_DECAY = 0.8
GELU_SCALE = math.sqrt(2.0 / math.pi)
GELU_CUBIC = 0.044715
EXACT = lax.Precision.HIGHEST
TN_DIMS = (((0,), (0,)), ((), ()))
NT_DIMS = (((1,), (1,)), ((), ()))
BOTH = ('model', 'data')


def gelu_value(pre_act):
    tanh_arg = GELU_SCALE * (pre_act + GELU_CUBIC * pre_act * pre_act * pre_act)
    return 0.5 * pre_act * (1.0 + jnp.tanh(tanh_arg))


def gelu_slope(pre_act):
    tanh_arg = GELU_SCALE * (pre_act + GELU_CUBIC * pre_act * pre_act * pre_act)
    tanh_val = jnp.tanh(tanh_arg)
    return 0.5 * (1.0 + tanh_val) + 0.5 * pre_act * (1.0 - tanh_val * tanh_val) * GELU_SCALE * (1.0 + 3.0 * GELU_CUBIC * pre_act * pre_act)


def activate(pre_act):
    return gelu_value(pre_act.astype(jnp.float32)).astype(jnp.bfloat16)


def back_gate(grad_act, pre_act):
    return (grad_act.astype(jnp.float32) * gelu_slope(pre_act.astype(jnp.float32))).astype(jnp.bfloat16)


def matmul(left_mat, right_mat):
    return jnp.dot(left_mat, right_mat, preferred_element_type=jnp.float32)


def matmul_tn(left_mat, right_mat):
    return lax.dot_general(left_mat, right_mat, TN_DIMS, preferred_element_type=jnp.float32)


def matmul_nt(left_mat, right_mat):
    return lax.dot_general(left_mat, right_mat, NT_DIMS, preferred_element_type=jnp.float32)


def exact_dot(left_mat, right_mat):
    return jnp.dot(left_mat, right_mat, precision=EXACT, preferred_element_type=jnp.float32)


MIB = 1024 * 1024
BLOCK = 256
HIDDEN = 1024
D_ROWS = 512
SYM_ROWS = 80
FULL_BASE = 512
BLOCK_BASE = 672
SHARE_ROWS = 800
LANES = 128
STRIP = 32
HALF_STRIP = 16
CORES = 8


def gram_kernel(x_ref, g1_ref, g2_ref, h1_ref, h2_ref, g3_ref, dy_ref, h3_ref, out_ref,
                act, stage, bstage, fstage, in_sem, out_sem, b_sem, f_sem):
    sources = [dy_ref, h3_ref, h2_ref, g3_ref, g2_ref, h1_ref, x_ref, g1_ref]
    slots = [3, 7, 2, 6, 1, 5, 0, 4]
    loads = [pltpu.make_async_copy(src, act.at[slot], in_sem.at[slot]) for src, slot in zip(sources, slots)]
    for load in loads:
        load.start()

    def out_copy(slot, dst):
        return pltpu.make_async_copy(stage.at[slot], dst, out_sem.at[slot])

    def f_copy(slot, n, which):
        return pltpu.make_async_copy(fstage.at[slot], out_ref.at[pl.ds(n * CORES, CORES), pl.ds(FULL_BASE + which * SYM_ROWS, SYM_ROWS)], f_sem.at[slot])

    for layer in (3, 2, 1, 0):
        pltpu.make_async_copy(x_ref, act.at[layer], in_sem.at[layer]).wait()
        pltpu.make_async_copy(x_ref, act.at[4 + layer], in_sem.at[4 + layer]).wait()

        def d_body(m, carry, layer=layer):
            slot = lax.rem(m, 2)
            cols = pl.ds(pl.multiple_of(m * BLOCK, BLOCK), BLOCK)
            right = act[4 + layer, :, cols]
            dst = out_ref.at[pl.ds(m * CORES + 2 * layer, 2), pl.ds(0, D_ROWS)]

            if layer == 3:
                @pl.when(m >= 2)
                def _():
                    out_copy(slot, dst).wait()
                    pltpu.make_async_copy(bstage.at[slot], out_ref.at[pl.ds(0, CORES), pl.ds(BLOCK_BASE, STRIP)], b_sem.at[slot]).wait()
            else:
                out_copy(slot, dst).wait()
                pltpu.make_async_copy(bstage.at[slot], out_ref.at[pl.ds(0, CORES), pl.ds(BLOCK_BASE, STRIP)], b_sem.at[slot]).wait()
            prod = lax.dot_general(act[layer], right, TN_DIMS, preferred_element_type=jnp.float32)
            stage[slot] = prod.reshape(2, D_ROWS, BLOCK)
            out_copy(slot, dst).start()
            blk = lax.dot_general(right, right, TN_DIMS, preferred_element_type=jnp.float32)
            bstage[slot] = blk.reshape(CORES, STRIP, BLOCK)
            pltpu.make_async_copy(bstage.at[slot], out_ref.at[pl.ds(m * CORES, CORES), pl.ds(BLOCK_BASE + STRIP * layer, STRIP)], b_sem.at[slot]).start()
            return carry

        lax.fori_loop(0, 4, d_body, 0)

        if layer in (2, 1):
            which = 0 if layer == 2 else 1

            def f_body(n, carry, layer=layer, which=which):
                slot = lax.rem(n, 2)
                if which == 0:
                    pl.when(n >= 2)(lambda: f_copy(slot, n, which).wait())
                else:
                    f_copy(slot, n, which).wait()
                put_sym(fstage.at[slot], sym_blocks(act.at[layer], n), False)
                f_copy(slot, n, which).start()
                return carry

            lax.fori_loop(0, 4, f_body, 0)
    for slot in range(2):
        f_copy(slot, 0, 0).wait()
        pltpu.make_async_copy(stage.at[slot], out_ref.at[pl.ds(0, 2), pl.ds(0, D_ROWS)], out_sem.at[slot]).wait()
        pltpu.make_async_copy(bstage.at[slot], out_ref.at[pl.ds(0, CORES), pl.ds(BLOCK_BASE, STRIP)], b_sem.at[slot]).wait()


def gram_call(x_loc, g_one, g_two, h_one, h_two, g_three, dy_loc, h_three):
    any_spec = pl.BlockSpec(memory_space=pl.ANY)
    return pl.pallas_call(
        gram_kernel,
        out_shape=jax.ShapeDtypeStruct((STRIP, SHARE_ROWS, BLOCK), jnp.float32),
        in_specs=[any_spec] * CORES,
        out_specs=any_spec,
        scratch_shapes=[
            pltpu.VMEM((CORES, HIDDEN, HIDDEN), jnp.bfloat16),
            pltpu.VMEM((2, 2, D_ROWS, BLOCK), jnp.float32),
            pltpu.VMEM((2, CORES, STRIP, BLOCK), jnp.float32),
            pltpu.VMEM((2, CORES, SYM_ROWS, BLOCK), jnp.float32),
            pltpu.SemaphoreType.DMA((CORES,)),
            pltpu.SemaphoreType.DMA((2,)),
            pltpu.SemaphoreType.DMA((2,)),
            pltpu.SemaphoreType.DMA((2,)),
        ],
        compiler_params=pltpu.CompilerParams(vmem_limit_bytes=48 * HIDDEN * HIDDEN),
        cost_estimate=pl.CostEstimate(flops=15_000_000_000, bytes_accessed=46_000_000, transcendentals=0),
        name='gram',
    )(x_loc, g_one, g_two, h_one, h_two, g_three, dy_loc, h_three)


MESH_ID = pl.DeviceIdType.MESH
CHUNK_ORDER = tuple((zd, h) for pair in ((0, 3), (1, 2)) for h in range(2) for zd in pair)


def torus_place():
    z = lax.axis_index('model')
    d = lax.axis_index('data')
    y = d // 4
    x = (d // 2) % 2
    c = d % 2
    near = {'x': (z, d + 2 - 4 * x), 'y': (z, d + 4 - CORES * y), 'c': (z, d + 1 - 2 * c), 'up': (z + 1, d), 'dn': (z - 1, d)}
    return z, y, x, c, near


def meet_neighbours(z, near):
    barrier = pltpu.get_barrier_semaphore()
    for side in ('x', 'y', 'c'):
        pl.semaphore_signal(barrier, inc=1, device_id=near[side], device_id_type=MESH_ID)

    @pl.when(z < 3)
    def _():
        pl.semaphore_signal(barrier, inc=1, device_id=near['up'], device_id_type=MESH_ID)

    @pl.when(z > 0)
    def _():
        pl.semaphore_signal(barrier, inc=1, device_id=near['dn'], device_id_type=MESH_ID)
    pl.semaphore_wait(barrier, 3 + (z + 3) // 4 + (6 - z) // 4)


def remote(src, dst, send_sem, recv_sem, where):
    return pltpu.make_async_remote_copy(src_ref=src, dst_ref=dst, send_sem=send_sem, recv_sem=recv_sem, device_id=where, device_id_type=MESH_ID)


def sym_blocks(left, n):
    def cols(at, size):
        return left[:, pl.ds(pl.multiple_of(at, LANES), size)]

    low = n % 2
    right = cols(n * BLOCK, BLOCK)
    pairs = ((right, right, STRIP), (cols((n + 1) % 4 * BLOCK, BLOCK), right, STRIP),
             (cols((low + 2) * BLOCK + n // 2 * LANES, LANES), cols(low * BLOCK, BLOCK), HALF_STRIP))
    return [lax.dot_general(a, b, TN_DIMS, preferred_element_type=jnp.float32).reshape(CORES, rows, BLOCK) for a, b, rows in pairs]


def put_sym(dst, blocks, more):
    at = 0
    for blk in blocks:
        span = pl.ds(at, blk.shape[1])
        dst[:, span] = dst[:, span] + blk if more else blk
        at += blk.shape[1]


def gather_kernel(plan, *refs):
    n = len(plan.items)
    pieces, refs = refs[:plan.n_in], refs[plan.n_in:]
    outs, refs = refs[:n], refs[n:]
    ends = len(plan.tokens) > 0
    if ends:
        ends_ref, refs = refs[0], refs[1:]
    lands, refs = refs[:n], refs[n:]
    if ends:
        tok, acc, tok_sem, acc_sem, *refs = refs
    load_sem, z_recv, x_recv, y_recv, d_recv, c_recv, up_send, dn_send, x_send, y_send, dy_send, dx_send, c_send, flush_sem = refs
    z, y, x, c, near = torus_place()

    def slot(ref, j, zs, yy, xx, cc):
        return plan.items[j].slot(ref, zs, 4 * yy + 2 * xx + cc)

    def view(j, zs, yy, xx, cc):
        return slot(lands[j], j, zs, yy, xx, cc)

    def half(j, zs, yy, xx, cc, which):
        return plan.items[j].half(lands[j], zs, 4 * yy + 2 * xx + cc, which)

    def flush(j, zs, yy, xx, cc, index):
        return pltpu.make_async_copy(view(j, zs, yy, xx, cc), slot(outs[j], j, zs, yy, xx, cc), flush_sem.at[j, zs, index])

    loads = [pltpu.make_async_copy(item.piece(pieces, z, 4 * y + 2 * x + c), view(j, z, y, x, c), load_sem.at[j]) for j, item in enumerate(plan.items)]
    for load in loads:
        load.start()

    def tok_load(t):
        src = pieces[plan.tokens[t // 4]].at[pl.ds(t % 4 * HIDDEN, HIDDEN)]
        return pltpu.make_async_copy(src, tok.at[t % 2], tok_sem.at[t % 2])

    def ends_out(mat):
        return pltpu.make_async_copy(acc.at[mat], ends_ref.at[mat], acc_sem.at[mat])

    def ends_step(t):
        tok_load(t).wait()
        put_sym(acc.at[t // 4], sym_blocks(tok.at[t % 2], z), t % 4 > 0)
        if t + 2 < CORES:
            tok_load(t + 2).start()
        if t % 4 == 3:
            ends_out(t // 4).start()

    todo = list(range(CORES)) if ends else []
    if ends:
        tok_load(0).start()
        tok_load(1).start()
    meet_neighbours(z, near)

    def side_copy(j, zs, side):
        send, recv = {'x': (x_send, x_recv), 'y': (y_send, y_recv), 'up': (up_send, z_recv), 'dn': (dn_send, z_recv)}[side]
        return remote(view(j, zs, y, x, c), view(j, zs, y, x, c), send.at[j, zs], recv.at[j, zs], near[side])

    def from_side(j, zs, side):
        yy, xx = (y, 1 - x) if side == 'x' else (1 - y, x)
        send, recv = {'x': (x_send, x_recv), 'y': (y_send, y_recv)}[side]
        return remote(view(j, zs, yy, xx, c), view(j, zs, yy, xx, c), send.at[j, zs], recv.at[j, zs], near[side])

    def dy_copy(j, zs):
        return remote(half(j, zs, y, 1 - x, c, 0), half(j, zs, y, 1 - x, c, 0), dy_send.at[j, zs], d_recv.at[j, zs, 0], near['y'])

    def dx_copy(j, zs):
        return remote(half(j, zs, 1 - y, x, c, 1), half(j, zs, 1 - y, x, c, 1), dx_send.at[j, zs], d_recv.at[j, zs, 1], near['x'])

    def kind_place(kind):
        return (y if kind < 2 else 1 - y), (x if kind % 2 == 0 else 1 - x)

    def c_copy(j, zs, kind):
        yy, xx = kind_place(kind)
        return remote(view(j, zs, yy, xx, c), view(j, zs, yy, xx, c), c_send.at[j, zs, kind], c_recv.at[j, zs, kind], near['c'])

    def share_core(j, zs, kind):
        yy, xx = kind_place(kind)
        c_copy(j, zs, kind).start()
        flush(j, zs, yy, xx, c, kind).start()

    def guard(off, body):
        if off == 0:
            body(z)
        elif off < 0:
            pl.when(z >= -off)(lambda: body(z + off))
        else:
            pl.when(z <= 3 - off)(lambda: body(z + off))

    def z_step(j, off):
        def body(zs):
            if off == 0:
                loads[j].wait()
            else:
                side_copy(j, zs, 'up').wait_recv()
            if off <= 0 and not plan.items[j].plane:
                pl.when(z < 3)(lambda: side_copy(j, zs, 'up').start())
            if off >= 0 and not plan.items[j].plane:
                pl.when(z > 0)(lambda: side_copy(j, zs, 'dn').start())
            side_copy(j, zs, 'x').start()
            side_copy(j, zs, 'y').start()
            share_core(j, zs, 0)
        guard(off, body)

    def xy_step(j, off):
        def body(zs):
            from_side(j, zs, 'x').wait_recv()
            dy_copy(j, zs).start()
            share_core(j, zs, 1)
            from_side(j, zs, 'y').wait_recv()
            dx_copy(j, zs).start()
            share_core(j, zs, 2)
        guard(off, body)

    def diag_step(j, off):
        def body(zs):
            for which in range(2):
                remote(half(j, zs, 1 - y, 1 - x, c, which), half(j, zs, 1 - y, 1 - x, c, which), dy_send.at[j, zs], d_recv.at[j, zs, which], near['y']).wait_recv()
            share_core(j, zs, 3)
        guard(off, body)

    def core_step(j, off):
        def body(zs):
            for kind in range(4):
                yy, xx = kind_place(kind)
                remote(view(j, zs, yy, xx, 1 - c), view(j, zs, yy, xx, 1 - c), c_send.at[j, zs, kind], c_recv.at[j, zs, kind], near['c']).wait_recv()
                flush(j, zs, yy, xx, 1 - c, 4 + kind).start()
        guard(off, body)

    def last_step(j, off):
        def body(zs):
            for kind in range(4):
                yy, xx = kind_place(kind)
                c_copy(j, zs, kind).wait_send()
                flush(j, zs, yy, xx, c, kind).wait()
                flush(j, zs, yy, xx, 1 - c, 4 + kind).wait()
            side_copy(j, zs, 'x').wait_send()
            side_copy(j, zs, 'y').wait_send()
            dy_copy(j, zs).wait_send()
            dx_copy(j, zs).wait_send()
            if off <= 0 and not plan.items[j].plane:
                pl.when(z < 3)(lambda: side_copy(j, zs, 'up').wait_send())
            if off >= 0 and not plan.items[j].plane:
                pl.when(z > 0)(lambda: side_copy(j, zs, 'dn').wait_send())
        guard(off, body)

    waves = [[(j, 0) for j in plan.order]]
    for far in range(1, 4):
        waves.append([(j, sign * far) for j in plan.order if not plan.items[j].plane for sign in (-1, 1)])
    for step in range(7):
        for func, lag in ((z_step, 0), (xy_step, 1), (diag_step, 2), (core_step, 3)):
            if 0 <= step - lag < 4:
                for j, off in waves[step - lag]:
                    func(j, off)
                if todo:
                    ends_step(todo.pop(0))
    for t in todo:
        ends_step(t)
    if ends:
        ends_out(0).wait()
        ends_out(1).wait()
    for wave in waves:
        for j, off in wave:
            last_step(j, off)


class Item:
    def __init__(self, shape, dtype, piece, slot, half, plane=False):
        self.shape, self.dtype, self.piece, self.slot, self.half, self.plane = shape, dtype, piece, slot, half, plane


class Plan:
    def __init__(self, n_in, items, order, tokens):
        self.n_in, self.items, self.order, self.tokens = n_in, items, order, tokens


def gather_call(args, items, order, collective_id, name, tokens=()):
    n = len(items)
    dma = pltpu.SemaphoreType.DMA
    size = sum(math.prod(item.shape) * jnp.dtype(item.dtype).itemsize for item in items)
    hbm = pl.BlockSpec(memory_space=pltpu.HBM)
    flat = dma((n, 4))
    shapes = [jax.ShapeDtypeStruct(item.shape, item.dtype) for item in items]
    extra = []
    if tokens:
        part = (2, CORES, SYM_ROWS, BLOCK)
        shapes.append(jax.ShapeDtypeStruct(part, jnp.float32))
        extra = [pltpu.VMEM((2, HIDDEN, HIDDEN), jnp.bfloat16), pltpu.VMEM(part, jnp.float32), dma((2,)), dma((2,))]
    return pl.pallas_call(
        functools.partial(gather_kernel, Plan(len(args), items, order, tokens)),
        out_shape=shapes,
        in_specs=[hbm] * len(args),
        out_specs=[hbm] * len(shapes),
        scratch_shapes=[pltpu.VMEM(item.shape, item.dtype) for item in items] + extra
        + [dma((n,)), flat, flat, flat, dma((n, 4, 2)), dma((n, 4, 4)), flat, flat, flat, flat, flat, flat, dma((n, 4, 4)), dma((n, 4, CORES))],
        compiler_params=pltpu.CompilerParams(collective_id=collective_id, has_side_effects=True, vmem_limit_bytes=size + HALF_STRIP * MIB),
        cost_estimate=pl.CostEstimate(flops=50_000_000_000, bytes_accessed=size, transcendentals=0),
        name=name,
    )(*args)


def col_slot(ref, zs, d):
    return ref.at[pl.ds(d * LANES, LANES), pl.ds(zs * BLOCK, BLOCK)]


def col_half(ref, zs, d, which):
    return ref.at[pl.ds(d * LANES + which * 64, 64), pl.ds(zs * BLOCK, BLOCK)]


def row_slot(ref, zs, d):
    return ref.at[pl.ds((zs * CORES + d) * STRIP, STRIP)]


def row_half(ref, zs, d, which):
    return ref.at[pl.ds((zs * CORES + d) * STRIP + which * HALF_STRIP, HALF_STRIP)]


def gather_weights(w_col, w_row, x_tokens, dy_tokens):
    shape = (HIDDEN, HIDDEN)
    items = [Item(shape, w_col.dtype, lambda refs, z, d, i=i: refs[0].at[i, pl.ds(d * LANES, LANES)], col_slot, col_half) for i in range(2)]
    items += [Item(shape, w_row.dtype, lambda refs, z, d, i=i: refs[1].at[i, pl.ds(d * STRIP, STRIP)], row_slot, row_half) for i in range(2)]
    return gather_call((w_col, w_row, x_tokens, dy_tokens), items, (0, 3, 2, 1), 1, 'weights', (2, 3))


def gather_results(facts, u_half, blocks):
    items = [
        Item((STRIP, 4, SYM_ROWS, BLOCK), facts.dtype, lambda refs, z, d: refs[0],
             lambda ref, zs, d: ref.at[zs * CORES + d], lambda ref, zs, d, which: ref.at[zs * CORES + d, pl.ds(2 * which, 2)]),
        Item((CORES, D_ROWS, BLOCK), facts.dtype, lambda refs, z, d: refs[1],
             lambda ref, zs, d: ref.at[d], lambda ref, zs, d, which: ref.at[d, pl.ds(which * BLOCK, BLOCK)], True),
        Item((4, BLOCK, BLOCK), facts.dtype, lambda refs, z, d: refs[2],
             lambda ref, zs, d: ref.at[:, pl.ds(d * STRIP, STRIP)], lambda ref, zs, d, which: ref.at[pl.ds(2 * which, 2), pl.ds(d * STRIP, STRIP)], True),
    ]
    return gather_call((facts, u_half, blocks), items, (1, 2, 0), 3, 'results')


def add_into(dst, src, rows):
    step = max(n for n in range(CORES, 65, CORES) if rows % n == 0)

    def body(i, carry):
        span = pl.ds(pl.multiple_of(i * step, CORES), step)
        dst[span, :] = dst[span, :] + src[span, :]
        return carry

    lax.fori_loop(0, rows // step, body, 0)


def scatter_kernel(rows, parts_ref, ends_ref, share_ref, eshare_ref, grad_ref, own, mate, one_x, one_y, two_x, two_y, up_buf, dn_buf,
                   eown, emate, eone, etwo, gland, e_sem, emate_sem, eone_sem, etwo_sem, g_sem, out2_sem,
                   own_sem, mate_send, mate_recv, x1_send, x1_recv, y1_send, y1_recv, x2_send, x2_recv, y2_send, y2_recv,
                   up_send, up_recv, dn_send, dn_recv, out_sem):
    z, y, x, c, near = torus_place()
    sub = rows // 4
    eload = pltpu.make_async_copy(ends_ref.at[:, :, :, c], eown, e_sem.at[0])
    eload.start()
    loads = {}
    for k, (zd, h) in enumerate(CHUNK_ORDER):
        loads[k] = []
        for col in range(2):
            span = pl.ds(col * 2 * sub + h * sub, sub)
            load = pltpu.make_async_copy(parts_ref.at[zd, :, :, c, span], own.at[zd, :, :, span], own_sem.at[k, col])
            load.start()
            loads[k].append(load)
    meet_neighbours(z, near)
    ematec = remote(ends_ref.at[:, :, :, 1 - c], emate, emate_sem.at[0], emate_sem.at[1], near['c'])
    ematec.start()
    eones = (remote(eown.at[0, :, 1 - x], eone.at[0], eone_sem.at[0], eone_sem.at[1], near['x']),
             remote(eown.at[1, 1 - y], eone.at[1], eone_sem.at[2], eone_sem.at[3], near['y']))
    etwos = (remote(eown.at[0, 1 - y, x], etwo.at[0], etwo_sem.at[0], etwo_sem.at[1], near['y']),
             remote(eown.at[1, y, 1 - x], etwo.at[1], etwo_sem.at[2], etwo_sem.at[3], near['x']))
    mates = {}
    for k, (zd, h) in enumerate(CHUNK_ORDER):
        mates[k] = []
        for col in range(2):
            span = pl.ds(col * 2 * sub + h * sub, sub)
            copy = remote(parts_ref.at[zd, :, :, 1 - c, span], mate.at[zd, :, :, span], mate_send.at[k, col], mate_recv.at[k, col], near['c'])
            copy.start()
            mates[k].append(copy)

    def spans(h):
        return pl.ds(h * sub, sub), pl.ds(2 * sub + h * sub, sub)

    def one_copies(k):
        zd, h = CHUNK_ORDER[k]
        first, second = spans(h)
        piece = pl.ds(h * sub, sub)
        return (remote(own.at[zd, :, 1 - x, first], one_x.at[zd, :, piece], x1_send.at[k], x1_recv.at[k], near['x']),
                remote(own.at[zd, 1 - y, :, second], one_y.at[zd, :, piece], y1_send.at[k], y1_recv.at[k], near['y']))

    def two_copies(k):
        zd, h = CHUNK_ORDER[k]
        first, second = spans(h)
        piece = pl.ds(h * sub, sub)
        return (remote(own.at[zd, 1 - y, x, first], two_y.at[zd, piece], y2_send.at[k], y2_recv.at[k], near['y']),
                remote(own.at[zd, y, 1 - x, second], two_x.at[zd, piece], x2_send.at[k], x2_recv.at[k], near['x']))

    def z_copies(k):
        zd, h = CHUNK_ORDER[k]
        out = []
        for col, span in enumerate(spans(h)):
            out.append((remote(own.at[zd, y, x, span], up_buf.at[zd, span], dn_send.at[k, col], up_recv.at[k, col], near['dn']),
                        remote(own.at[zd, y, x, span], dn_buf.at[zd, span], up_send.at[k, col], dn_recv.at[k, col], near['up'])))
        return out

    def step_a(k):
        zd, h = CHUNK_ORDER[k]
        first, second = spans(h)
        ones = one_copies(k)
        loads[k][0].wait()
        mates[k][0].wait_recv()
        for yy in range(2):
            add_into(own.at[zd, yy, 1 - x, first], mate.at[zd, yy, 1 - x, first], sub)
        ones[0].start()
        loads[k][1].wait()
        mates[k][1].wait_recv()
        for xx in range(2):
            add_into(own.at[zd, 1 - y, xx, second], mate.at[zd, 1 - y, xx, second], sub)
        ones[1].start()
        for yy in range(2):
            add_into(own.at[zd, yy, x, first], mate.at[zd, yy, x, first], sub)
        for xx in range(2):
            add_into(own.at[zd, y, xx, second], mate.at[zd, y, xx, second], sub)

    def step_b(k):
        zd, h = CHUNK_ORDER[k]
        first, second = spans(h)
        piece = pl.ds(h * sub, sub)
        ones, twos = one_copies(k), two_copies(k)
        ones[0].wait_recv()
        add_into(own.at[zd, 1 - y, x, first], one_x.at[zd, 1 - y, piece], sub)
        twos[0].start()
        ones[1].wait_recv()
        add_into(own.at[zd, y, 1 - x, second], one_y.at[zd, 1 - x, piece], sub)
        twos[1].start()
        add_into(own.at[zd, y, x, first], one_x.at[zd, y, piece], sub)
        add_into(own.at[zd, y, x, second], one_y.at[zd, x, piece], sub)

    def step_c(k):
        zd, h = CHUNK_ORDER[k]
        first, second = spans(h)
        piece = pl.ds(h * sub, sub)
        twos = two_copies(k)
        zcs = z_copies(k)
        for col, (copy, buf, span) in enumerate(((twos[0], two_y, first), (twos[1], two_x, second))):
            copy.wait_recv()
            add_into(own.at[zd, y, x, span], buf.at[zd, piece], sub)

            @pl.when((z < 3) & (z >= zd))
            def _(col=col, span=span):
                zcs[col][0].wait_recv()
                add_into(own.at[zd, y, x, span], up_buf.at[zd, span], sub)

            @pl.when((z > 0) & (z <= zd))
            def _(col=col, span=span):
                zcs[col][1].wait_recv()
                add_into(own.at[zd, y, x, span], dn_buf.at[zd, span], sub)
            pl.when(z > zd)(lambda: zcs[col][0].start())
            pl.when(z < zd)(lambda: zcs[col][1].start())

            @pl.when(z == zd)
            def _(col=col, span=span):
                pltpu.make_async_copy(own.at[zd, y, x, span], share_ref.at[span], out_sem.at[h, col]).start()

    def ends_a():
        eload.wait()
        ematec.wait_recv()
        for mat in range(2):
            for yy in range(2):
                for xx in range(2):
                    add_into(eown.at[mat, yy, xx], emate.at[mat, yy, xx], SYM_ROWS)
            eones[mat].start()

    def ends_b():
        eones[0].wait_recv()
        for yy in range(2):
            add_into(eown.at[0, yy, x], eone.at[0, yy], SYM_ROWS)
        etwos[0].start()
        eones[1].wait_recv()
        for xx in range(2):
            add_into(eown.at[1, y, xx], eone.at[1, xx], SYM_ROWS)
        etwos[1].start()

    def ends_c():
        for mat in range(2):
            etwos[mat].wait_recv()
            add_into(eown.at[mat, y, x], etwo.at[mat], SYM_ROWS)
            pltpu.make_async_copy(eown.at[mat, y, x], eshare_ref.at[mat], out2_sem.at[mat]).start()

    n = len(CHUNK_ORDER)
    ends_a()
    for step in range(n + 3):
        if step == 1:
            ends_b()
        if step == 2:
            ends_c()
        if step < n:
            step_a(step)
        if 0 <= step - 1 < n:
            step_b(step - 1)
        if 0 <= step - 3 < n:
            step_c(step - 3)
    mine = own.at[z, y, x, pl.ds(0, D_ROWS)]
    gcopy = remote(mine, gland, g_sem.at[0], g_sem.at[1], near['c'])
    gcopy.start()
    gout = pltpu.make_async_copy(mine, grad_ref.at[c], out2_sem.at[2])
    gout.start()
    gcopy.wait_recv()
    gmate = pltpu.make_async_copy(gland, grad_ref.at[1 - c], out2_sem.at[3])
    gmate.start()
    for copy in (ematec, gcopy) + eones + etwos:
        copy.wait_send()
    for k, (zd, h) in enumerate(CHUNK_ORDER):
        for copy in mates[k] + list(one_copies(k)) + list(two_copies(k)):
            copy.wait_send()
        for col, (down, up) in enumerate(z_copies(k)):
            pl.when(z > zd)(lambda: down.wait_send())
            pl.when(z < zd)(lambda: up.wait_send())
    for h in range(2):
        for col in range(2):
            span = spans(h)[col]
            pltpu.make_async_copy(own.at[0, y, x, span], share_ref.at[span], out_sem.at[h, col]).wait()
    for mat in range(2):
        pltpu.make_async_copy(eown.at[mat, y, x], eshare_ref.at[mat], out2_sem.at[mat]).wait()
    gout.wait()
    gmate.wait()


def scatter_call(parts, ends, collective_id, name):
    rows = parts.shape[-2]
    half = rows // 2
    f32 = jnp.float32
    dma = pltpu.SemaphoreType.DMA
    n = len(CHUNK_ORDER)
    whole = pltpu.VMEM((4, 2, 2, rows, BLOCK), f32)
    one_buf = pltpu.VMEM((4, 2, half, BLOCK), f32)
    two_buf = pltpu.VMEM((4, half, BLOCK), f32)
    z_buf = pltpu.VMEM((4, rows, BLOCK), f32)
    e_buf = pltpu.VMEM((2, 2, 2, SYM_ROWS, BLOCK), f32)
    hbm = pl.BlockSpec(memory_space=pltpu.HBM)
    return pl.pallas_call(
        functools.partial(scatter_kernel, rows),
        out_shape=[jax.ShapeDtypeStruct((rows, BLOCK), f32), jax.ShapeDtypeStruct((2, SYM_ROWS, BLOCK), f32), jax.ShapeDtypeStruct((2, D_ROWS, BLOCK), f32)],
        in_specs=[hbm] * 2,
        out_specs=[hbm] * 3,
        scratch_shapes=[whole, whole, one_buf, one_buf, two_buf, two_buf, z_buf, z_buf,
                        e_buf, e_buf, pltpu.VMEM((2, 2, SYM_ROWS, BLOCK), f32), pltpu.VMEM((2, SYM_ROWS, BLOCK), f32), pltpu.VMEM((D_ROWS, BLOCK), f32),
                        dma((1,)), dma((2,)), dma((4,)), dma((4,)), dma((2,)), dma((4,))]
        + [dma((n, 2))] * 3 + [dma((n,))] * CORES + [dma((n, 2))] * 4 + [dma((2, 2))],
        compiler_params=pltpu.CompilerParams(collective_id=collective_id, has_side_effects=True, vmem_limit_bytes=60 * MIB),
        cost_estimate=pl.CostEstimate(flops=120_000_000_000, bytes_accessed=60 * MIB, transcendentals=0),
        name=name,
    )(parts.reshape(4, 2, 2, 2, rows, BLOCK), ends.reshape(2, 2, 2, 2, SYM_ROWS, BLOCK))


def mirror_kernel(in_ref, a_ref, s_ref):
    def block(i, j, mat):
        def take(plane, at, size):
            return in_ref[plane, :, mat, pl.ds(at, size)].reshape(CORES * size, BLOCK)

        if i == j:
            return take(j, 0, STRIP)
        if i == (j + 1) % 4:
            return take(j, STRIP, STRIP)
        if j == (i + 1) % 4:
            return take(i, STRIP, STRIP).T
        low = min(i, j)
        both = jnp.concatenate([take(low, 64, HALF_STRIP), take(low + 2, 64, HALF_STRIP)], axis=0)
        return both if i > j else both.T

    for i in range(4):
        @pl.when(pl.program_id(1) == i)
        def _(i=i):
            for mat, out in enumerate((a_ref, s_ref)):
                for j in range(4):
                    out[0, :, pl.ds(j * BLOCK, BLOCK)] = block(i, j, mat)


def mirror_call(facts):
    full = jax.ShapeDtypeStruct((2, HIDDEN, HIDDEN), facts.dtype)
    out_spec = pl.BlockSpec((1, BLOCK, HIDDEN), lambda k, i: (k, i, 0))
    return pl.pallas_call(
        mirror_kernel,
        grid=(2, 4),
        out_shape=[full, full],
        in_specs=[pl.BlockSpec((4, CORES, 2, SYM_ROWS, BLOCK), lambda k, i: (0, 0, k, 0, 0))],
        out_specs=[out_spec, out_spec],
        compiler_params=pltpu.CompilerParams(vmem_limit_bytes=STRIP * MIB),
        cost_estimate=pl.CostEstimate(flops=10_000_000_000, bytes_accessed=26 * MIB, transcendentals=0),
        name='mirror',
    )(facts.reshape(4, CORES, 4, SYM_ROWS, BLOCK))


def solution(mesh):
    data_ways = mesh.shape['data']
    model_ways = mesh.shape['model']

    def shard_body(x_tokens, dy_tokens, w_col, w_row, a_old_col, s_old_col, a_old_row, s_old_row, a_inv_col, s_inv_col, a_inv_row, s_inv_row):
        model_id = lax.axis_index('model')
        data_id = lax.axis_index('data')
        inv_rows = 1.0 / (x_tokens.shape[0] * data_ways)
        w_one, w_three, w_two, w_four, ends = gather_weights(w_col, w_row, x_tokens, dy_tokens)
        rows_dev = x_tokens.shape[0] // model_ways
        x_loc = lax.dynamic_slice(x_tokens, (rows_dev * model_id, 0), (rows_dev, HIDDEN))
        dy_loc = lax.dynamic_slice(dy_tokens, (rows_dev * model_id, 0), (rows_dev, HIDDEN))
        z_one = matmul(x_loc, w_one).astype(jnp.bfloat16)
        h_one = activate(z_one)
        z_two = matmul(h_one, w_two).astype(jnp.bfloat16)
        h_two = activate(z_two)
        z_three = matmul(h_two, w_three).astype(jnp.bfloat16)
        h_three = activate(z_three)
        g_three = back_gate(matmul_nt(dy_loc, w_four).astype(jnp.bfloat16), z_three)
        g_two = back_gate(matmul_nt(g_three, w_three).astype(jnp.bfloat16), z_two)
        g_one = back_gate(matmul_nt(g_two, w_two).astype(jnp.bfloat16), z_one)
        parts = gram_call(x_loc, g_one, g_two, h_one, h_two, g_three, dy_loc, h_three)
        share, eshare, grad_mat = scatter_call(parts, ends, 2, 'sums')
        keep = 1.0 - FACTOR_DECAY
        low = lax.rem(model_id, 2)
        spots = ((model_id * BLOCK + STRIP * data_id, model_id * BLOCK, STRIP),
                 (lax.rem(model_id + 1, 4) * BLOCK + STRIP * data_id, model_id * BLOCK, STRIP),
                 ((low + 2) * BLOCK + model_id // 2 * LANES + HALF_STRIP * data_id, low * BLOCK, HALF_STRIP))
        olds = [jnp.concatenate([lax.dynamic_slice(old, (0, at, col), (2, size, BLOCK)) for at, col, size in spots], axis=1) for old in (a_old_col, s_old_row)]
        mids = share[FULL_BASE:BLOCK_BASE].reshape(2, SYM_ROWS, BLOCK)
        sums = jnp.stack([eshare[0], mids[1], mids[0], eshare[1]])
        facts = FACTOR_DECAY * jnp.stack(olds, axis=1).reshape(4, SYM_ROWS, BLOCK) + keep * inv_rows * sums
        grad_mat = grad_mat.reshape(HIDDEN, BLOCK) * inv_rows
        layer_id = data_id // 2
        stack_id = layer_id // 2
        is_col = lax.rem(layer_id, 2) == 0
        half_at = lax.rem(data_id, 2) * D_ROWS
        full_inv = jnp.where(is_col, *[lax.dynamic_slice(inv, (stack_id, half_at, 0), (1, D_ROWS, HIDDEN))[0] for inv in (a_inv_col, s_inv_row)])
        block_inv = jnp.where(is_col, *[lax.dynamic_slice(inv, (stack_id, 0, 0), (1, BLOCK, BLOCK))[0] for inv in (s_inv_col, a_inv_row)])
        u_half = exact_dot(exact_dot(full_inv, grad_mat), block_inv)
        old_blocks = jnp.concatenate([lax.dynamic_slice(old, (0, STRIP * data_id, 0), (2, STRIP, BLOCK)) for old in (s_old_col, a_old_row)])
        new_blocks = jnp.swapaxes(share[BLOCK_BASE:].reshape(2, 2, STRIP, BLOCK), 0, 1).reshape(4, STRIP, BLOCK)
        blocks = FACTOR_DECAY * old_blocks + keep * inv_rows * new_blocks
        fact_all, u_all, blk_all = gather_results(facts, u_half, blocks)
        a_new_col, s_new_row = mirror_call(fact_all)
        u_all = u_all.reshape(2, 2, HIDDEN, BLOCK)
        u_col = u_all[:, 0]
        u_row = jnp.swapaxes(u_all[:, 1], 1, 2)
        return (u_col, u_row, a_new_col, blk_all[:2], blk_all[2:], s_new_row)

    batch_split = P('data', None)
    col_split = P(None, None, 'model')
    row_split = P(None, 'model', None)
    replicated = P()
    return jax.shard_map(
        shard_body,
        mesh=mesh,
        in_specs=(batch_split, batch_split, col_split, row_split, replicated, row_split, row_split, replicated, replicated, row_split, row_split, replicated),
        out_specs=(col_split, row_split, replicated, row_split, row_split, replicated),
        check_vma=False,
    )
```

```python
import functools
import math
import jax
import jax.numpy as jnp
from jax import lax
from jax.sharding import PartitionSpec as P
from jax.experimental import pallas as pl
from jax.experimental.pallas import tpu as pltpu

FACTOR_DECAY = 0.8
GELU_SCALE = math.sqrt(2.0 / math.pi)
GELU_CUBIC = 0.044715
EXACT = lax.Precision.HIGHEST
TN_DIMS = (((0,), (0,)), ((), ()))
NT_DIMS = (((1,), (1,)), ((), ()))
BOTH = ('model', 'data')


def gelu_value(pre_act):
    tanh_arg = GELU_SCALE * (pre_act + GELU_CUBIC * pre_act * pre_act * pre_act)
    return 0.5 * pre_act * (1.0 + jnp.tanh(tanh_arg))


def gelu_slope(pre_act):
    tanh_arg = GELU_SCALE * (pre_act + GELU_CUBIC * pre_act * pre_act * pre_act)
    tanh_val = jnp.tanh(tanh_arg)
    return 0.5 * (1.0 + tanh_val) + 0.5 * pre_act * (1.0 - tanh_val * tanh_val) * GELU_SCALE * (1.0 + 3.0 * GELU_CUBIC * pre_act * pre_act)


def activate(pre_act):
    return gelu_value(pre_act.astype(jnp.float32)).astype(jnp.bfloat16)


def back_gate(grad_act, pre_act):
    return (grad_act.astype(jnp.float32) * gelu_slope(pre_act.astype(jnp.float32))).astype(jnp.bfloat16)


def matmul(left_mat, right_mat):
    return jnp.dot(left_mat, right_mat, preferred_element_type=jnp.float32)


def matmul_tn(left_mat, right_mat):
    return lax.dot_general(left_mat, right_mat, TN_DIMS, preferred_element_type=jnp.float32)


def matmul_nt(left_mat, right_mat):
    return lax.dot_general(left_mat, right_mat, NT_DIMS, preferred_element_type=jnp.float32)


def exact_dot(left_mat, right_mat):
    return jnp.dot(left_mat, right_mat, precision=EXACT, preferred_element_type=jnp.float32)


MIB = 1024 * 1024
BLOCK = 256
HIDDEN = 1024
D_ROWS = 512
SYM_ROWS = 80
FULL_BASE = 512
BLOCK_BASE = 672
SHARE_ROWS = 800
LANES = 128
STRIP = 32
HALF_STRIP = 16
CORES = 8


def gram_kernel(x_ref, g1_ref, g2_ref, h1_ref, h2_ref, g3_ref, dy_ref, h3_ref, out_ref,
                act, stage, bstage, fstage, in_sem, out_sem, b_sem, f_sem):
    sources = [dy_ref, h3_ref, h2_ref, g3_ref, g2_ref, h1_ref, x_ref, g1_ref]
    slots = [3, 7, 2, 6, 1, 5, 0, 4]
    loads = [pltpu.make_async_copy(src, act.at[slot], in_sem.at[slot]) for src, slot in zip(sources, slots)]
    for load in loads:
        load.start()

    def out_copy(slot, dst):
        return pltpu.make_async_copy(stage.at[slot], dst, out_sem.at[slot])

    def f_copy(slot, n, which):
        return pltpu.make_async_copy(fstage.at[slot], out_ref.at[pl.ds(n * CORES, CORES), pl.ds(FULL_BASE + which * SYM_ROWS, SYM_ROWS)], f_sem.at[slot])

    for layer in (3, 2, 1, 0):
        pltpu.make_async_copy(x_ref, act.at[layer], in_sem.at[layer]).wait()
        pltpu.make_async_copy(x_ref, act.at[4 + layer], in_sem.at[4 + layer]).wait()

        def d_body(m, carry, layer=layer):
            slot = lax.rem(m, 2)
            cols = pl.ds(pl.multiple_of(m * BLOCK, BLOCK), BLOCK)
            right = act[4 + layer, :, cols]
            dst = out_ref.at[pl.ds(m * CORES + 2 * layer, 2), pl.ds(0, D_ROWS)]

            if layer == 3:
                @pl.when(m >= 2)
                def _():
                    out_copy(slot, dst).wait()
                    pltpu.make_async_copy(bstage.at[slot], out_ref.at[pl.ds(0, CORES), pl.ds(BLOCK_BASE, STRIP)], b_sem.at[slot]).wait()
            else:
                out_copy(slot, dst).wait()
                pltpu.make_async_copy(bstage.at[slot], out_ref.at[pl.ds(0, CORES), pl.ds(BLOCK_BASE, STRIP)], b_sem.at[slot]).wait()
            right_t = right.T
            prod = matmul(right_t, act[layer])
            for q in range(4):
                stage[slot, q // 2, pl.ds(q % 2 * BLOCK, BLOCK)] = prod[:, q * BLOCK:(q + 1) * BLOCK]
            out_copy(slot, dst).start()
            blk = matmul(right_t, right)
            bstage[slot] = blk.reshape(CORES, STRIP, BLOCK)
            pltpu.make_async_copy(bstage.at[slot], out_ref.at[pl.ds(m * CORES, CORES), pl.ds(BLOCK_BASE + STRIP * layer, STRIP)], b_sem.at[slot]).start()
            return carry

        lax.fori_loop(0, 4, d_body, 0)

        if layer in (2, 1):
            which = 0 if layer == 2 else 1

            def f_body(n, carry, layer=layer, which=which):
                slot = lax.rem(n, 2)
                if which == 0:
                    pl.when(n >= 2)(lambda: f_copy(slot, n, which).wait())
                else:
                    f_copy(slot, n, which).wait()
                put_sym(fstage.at[slot], sym_blocks(act.at[layer], n), False)
                f_copy(slot, n, which).start()
                return carry

            lax.fori_loop(0, 4, f_body, 0)
    for slot in range(2):
        f_copy(slot, 0, 0).wait()
        pltpu.make_async_copy(stage.at[slot], out_ref.at[pl.ds(0, 2), pl.ds(0, D_ROWS)], out_sem.at[slot]).wait()
        pltpu.make_async_copy(bstage.at[slot], out_ref.at[pl.ds(0, CORES), pl.ds(BLOCK_BASE, STRIP)], b_sem.at[slot]).wait()


def gram_call(x_loc, g_one, g_two, h_one, h_two, g_three, dy_loc, h_three):
    any_spec = pl.BlockSpec(memory_space=pl.ANY)
    return pl.pallas_call(
        gram_kernel,
        out_shape=jax.ShapeDtypeStruct((STRIP, SHARE_ROWS, BLOCK), jnp.float32),
        in_specs=[any_spec] * CORES,
        out_specs=any_spec,
        scratch_shapes=[
            pltpu.VMEM((CORES, HIDDEN, HIDDEN), jnp.bfloat16),
            pltpu.VMEM((2, 2, D_ROWS, BLOCK), jnp.float32),
            pltpu.VMEM((2, CORES, STRIP, BLOCK), jnp.float32),
            pltpu.VMEM((2, CORES, SYM_ROWS, BLOCK), jnp.float32),
            pltpu.SemaphoreType.DMA((CORES,)),
            pltpu.SemaphoreType.DMA((2,)),
            pltpu.SemaphoreType.DMA((2,)),
            pltpu.SemaphoreType.DMA((2,)),
        ],
        compiler_params=pltpu.CompilerParams(vmem_limit_bytes=48 * HIDDEN * HIDDEN),
        cost_estimate=pl.CostEstimate(flops=15_000_000_000, bytes_accessed=46_000_000, transcendentals=0),
        name='gram',
    )(x_loc, g_one, g_two, h_one, h_two, g_three, dy_loc, h_three)


MESH_ID = pl.DeviceIdType.MESH
CHUNK_ORDER = tuple((zd, h) for pair in ((0, 3), (1, 2)) for h in range(2) for zd in pair)


def torus_place():
    z = lax.axis_index('model')
    d = lax.axis_index('data')
    y = d // 4
    x = (d // 2) % 2
    c = d % 2
    near = {'x': (z, d + 2 - 4 * x), 'y': (z, d + 4 - CORES * y), 'c': (z, d + 1 - 2 * c), 'up': (z + 1, d), 'dn': (z - 1, d)}
    return z, y, x, c, near


def meet_neighbours(z, near):
    barrier = pltpu.get_barrier_semaphore()
    for side in ('x', 'y', 'c'):
        pl.semaphore_signal(barrier, inc=1, device_id=near[side], device_id_type=MESH_ID)

    @pl.when(z < 3)
    def _():
        pl.semaphore_signal(barrier, inc=1, device_id=near['up'], device_id_type=MESH_ID)

    @pl.when(z > 0)
    def _():
        pl.semaphore_signal(barrier, inc=1, device_id=near['dn'], device_id_type=MESH_ID)
    pl.semaphore_wait(barrier, 3 + (z + 3) // 4 + (6 - z) // 4)


def remote(src, dst, send_sem, recv_sem, where):
    return pltpu.make_async_remote_copy(src_ref=src, dst_ref=dst, send_sem=send_sem, recv_sem=recv_sem, device_id=where, device_id_type=MESH_ID)


def sym_blocks(left, n):
    def cols(at, size):
        return left[:, pl.ds(pl.multiple_of(at, LANES), size)]

    low = n % 2
    right = cols(n * BLOCK, BLOCK)
    pairs = ((right, right, STRIP), (cols((n + 1) % 4 * BLOCK, BLOCK), right, STRIP),
             (cols((low + 2) * BLOCK + n // 2 * LANES, LANES), cols(low * BLOCK, BLOCK), HALF_STRIP))
    return [lax.dot_general(a, b, TN_DIMS, preferred_element_type=jnp.float32).reshape(CORES, rows, BLOCK) for a, b, rows in pairs]


def put_sym(dst, blocks, more):
    at = 0
    for blk in blocks:
        span = pl.ds(at, blk.shape[1])
        dst[:, span] = dst[:, span] + blk if more else blk
        at += blk.shape[1]


def gather_kernel(plan, *refs):
    n = len(plan.items)
    pieces, refs = refs[:plan.n_in], refs[plan.n_in:]
    outs, refs = refs[:n], refs[n:]
    lands, refs = refs[:n], refs[n:]
    load_sem, z_recv, x_recv, y_recv, d_recv, c_recv, up_send, dn_send, x_send, y_send, dy_send, dx_send, c_send, flush_sem = refs
    z, y, x, c, near = torus_place()

    def slot(ref, j, zs, yy, xx, cc):
        return plan.items[j].slot(ref, zs, 4 * yy + 2 * xx + cc)

    def view(j, zs, yy, xx, cc):
        return slot(lands[j], j, zs, yy, xx, cc)

    def half(j, zs, yy, xx, cc, which):
        return plan.items[j].half(lands[j], zs, 4 * yy + 2 * xx + cc, which)

    def flush(j, zs, yy, xx, cc, index):
        return pltpu.make_async_copy(view(j, zs, yy, xx, cc), slot(outs[j], j, zs, yy, xx, cc), flush_sem.at[j, zs, index])

    loads = [pltpu.make_async_copy(item.piece(pieces, z, 4 * y + 2 * x + c), view(j, z, y, x, c), load_sem.at[j]) for j, item in enumerate(plan.items)]
    for load in loads:
        load.start()

    meet_neighbours(z, near)

    def side_copy(j, zs, side):
        send, recv = {'x': (x_send, x_recv), 'y': (y_send, y_recv), 'up': (up_send, z_recv), 'dn': (dn_send, z_recv)}[side]
        return remote(view(j, zs, y, x, c), view(j, zs, y, x, c), send.at[j, zs], recv.at[j, zs], near[side])

    def from_side(j, zs, side):
        yy, xx = (y, 1 - x) if side == 'x' else (1 - y, x)
        send, recv = {'x': (x_send, x_recv), 'y': (y_send, y_recv)}[side]
        return remote(view(j, zs, yy, xx, c), view(j, zs, yy, xx, c), send.at[j, zs], recv.at[j, zs], near[side])

    def dy_copy(j, zs):
        return remote(half(j, zs, y, 1 - x, c, 0), half(j, zs, y, 1 - x, c, 0), dy_send.at[j, zs], d_recv.at[j, zs, 0], near['y'])

    def dx_copy(j, zs):
        return remote(half(j, zs, 1 - y, x, c, 1), half(j, zs, 1 - y, x, c, 1), dx_send.at[j, zs], d_recv.at[j, zs, 1], near['x'])

    def kind_place(kind):
        return (y if kind < 2 else 1 - y), (x if kind % 2 == 0 else 1 - x)

    def c_copy(j, zs, kind):
        yy, xx = kind_place(kind)
        return remote(view(j, zs, yy, xx, c), view(j, zs, yy, xx, c), c_send.at[j, zs, kind], c_recv.at[j, zs, kind], near['c'])

    def share_core(j, zs, kind):
        yy, xx = kind_place(kind)
        c_copy(j, zs, kind).start()
        flush(j, zs, yy, xx, c, kind).start()

    def guard(off, body):
        if off == 0:
            body(z)
        elif off < 0:
            pl.when(z >= -off)(lambda: body(z + off))
        else:
            pl.when(z <= 3 - off)(lambda: body(z + off))

    def z_step(j, off):
        def body(zs):
            if off == 0:
                loads[j].wait()
            else:
                side_copy(j, zs, 'up').wait_recv()
            if off <= 0 and not plan.items[j].plane:
                pl.when(z < 3)(lambda: side_copy(j, zs, 'up').start())
            if off >= 0 and not plan.items[j].plane:
                pl.when(z > 0)(lambda: side_copy(j, zs, 'dn').start())
            side_copy(j, zs, 'x').start()
            side_copy(j, zs, 'y').start()
            share_core(j, zs, 0)
        guard(off, body)

    def xy_step(j, off):
        def body(zs):
            from_side(j, zs, 'x').wait_recv()
            dy_copy(j, zs).start()
            share_core(j, zs, 1)
            from_side(j, zs, 'y').wait_recv()
            dx_copy(j, zs).start()
            share_core(j, zs, 2)
        guard(off, body)

    def diag_step(j, off):
        def body(zs):
            for which in range(2):
                remote(half(j, zs, 1 - y, 1 - x, c, which), half(j, zs, 1 - y, 1 - x, c, which), dy_send.at[j, zs], d_recv.at[j, zs, which], near['y']).wait_recv()
            share_core(j, zs, 3)
        guard(off, body)

    def core_step(j, off):
        def body(zs):
            for kind in range(4):
                yy, xx = kind_place(kind)
                remote(view(j, zs, yy, xx, 1 - c), view(j, zs, yy, xx, 1 - c), c_send.at[j, zs, kind], c_recv.at[j, zs, kind], near['c']).wait_recv()
                flush(j, zs, yy, xx, 1 - c, 4 + kind).start()
        guard(off, body)

    def last_step(j, off):
        def body(zs):
            for kind in range(4):
                yy, xx = kind_place(kind)
                c_copy(j, zs, kind).wait_send()
                flush(j, zs, yy, xx, c, kind).wait()
                flush(j, zs, yy, xx, 1 - c, 4 + kind).wait()
            side_copy(j, zs, 'x').wait_send()
            side_copy(j, zs, 'y').wait_send()
            dy_copy(j, zs).wait_send()
            dx_copy(j, zs).wait_send()
            if off <= 0 and not plan.items[j].plane:
                pl.when(z < 3)(lambda: side_copy(j, zs, 'up').wait_send())
            if off >= 0 and not plan.items[j].plane:
                pl.when(z > 0)(lambda: side_copy(j, zs, 'dn').wait_send())
        guard(off, body)

    waves = [[(j, 0) for j in plan.order]]
    for far in range(1, 4):
        waves.append([(j, sign * far) for j in plan.order if not plan.items[j].plane for sign in (-1, 1)])
    for step in range(7):
        for func, lag in ((z_step, 0), (xy_step, 1), (diag_step, 2), (core_step, 3)):
            if 0 <= step - lag < 4:
                for j, off in waves[step - lag]:
                    func(j, off)
    for wave in waves:
        for j, off in wave:
            last_step(j, off)


class Item:
    def __init__(self, shape, dtype, piece, slot, half, plane=False):
        self.shape, self.dtype, self.piece, self.slot, self.half, self.plane = shape, dtype, piece, slot, half, plane


class Plan:
    def __init__(self, n_in, items, order):
        self.n_in, self.items, self.order = n_in, items, order


def gather_call(args, items, order, collective_id, name):
    n = len(items)
    dma = pltpu.SemaphoreType.DMA
    size = sum(math.prod(item.shape) * jnp.dtype(item.dtype).itemsize for item in items)
    hbm = pl.BlockSpec(memory_space=pltpu.HBM)
    flat = dma((n, 4))
    shapes = [jax.ShapeDtypeStruct(item.shape, item.dtype) for item in items]
    return pl.pallas_call(
        functools.partial(gather_kernel, Plan(len(args), items, order)),
        out_shape=shapes,
        in_specs=[hbm] * len(args),
        out_specs=[hbm] * len(shapes),
        scratch_shapes=[pltpu.VMEM(item.shape, item.dtype) for item in items]
        + [dma((n,)), flat, flat, flat, dma((n, 4, 2)), dma((n, 4, 4)), flat, flat, flat, flat, flat, flat, dma((n, 4, 4)), dma((n, 4, CORES))],
        compiler_params=pltpu.CompilerParams(collective_id=collective_id, has_side_effects=True, vmem_limit_bytes=size + HALF_STRIP * MIB),
        cost_estimate=pl.CostEstimate(flops=50_000_000_000, bytes_accessed=size, transcendentals=0),
        name=name,
    )(*args)


def col_slot(ref, zs, d):
    return ref.at[pl.ds(d * LANES, LANES), pl.ds(zs * BLOCK, BLOCK)]


def col_half(ref, zs, d, which):
    return ref.at[pl.ds(d * LANES + which * 64, 64), pl.ds(zs * BLOCK, BLOCK)]


def row_slot(ref, zs, d):
    return ref.at[pl.ds((zs * CORES + d) * STRIP, STRIP)]


def row_half(ref, zs, d, which):
    return ref.at[pl.ds((zs * CORES + d) * STRIP + which * HALF_STRIP, HALF_STRIP)]


def gather_weights(w_col, w_row):
    shape = (HIDDEN, HIDDEN)
    items = [Item(shape, w_col.dtype, lambda refs, z, d, i=i: refs[0].at[i, pl.ds(d * LANES, LANES)], col_slot, col_half) for i in range(2)]
    items += [Item(shape, w_row.dtype, lambda refs, z, d, i=i: refs[1].at[i, pl.ds(d * STRIP, STRIP)], row_slot, row_half) for i in range(2)]
    return gather_call((w_col, w_row), items, (0, 3, 2, 1), 1, 'weights')


def gather_results(facts, u_half, blocks):
    items = [
        Item((STRIP, 4, SYM_ROWS, BLOCK), facts.dtype, lambda refs, z, d: refs[0],
             lambda ref, zs, d: ref.at[zs * CORES + d], lambda ref, zs, d, which: ref.at[zs * CORES + d, pl.ds(2 * which, 2)]),
        Item((CORES, BLOCK, D_ROWS), facts.dtype, lambda refs, z, d: refs[1],
             lambda ref, zs, d: ref.at[d], lambda ref, zs, d, which: ref.at[d, pl.ds(which * LANES, LANES)], True),
        Item((4, BLOCK, BLOCK), facts.dtype, lambda refs, z, d: refs[2],
             lambda ref, zs, d: ref.at[:, pl.ds(d * STRIP, STRIP)], lambda ref, zs, d, which: ref.at[pl.ds(2 * which, 2), pl.ds(d * STRIP, STRIP)], True),
    ]
    return gather_call((facts, u_half, blocks), items, (1, 2, 0), 3, 'results')


def add_into(dst, src, rows):
    step = max(n for n in range(CORES, 65, CORES) if rows % n == 0)

    def body(i, carry):
        span = pl.ds(pl.multiple_of(i * step, CORES), step)
        dst[span, :] = dst[span, :] + src[span, :]
        return carry

    lax.fori_loop(0, rows // step, body, 0)


def scatter_kernel(rows, parts_ref, x_ref, dy_ref, share_ref, eshare_ref, grad_ref, own, mate, one_x, one_y, two_x, two_y, up_buf, dn_buf,
                   tok, eacc, emate, eone, etwo, gland, e_sem, emate_sem, eone_sem, etwo_sem, g_sem, out2_sem,
                   own_sem, mate_send, mate_recv, x1_send, x1_recv, y1_send, y1_recv, x2_send, x2_recv, y2_send, y2_recv,
                   up_send, up_recv, dn_send, dn_recv, out_sem):
    z, y, x, c, near = torus_place()
    sub = rows // 4
    def tok_load(t):
        return pltpu.make_async_copy((x_ref, dy_ref)[t // 4].at[pl.ds(t % 4 * HIDDEN, HIDDEN)], tok.at[t % 2], e_sem.at[t % 2])

    def ends_step(t):
        tok_load(t).wait()
        put_sym(eacc.at[t // 4].reshape(CORES, SYM_ROWS, BLOCK), sym_blocks(tok.at[t % 2], z), t % 4 > 0)
        if t + 2 < CORES:
            tok_load(t + 2).start()

    def eown(mat, *where):
        return eacc.at[(mat,) + where + (c,)]

    tok_load(0).start()
    tok_load(1).start()
    loads = {}
    for k, (zd, h) in enumerate(CHUNK_ORDER):
        loads[k] = []
        for col in range(2):
            span = pl.ds(col * 2 * sub + h * sub, sub)
            load = pltpu.make_async_copy(parts_ref.at[zd, :, :, c, span], own.at[zd, :, :, span], own_sem.at[k, col])
            load.start()
            loads[k].append(load)
    meet_neighbours(z, near)
    every = slice(None)
    ematec = remote(eacc.at[:, :, :, 1 - c], emate, emate_sem.at[0], emate_sem.at[1], near['c'])
    eones = (remote(eown(0, every, 1 - x), eone.at[0], eone_sem.at[0], eone_sem.at[1], near['x']),
             remote(eown(1, 1 - y, every), eone.at[1], eone_sem.at[2], eone_sem.at[3], near['y']))
    etwos = (remote(eown(0, 1 - y, x), etwo.at[0], etwo_sem.at[0], etwo_sem.at[1], near['y']),
             remote(eown(1, y, 1 - x), etwo.at[1], etwo_sem.at[2], etwo_sem.at[3], near['x']))
    mates = {}
    for k, (zd, h) in enumerate(CHUNK_ORDER):
        mates[k] = []
        for col in range(2):
            span = pl.ds(col * 2 * sub + h * sub, sub)
            copy = remote(parts_ref.at[zd, :, :, 1 - c, span], mate.at[zd, :, :, span], mate_send.at[k, col], mate_recv.at[k, col], near['c'])
            copy.start()
            mates[k].append(copy)

    def spans(h):
        return pl.ds(h * sub, sub), pl.ds(2 * sub + h * sub, sub)

    def one_copies(k):
        zd, h = CHUNK_ORDER[k]
        first, second = spans(h)
        piece = pl.ds(h * sub, sub)
        return (remote(own.at[zd, :, 1 - x, first], one_x.at[zd, :, piece], x1_send.at[k], x1_recv.at[k], near['x']),
                remote(own.at[zd, 1 - y, :, second], one_y.at[zd, :, piece], y1_send.at[k], y1_recv.at[k], near['y']))

    def two_copies(k):
        zd, h = CHUNK_ORDER[k]
        first, second = spans(h)
        piece = pl.ds(h * sub, sub)
        return (remote(own.at[zd, 1 - y, x, first], two_y.at[zd, piece], y2_send.at[k], y2_recv.at[k], near['y']),
                remote(own.at[zd, y, 1 - x, second], two_x.at[zd, piece], x2_send.at[k], x2_recv.at[k], near['x']))

    def z_copies(k):
        zd, h = CHUNK_ORDER[k]
        out = []
        for col, span in enumerate(spans(h)):
            out.append((remote(own.at[zd, y, x, span], up_buf.at[zd, span], dn_send.at[k, col], up_recv.at[k, col], near['dn']),
                        remote(own.at[zd, y, x, span], dn_buf.at[zd, span], up_send.at[k, col], dn_recv.at[k, col], near['up'])))
        return out

    def step_a(k):
        zd, h = CHUNK_ORDER[k]
        first, second = spans(h)
        ones = one_copies(k)
        loads[k][0].wait()
        mates[k][0].wait_recv()
        for yy in range(2):
            add_into(own.at[zd, yy, 1 - x, first], mate.at[zd, yy, 1 - x, first], sub)
        ones[0].start()
        loads[k][1].wait()
        mates[k][1].wait_recv()
        for xx in range(2):
            add_into(own.at[zd, 1 - y, xx, second], mate.at[zd, 1 - y, xx, second], sub)
        ones[1].start()
        for yy in range(2):
            add_into(own.at[zd, yy, x, first], mate.at[zd, yy, x, first], sub)
        for xx in range(2):
            add_into(own.at[zd, y, xx, second], mate.at[zd, y, xx, second], sub)

    def step_b(k):
        zd, h = CHUNK_ORDER[k]
        first, second = spans(h)
        piece = pl.ds(h * sub, sub)
        ones, twos = one_copies(k), two_copies(k)
        ones[0].wait_recv()
        add_into(own.at[zd, 1 - y, x, first], one_x.at[zd, 1 - y, piece], sub)
        twos[0].start()
        ones[1].wait_recv()
        add_into(own.at[zd, y, 1 - x, second], one_y.at[zd, 1 - x, piece], sub)
        twos[1].start()
        add_into(own.at[zd, y, x, first], one_x.at[zd, y, piece], sub)
        add_into(own.at[zd, y, x, second], one_y.at[zd, x, piece], sub)

    def step_c(k):
        zd, h = CHUNK_ORDER[k]
        first, second = spans(h)
        piece = pl.ds(h * sub, sub)
        twos = two_copies(k)
        zcs = z_copies(k)
        for col, (copy, buf, span) in enumerate(((twos[0], two_y, first), (twos[1], two_x, second))):
            copy.wait_recv()
            add_into(own.at[zd, y, x, span], buf.at[zd, piece], sub)

            @pl.when((z < 3) & (z >= zd))
            def _(col=col, span=span):
                zcs[col][0].wait_recv()
                add_into(own.at[zd, y, x, span], up_buf.at[zd, span], sub)

            @pl.when((z > 0) & (z <= zd))
            def _(col=col, span=span):
                zcs[col][1].wait_recv()
                add_into(own.at[zd, y, x, span], dn_buf.at[zd, span], sub)
            pl.when(z > zd)(lambda: zcs[col][0].start())
            pl.when(z < zd)(lambda: zcs[col][1].start())

            @pl.when(z == zd)
            def _(col=col, span=span):
                pltpu.make_async_copy(own.at[zd, y, x, span], share_ref.at[span], out_sem.at[h, col]).start()

    def ends_a():
        ematec.wait_recv()
        for mat in range(2):
            for yy in range(2):
                for xx in range(2):
                    add_into(eown(mat, yy, xx), emate.at[mat, yy, xx], SYM_ROWS)
            eones[mat].start()

    def ends_b():
        eones[0].wait_recv()
        for yy in range(2):
            add_into(eown(0, yy, x), eone.at[0, yy], SYM_ROWS)
        etwos[0].start()
        eones[1].wait_recv()
        for xx in range(2):
            add_into(eown(1, y, xx), eone.at[1, xx], SYM_ROWS)
        etwos[1].start()

    def ends_c():
        for mat in range(2):
            etwos[mat].wait_recv()
            add_into(eown(mat, y, x), etwo.at[mat], SYM_ROWS)
            pltpu.make_async_copy(eown(mat, y, x), eshare_ref.at[mat], out2_sem.at[mat]).start()

    n = len(CHUNK_ORDER)
    for step in range(n + 3):
        if step < n:
            step_a(step)
        if step < 4:
            ends_step(2 * step)
            ends_step(2 * step + 1)
        if step == 4:
            ematec.start()
        if step == 5:
            ends_a()
        if step == 6:
            ends_b()
        if step == CORES:
            ends_c()
        if 0 <= step - 1 < n:
            step_b(step - 1)
        if 0 <= step - 3 < n:
            step_c(step - 3)
    mine = own.at[z, y, x, pl.ds(0, D_ROWS)]
    gcopy = remote(mine, gland, g_sem.at[0], g_sem.at[1], near['c'])
    gcopy.start()
    gout = pltpu.make_async_copy(mine, grad_ref.at[c], out2_sem.at[2])
    gout.start()
    gcopy.wait_recv()
    gmate = pltpu.make_async_copy(gland, grad_ref.at[1 - c], out2_sem.at[3])
    gmate.start()
    for copy in (ematec, gcopy) + eones + etwos:
        copy.wait_send()
    for k, (zd, h) in enumerate(CHUNK_ORDER):
        for copy in mates[k] + list(one_copies(k)) + list(two_copies(k)):
            copy.wait_send()
        for col, (down, up) in enumerate(z_copies(k)):
            pl.when(z > zd)(lambda: down.wait_send())
            pl.when(z < zd)(lambda: up.wait_send())
    for h in range(2):
        for col in range(2):
            span = spans(h)[col]
            pltpu.make_async_copy(own.at[0, y, x, span], share_ref.at[span], out_sem.at[h, col]).wait()
    for mat in range(2):
        pltpu.make_async_copy(eown(mat, y, x), eshare_ref.at[mat], out2_sem.at[mat]).wait()
    gout.wait()
    gmate.wait()


def scatter_call(parts, x_tokens, dy_tokens, collective_id, name):
    rows = parts.shape[-2]
    half = rows // 2
    f32 = jnp.float32
    dma = pltpu.SemaphoreType.DMA
    n = len(CHUNK_ORDER)
    whole = pltpu.VMEM((4, 2, 2, rows, BLOCK), f32)
    one_buf = pltpu.VMEM((4, 2, half, BLOCK), f32)
    two_buf = pltpu.VMEM((4, half, BLOCK), f32)
    z_buf = pltpu.VMEM((4, rows, BLOCK), f32)
    hbm = pl.BlockSpec(memory_space=pltpu.HBM)
    return pl.pallas_call(
        functools.partial(scatter_kernel, rows),
        out_shape=[jax.ShapeDtypeStruct((rows, BLOCK), f32), jax.ShapeDtypeStruct((2, SYM_ROWS, BLOCK), f32), jax.ShapeDtypeStruct((2, D_ROWS, BLOCK), f32)],
        in_specs=[hbm] * 3,
        out_specs=[hbm] * 3,
        scratch_shapes=[whole, whole, one_buf, one_buf, two_buf, two_buf, z_buf, z_buf,
                        pltpu.VMEM((2, HIDDEN, HIDDEN), x_tokens.dtype), pltpu.VMEM((2, 2, 2, 2, SYM_ROWS, BLOCK), f32), pltpu.VMEM((2, 2, 2, SYM_ROWS, BLOCK), f32), pltpu.VMEM((2, 2, SYM_ROWS, BLOCK), f32), pltpu.VMEM((2, SYM_ROWS, BLOCK), f32), pltpu.VMEM((D_ROWS, BLOCK), f32),
                        dma((2,)), dma((2,)), dma((4,)), dma((4,)), dma((2,)), dma((4,))]
        + [dma((n, 2))] * 3 + [dma((n,))] * CORES + [dma((n, 2))] * 4 + [dma((2, 2))],
        compiler_params=pltpu.CompilerParams(collective_id=collective_id, has_side_effects=True, vmem_limit_bytes=60 * MIB),
        cost_estimate=pl.CostEstimate(flops=120_000_000_000, bytes_accessed=60 * MIB, transcendentals=0),
        name=name,
    )(parts.reshape(4, 2, 2, 2, rows, BLOCK), x_tokens, dy_tokens)


def mirror_kernel(in_ref, a_ref, s_ref):
    def block(i, j, mat):
        def take(plane, at, size):
            return in_ref[plane, :, mat, pl.ds(at, size)].reshape(CORES * size, BLOCK)

        if i == j:
            return take(j, 0, STRIP)
        if i == (j + 1) % 4:
            return take(j, STRIP, STRIP)
        if j == (i + 1) % 4:
            return take(i, STRIP, STRIP).T
        low = min(i, j)
        both = jnp.concatenate([take(low, 64, HALF_STRIP), take(low + 2, 64, HALF_STRIP)], axis=0)
        return both if i > j else both.T

    for i in range(4):
        @pl.when(pl.program_id(1) == i)
        def _(i=i):
            for mat, out in enumerate((a_ref, s_ref)):
                for j in range(4):
                    out[0, :, pl.ds(j * BLOCK, BLOCK)] = block(i, j, mat)


def mirror_call(facts):
    full = jax.ShapeDtypeStruct((2, HIDDEN, HIDDEN), facts.dtype)
    out_spec = pl.BlockSpec((1, BLOCK, HIDDEN), lambda k, i: (k, i, 0))
    return pl.pallas_call(
        mirror_kernel,
        grid=(2, 4),
        out_shape=[full, full],
        in_specs=[pl.BlockSpec((4, CORES, 2, SYM_ROWS, BLOCK), lambda k, i: (0, 0, k, 0, 0))],
        out_specs=[out_spec, out_spec],
        compiler_params=pltpu.CompilerParams(vmem_limit_bytes=STRIP * MIB),
        cost_estimate=pl.CostEstimate(flops=10_000_000_000, bytes_accessed=26 * MIB, transcendentals=0),
        name='mirror',
    )(facts.reshape(4, CORES, 4, SYM_ROWS, BLOCK))


def solution(mesh):
    data_ways = mesh.shape['data']
    model_ways = mesh.shape['model']

    def shard_body(x_tokens, dy_tokens, w_col, w_row, a_old_col, s_old_col, a_old_row, s_old_row, a_inv_col, s_inv_col, a_inv_row, s_inv_row):
        model_id = lax.axis_index('model')
        data_id = lax.axis_index('data')
        inv_rows = 1.0 / (x_tokens.shape[0] * data_ways)
        w_one, w_three, w_two, w_four = gather_weights(w_col, w_row)
        rows_dev = x_tokens.shape[0] // model_ways
        x_loc = lax.dynamic_slice(x_tokens, (rows_dev * model_id, 0), (rows_dev, HIDDEN))
        dy_loc = lax.dynamic_slice(dy_tokens, (rows_dev * model_id, 0), (rows_dev, HIDDEN))
        z_one = matmul(x_loc, w_one).astype(jnp.bfloat16)
        h_one = activate(z_one)
        z_two = matmul(h_one, w_two).astype(jnp.bfloat16)
        h_two = activate(z_two)
        z_three = matmul(h_two, w_three).astype(jnp.bfloat16)
        h_three = activate(z_three)
        g_three = back_gate(matmul_nt(dy_loc, w_four).astype(jnp.bfloat16), z_three)
        g_two = back_gate(matmul_nt(g_three, w_three).astype(jnp.bfloat16), z_two)
        g_one = back_gate(matmul_nt(g_two, w_two).astype(jnp.bfloat16), z_one)
        parts = gram_call(x_loc, g_one, g_two, h_one, h_two, g_three, dy_loc, h_three)
        share, eshare, grad_mat = scatter_call(parts, x_tokens, dy_tokens, 2, 'sums')
        keep = 1.0 - FACTOR_DECAY
        low = lax.rem(model_id, 2)
        spots = ((model_id * BLOCK + STRIP * data_id, model_id * BLOCK, STRIP),
                 (lax.rem(model_id + 1, 4) * BLOCK + STRIP * data_id, model_id * BLOCK, STRIP),
                 ((low + 2) * BLOCK + model_id // 2 * LANES + HALF_STRIP * data_id, low * BLOCK, HALF_STRIP))
        olds = [jnp.concatenate([lax.dynamic_slice(old, (0, at, col), (2, size, BLOCK)) for at, col, size in spots], axis=1) for old in (a_old_col, s_old_row)]
        mids = share[FULL_BASE:BLOCK_BASE].reshape(2, SYM_ROWS, BLOCK)
        sums = jnp.stack([eshare[0], mids[1], mids[0], eshare[1]])
        facts = FACTOR_DECAY * jnp.stack(olds, axis=1).reshape(4, SYM_ROWS, BLOCK) + keep * inv_rows * sums
        grad_mat = jnp.swapaxes(grad_mat.reshape(4, BLOCK, BLOCK), 0, 1).reshape(BLOCK, HIDDEN) * inv_rows
        layer_id = data_id // 2
        stack_id = layer_id // 2
        is_col = lax.rem(layer_id, 2) == 0
        half_at = lax.rem(data_id, 2) * D_ROWS
        full_inv = jnp.where(is_col, *[lax.dynamic_slice(inv, (stack_id, half_at, 0), (1, D_ROWS, HIDDEN))[0] for inv in (a_inv_col, s_inv_row)])
        block_inv = jnp.where(is_col, *[lax.dynamic_slice(inv, (stack_id, 0, 0), (1, BLOCK, BLOCK))[0] for inv in (s_inv_col, a_inv_row)])
        u_half = lax.dot_general(exact_dot(block_inv, grad_mat), full_inv, NT_DIMS, precision=EXACT, preferred_element_type=jnp.float32)
        old_blocks = jnp.concatenate([lax.dynamic_slice(old, (0, STRIP * data_id, 0), (2, STRIP, BLOCK)) for old in (s_old_col, a_old_row)])
        new_blocks = jnp.swapaxes(share[BLOCK_BASE:].reshape(2, 2, STRIP, BLOCK), 0, 1).reshape(4, STRIP, BLOCK)
        blocks = FACTOR_DECAY * old_blocks + keep * inv_rows * new_blocks
        fact_all, u_all, blk_all = gather_results(facts, u_half, blocks)
        a_new_col, s_new_row = mirror_call(fact_all)
        u_all = u_all.reshape(2, 2, 2, BLOCK, D_ROWS)
        u_col = jnp.transpose(u_all[:, 0], (0, 1, 3, 2)).reshape(2, HIDDEN, BLOCK)
        u_row = jnp.swapaxes(u_all[:, 1], 1, 2).reshape(2, BLOCK, HIDDEN)
        return (u_col, u_row, a_new_col, blk_all[:2], blk_all[2:], s_new_row)

    batch_split = P('data', None)
    col_split = P(None, None, 'model')
    row_split = P(None, 'model', None)
    replicated = P()
    return jax.shard_map(
        shard_body,
        mesh=mesh,
        in_specs=(batch_split, batch_split, col_split, row_split, replicated, row_split, row_split, replicated, replicated, row_split, row_split, replicated),
        out_specs=(col_split, row_split, replicated, row_split, row_split, replicated),
        check_vma=False,
    )
```

```python
import functools
import math
import jax
import jax.numpy as jnp
from jax import lax
from jax.sharding import PartitionSpec as P
from jax.experimental import pallas as pl
from jax.experimental.pallas import tpu as pltpu

FACTOR_DECAY = 0.8
GELU_SCALE = math.sqrt(2.0 / math.pi)
GELU_CUBIC = 0.044715
EXACT = lax.Precision.HIGHEST
TN_DIMS = (((0,), (0,)), ((), ()))
NT_DIMS = (((1,), (1,)), ((), ()))
BOTH = ('model', 'data')


def gelu_value(pre_act):
    tanh_arg = GELU_SCALE * (pre_act + GELU_CUBIC * pre_act * pre_act * pre_act)
    return 0.5 * pre_act * (1.0 + jnp.tanh(tanh_arg))


def gelu_slope(pre_act):
    tanh_arg = GELU_SCALE * (pre_act + GELU_CUBIC * pre_act * pre_act * pre_act)
    tanh_val = jnp.tanh(tanh_arg)
    return 0.5 * (1.0 + tanh_val) + 0.5 * pre_act * (1.0 - tanh_val * tanh_val) * GELU_SCALE * (1.0 + 3.0 * GELU_CUBIC * pre_act * pre_act)


def activate(pre_act):
    return gelu_value(pre_act.astype(jnp.float32)).astype(jnp.bfloat16)


def back_gate(grad_act, pre_act):
    return (grad_act.astype(jnp.float32) * gelu_slope(pre_act.astype(jnp.float32))).astype(jnp.bfloat16)


def matmul(left_mat, right_mat):
    return jnp.dot(left_mat, right_mat, preferred_element_type=jnp.float32)


def matmul_tn(left_mat, right_mat):
    return lax.dot_general(left_mat, right_mat, TN_DIMS, preferred_element_type=jnp.float32)


def matmul_nt(left_mat, right_mat):
    return lax.dot_general(left_mat, right_mat, NT_DIMS, preferred_element_type=jnp.float32)


def exact_dot(left_mat, right_mat):
    return jnp.dot(left_mat, right_mat, precision=EXACT, preferred_element_type=jnp.float32)


MIB = 1024 * 1024
BLOCK = 256
HIDDEN = 1024
D_ROWS = 512
SYM_ROWS = 80
FULL_BASE = 512
BLOCK_BASE = 672
SHARE_ROWS = 800
LANES = 128
STRIP = 32
HALF_STRIP = 16
CORES = 8


def gram_kernel(x_ref, g1_ref, g2_ref, h1_ref, h2_ref, g3_ref, dy_ref, h3_ref, out_ref,
                act, stage, bstage, fstage, in_sem, out_sem, b_sem, f_sem):
    sources = [dy_ref, h3_ref, h2_ref, g3_ref, g2_ref, h1_ref, x_ref, g1_ref]
    slots = [3, 7, 2, 6, 1, 5, 0, 4]
    loads = [pltpu.make_async_copy(src, act.at[slot], in_sem.at[slot]) for src, slot in zip(sources, slots)]
    for load in loads:
        load.start()

    def out_copy(slot, dst):
        return pltpu.make_async_copy(stage.at[slot], dst, out_sem.at[slot])

    def f_copy(slot, n, which):
        return pltpu.make_async_copy(fstage.at[slot], out_ref.at[pl.ds(n * CORES, CORES), pl.ds(FULL_BASE + which * SYM_ROWS, SYM_ROWS)], f_sem.at[slot])

    for layer in (3, 2, 1, 0):
        pltpu.make_async_copy(x_ref, act.at[layer], in_sem.at[layer]).wait()
        pltpu.make_async_copy(x_ref, act.at[4 + layer], in_sem.at[4 + layer]).wait()

        def d_body(m, carry, layer=layer):
            slot = lax.rem(m, 2)
            cols = pl.ds(pl.multiple_of(m * BLOCK, BLOCK), BLOCK)
            right = act[4 + layer, :, cols]
            dst = out_ref.at[pl.ds(m * CORES + 2 * layer, 2), pl.ds(0, D_ROWS)]

            if layer == 3:
                @pl.when(m >= 2)
                def _():
                    out_copy(slot, dst).wait()
                    pltpu.make_async_copy(bstage.at[slot], out_ref.at[pl.ds(0, CORES), pl.ds(BLOCK_BASE, STRIP)], b_sem.at[slot]).wait()
            else:
                out_copy(slot, dst).wait()
                pltpu.make_async_copy(bstage.at[slot], out_ref.at[pl.ds(0, CORES), pl.ds(BLOCK_BASE, STRIP)], b_sem.at[slot]).wait()
            prod = lax.dot_general(act[layer], right, TN_DIMS, preferred_element_type=jnp.float32)
            stage[slot] = prod.reshape(2, D_ROWS, BLOCK)
            out_copy(slot, dst).start()
            blk = lax.dot_general(right, right, TN_DIMS, preferred_element_type=jnp.float32)
            bstage[slot] = blk.reshape(CORES, STRIP, BLOCK)
            pltpu.make_async_copy(bstage.at[slot], out_ref.at[pl.ds(m * CORES, CORES), pl.ds(BLOCK_BASE + STRIP * layer, STRIP)], b_sem.at[slot]).start()
            return carry

        lax.fori_loop(0, 4, d_body, 0)

        if layer in (2, 1):
            which = 0 if layer == 2 else 1

            def f_body(n, carry, layer=layer, which=which):
                slot = lax.rem(n, 2)
                if which == 0:
                    pl.when(n >= 2)(lambda: f_copy(slot, n, which).wait())
                else:
                    f_copy(slot, n, which).wait()
                put_sym(fstage.at[slot], sym_blocks(act.at[layer], n), False)
                f_copy(slot, n, which).start()
                return carry

            lax.fori_loop(0, 4, f_body, 0)
    for slot in range(2):
        f_copy(slot, 0, 0).wait()
        pltpu.make_async_copy(stage.at[slot], out_ref.at[pl.ds(0, 2), pl.ds(0, D_ROWS)], out_sem.at[slot]).wait()
        pltpu.make_async_copy(bstage.at[slot], out_ref.at[pl.ds(0, CORES), pl.ds(BLOCK_BASE, STRIP)], b_sem.at[slot]).wait()


def gram_call(x_loc, g_one, g_two, h_one, h_two, g_three, dy_loc, h_three):
    any_spec = pl.BlockSpec(memory_space=pl.ANY)
    return pl.pallas_call(
        gram_kernel,
        out_shape=jax.ShapeDtypeStruct((STRIP, SHARE_ROWS, BLOCK), jnp.float32),
        in_specs=[any_spec] * CORES,
        out_specs=any_spec,
        scratch_shapes=[
            pltpu.VMEM((CORES, HIDDEN, HIDDEN), jnp.bfloat16),
            pltpu.VMEM((2, 2, D_ROWS, BLOCK), jnp.float32),
            pltpu.VMEM((2, CORES, STRIP, BLOCK), jnp.float32),
            pltpu.VMEM((2, CORES, SYM_ROWS, BLOCK), jnp.float32),
            pltpu.SemaphoreType.DMA((CORES,)),
            pltpu.SemaphoreType.DMA((2,)),
            pltpu.SemaphoreType.DMA((2,)),
            pltpu.SemaphoreType.DMA((2,)),
        ],
        compiler_params=pltpu.CompilerParams(vmem_limit_bytes=48 * HIDDEN * HIDDEN),
        cost_estimate=pl.CostEstimate(flops=15_000_000_000, bytes_accessed=46_000_000, transcendentals=0),
        name='gram',
    )(x_loc, g_one, g_two, h_one, h_two, g_three, dy_loc, h_three)


MESH_ID = pl.DeviceIdType.MESH
PIECES = 5
CHUNK_ORDER = tuple((zd, h) for pair in ((0, 3), (1, 2)) for h in range(PIECES) for zd in pair)


def torus_place():
    z = lax.axis_index('model')
    d = lax.axis_index('data')
    y = d // 4
    x = (d // 2) % 2
    c = d % 2
    near = {'x': (z, d + 2 - 4 * x), 'y': (z, d + 4 - CORES * y), 'c': (z, d + 1 - 2 * c), 'up': (z + 1, d), 'dn': (z - 1, d)}
    return z, y, x, c, near


def meet_neighbours(z, near):
    barrier = pltpu.get_barrier_semaphore()
    for side in ('x', 'y', 'c'):
        pl.semaphore_signal(barrier, inc=1, device_id=near[side], device_id_type=MESH_ID)

    @pl.when(z < 3)
    def _():
        pl.semaphore_signal(barrier, inc=1, device_id=near['up'], device_id_type=MESH_ID)

    @pl.when(z > 0)
    def _():
        pl.semaphore_signal(barrier, inc=1, device_id=near['dn'], device_id_type=MESH_ID)
    pl.semaphore_wait(barrier, 3 + (z + 3) // 4 + (6 - z) // 4)


def remote(src, dst, send_sem, recv_sem, where):
    return pltpu.make_async_remote_copy(src_ref=src, dst_ref=dst, send_sem=send_sem, recv_sem=recv_sem, device_id=where, device_id_type=MESH_ID)


def sym_blocks(left, n):
    def cols(at, size):
        return left[:, pl.ds(pl.multiple_of(at, LANES), size)]

    low = n % 2
    right = cols(n * BLOCK, BLOCK)
    pairs = ((right, right, STRIP), (cols((n + 1) % 4 * BLOCK, BLOCK), right, STRIP),
             (cols((low + 2) * BLOCK + n // 2 * LANES, LANES), cols(low * BLOCK, BLOCK), HALF_STRIP))
    return [lax.dot_general(a, b, TN_DIMS, preferred_element_type=jnp.float32).reshape(CORES, rows, BLOCK) for a, b, rows in pairs]


def put_sym(dst, blocks, more):
    at = 0
    for blk in blocks:
        span = pl.ds(at, blk.shape[1])
        dst[:, span] = dst[:, span] + blk if more else blk
        at += blk.shape[1]


def gather_kernel(plan, *refs):
    n = len(plan.items)
    pieces, refs = refs[:plan.n_in], refs[plan.n_in:]
    outs, refs = refs[:n], refs[n:]
    ends = len(plan.tokens) > 0
    if ends:
        ends_ref, refs = refs[0], refs[1:]
    lands, refs = refs[:n], refs[n:]
    if ends:
        tok, acc, tok_sem, acc_sem, *refs = refs
    load_sem, z_recv, x_recv, y_recv, d_recv, c_recv, up_send, dn_send, x_send, y_send, dy_send, dx_send, c_send, flush_sem = refs
    z, y, x, c, near = torus_place()

    def slot(ref, j, zs, yy, xx, cc):
        return plan.items[j].slot(ref, zs, 4 * yy + 2 * xx + cc)

    def view(j, zs, yy, xx, cc):
        return slot(lands[j], j, zs, yy, xx, cc)

    def half(j, zs, yy, xx, cc, which):
        return plan.items[j].half(lands[j], zs, 4 * yy + 2 * xx + cc, which)

    def flush(j, zs, yy, xx, cc, index):
        return pltpu.make_async_copy(view(j, zs, yy, xx, cc), slot(outs[j], j, zs, yy, xx, cc), flush_sem.at[j, zs, index])

    loads = [pltpu.make_async_copy(item.piece(pieces, z, 4 * y + 2 * x + c), view(j, z, y, x, c), load_sem.at[j]) for j, item in enumerate(plan.items)]
    for load in loads:
        load.start()

    def tok_load(t):
        src = pieces[plan.tokens[t // 4]].at[pl.ds(t % 4 * HIDDEN, HIDDEN)]
        return pltpu.make_async_copy(src, tok.at[t % 2], tok_sem.at[t % 2])

    def ends_out(mat):
        return pltpu.make_async_copy(acc.at[mat], ends_ref.at[mat], acc_sem.at[mat])

    def ends_step(t):
        tok_load(t).wait()
        put_sym(acc.at[t // 4], sym_blocks(tok.at[t % 2], z), t % 4 > 0)
        if t + 2 < CORES:
            tok_load(t + 2).start()
        if t % 4 == 3:
            ends_out(t // 4).start()

    todo = list(range(CORES)) if ends else []
    if ends:
        tok_load(0).start()
        tok_load(1).start()
    meet_neighbours(z, near)

    def side_copy(j, zs, side):
        send, recv = {'x': (x_send, x_recv), 'y': (y_send, y_recv), 'up': (up_send, z_recv), 'dn': (dn_send, z_recv)}[side]
        return remote(view(j, zs, y, x, c), view(j, zs, y, x, c), send.at[j, zs], recv.at[j, zs], near[side])

    def from_side(j, zs, side):
        yy, xx = (y, 1 - x) if side == 'x' else (1 - y, x)
        send, recv = {'x': (x_send, x_recv), 'y': (y_send, y_recv)}[side]
        return remote(view(j, zs, yy, xx, c), view(j, zs, yy, xx, c), send.at[j, zs], recv.at[j, zs], near[side])

    def dy_copy(j, zs):
        return remote(half(j, zs, y, 1 - x, c, 0), half(j, zs, y, 1 - x, c, 0), dy_send.at[j, zs], d_recv.at[j, zs, 0], near['y'])

    def dx_copy(j, zs):
        return remote(half(j, zs, 1 - y, x, c, 1), half(j, zs, 1 - y, x, c, 1), dx_send.at[j, zs], d_recv.at[j, zs, 1], near['x'])

    def kind_place(kind):
        return (y if kind < 2 else 1 - y), (x if kind % 2 == 0 else 1 - x)

    def c_copy(j, zs, kind):
        yy, xx = kind_place(kind)
        return remote(view(j, zs, yy, xx, c), view(j, zs, yy, xx, c), c_send.at[j, zs, kind], c_recv.at[j, zs, kind], near['c'])

    def share_core(j, zs, kind):
        yy, xx = kind_place(kind)
        c_copy(j, zs, kind).start()
        flush(j, zs, yy, xx, c, kind).start()

    def guard(off, body):
        if off == 0:
            body(z)
        elif off < 0:
            pl.when(z >= -off)(lambda: body(z + off))
        else:
            pl.when(z <= 3 - off)(lambda: body(z + off))

    def z_step(j, off):
        def body(zs):
            if off == 0:
                loads[j].wait()
            else:
                side_copy(j, zs, 'up').wait_recv()
            if off <= 0 and not plan.items[j].plane:
                pl.when(z < 3)(lambda: side_copy(j, zs, 'up').start())
            if off >= 0 and not plan.items[j].plane:
                pl.when(z > 0)(lambda: side_copy(j, zs, 'dn').start())
            side_copy(j, zs, 'x').start()
            side_copy(j, zs, 'y').start()
            share_core(j, zs, 0)
        guard(off, body)

    def xy_step(j, off):
        def body(zs):
            from_side(j, zs, 'x').wait_recv()
            dy_copy(j, zs).start()
            share_core(j, zs, 1)
            from_side(j, zs, 'y').wait_recv()
            dx_copy(j, zs).start()
            share_core(j, zs, 2)
        guard(off, body)

    def diag_step(j, off):
        def body(zs):
            for which in range(2):
                remote(half(j, zs, 1 - y, 1 - x, c, which), half(j, zs, 1 - y, 1 - x, c, which), dy_send.at[j, zs], d_recv.at[j, zs, which], near['y']).wait_recv()
            share_core(j, zs, 3)
        guard(off, body)

    def core_step(j, off):
        def body(zs):
            for kind in range(4):
                yy, xx = kind_place(kind)
                remote(view(j, zs, yy, xx, 1 - c), view(j, zs, yy, xx, 1 - c), c_send.at[j, zs, kind], c_recv.at[j, zs, kind], near['c']).wait_recv()
                flush(j, zs, yy, xx, 1 - c, 4 + kind).start()
        guard(off, body)

    def last_step(j, off):
        def body(zs):
            for kind in range(4):
                yy, xx = kind_place(kind)
                c_copy(j, zs, kind).wait_send()
                flush(j, zs, yy, xx, c, kind).wait()
                flush(j, zs, yy, xx, 1 - c, 4 + kind).wait()
            side_copy(j, zs, 'x').wait_send()
            side_copy(j, zs, 'y').wait_send()
            dy_copy(j, zs).wait_send()
            dx_copy(j, zs).wait_send()
            if off <= 0 and not plan.items[j].plane:
                pl.when(z < 3)(lambda: side_copy(j, zs, 'up').wait_send())
            if off >= 0 and not plan.items[j].plane:
                pl.when(z > 0)(lambda: side_copy(j, zs, 'dn').wait_send())
        guard(off, body)

    waves = [[(j, 0) for j in plan.order]]
    for far in range(1, 4):
        waves.append([(j, sign * far) for j in plan.order if not plan.items[j].plane for sign in (-1, 1)])
    for step in range(7):
        for func, lag in ((z_step, 0), (xy_step, 1), (diag_step, 2), (core_step, 3)):
            if 0 <= step - lag < 4:
                for j, off in waves[step - lag]:
                    func(j, off)
                if todo and step >= 3 and lag:
                    ends_step(todo.pop(0))
    for t in todo:
        ends_step(t)
    if ends:
        ends_out(0).wait()
        ends_out(1).wait()
    for wave in waves:
        for j, off in wave:
            last_step(j, off)


class Item:
    def __init__(self, shape, dtype, piece, slot, half, plane=False):
        self.shape, self.dtype, self.piece, self.slot, self.half, self.plane = shape, dtype, piece, slot, half, plane


class Plan:
    def __init__(self, n_in, items, order, tokens):
        self.n_in, self.items, self.order, self.tokens = n_in, items, order, tokens


def gather_call(args, items, order, collective_id, name, tokens=()):
    n = len(items)
    dma = pltpu.SemaphoreType.DMA
    size = sum(math.prod(item.shape) * jnp.dtype(item.dtype).itemsize for item in items)
    hbm = pl.BlockSpec(memory_space=pltpu.HBM)
    flat = dma((n, 4))
    shapes = [jax.ShapeDtypeStruct(item.shape, item.dtype) for item in items]
    extra = []
    if tokens:
        part = (2, CORES, SYM_ROWS, BLOCK)
        shapes.append(jax.ShapeDtypeStruct(part, jnp.float32))
        extra = [pltpu.VMEM((2, HIDDEN, HIDDEN), jnp.bfloat16), pltpu.VMEM(part, jnp.float32), dma((2,)), dma((2,))]
    return pl.pallas_call(
        functools.partial(gather_kernel, Plan(len(args), items, order, tokens)),
        out_shape=shapes,
        in_specs=[hbm] * len(args),
        out_specs=[hbm] * len(shapes),
        scratch_shapes=[pltpu.VMEM(item.shape, item.dtype) for item in items] + extra
        + [dma((n,)), flat, flat, flat, dma((n, 4, 2)), dma((n, 4, 4)), flat, flat, flat, flat, flat, flat, dma((n, 4, 4)), dma((n, 4, CORES))],
        compiler_params=pltpu.CompilerParams(collective_id=collective_id, has_side_effects=True, vmem_limit_bytes=60 * MIB if tokens else size + CORES * MIB),
        cost_estimate=pl.CostEstimate(flops=50_000_000_000, bytes_accessed=size, transcendentals=0),
        name=name,
    )(*args)


def col_slot(ref, zs, d):
    return ref.at[pl.ds(d * LANES, LANES), pl.ds(zs * BLOCK, BLOCK)]


def col_half(ref, zs, d, which):
    return ref.at[pl.ds(d * LANES + which * 64, 64), pl.ds(zs * BLOCK, BLOCK)]


def row_slot(ref, zs, d):
    return ref.at[pl.ds((zs * CORES + d) * STRIP, STRIP)]


def row_half(ref, zs, d, which):
    return ref.at[pl.ds((zs * CORES + d) * STRIP + which * HALF_STRIP, HALF_STRIP)]


def gather_weights(w_col, w_row, x_tokens, dy_tokens):
    shape = (HIDDEN, HIDDEN)
    items = [Item(shape, w_col.dtype, lambda refs, z, d, i=i: refs[0].at[i, pl.ds(d * LANES, LANES)], col_slot, col_half) for i in range(2)]
    items += [Item(shape, w_row.dtype, lambda refs, z, d, i=i: refs[1].at[i, pl.ds(d * STRIP, STRIP)], row_slot, row_half) for i in range(2)]
    return gather_call((w_col, w_row, x_tokens, dy_tokens), items, (0, 3, 2, 1), 1, 'weights', (2, 3))


def gather_results(facts, u_half, blocks):
    items = [
        Item((STRIP, 4, SYM_ROWS, BLOCK), facts.dtype, lambda refs, z, d: refs[0],
             lambda ref, zs, d: ref.at[zs * CORES + d], lambda ref, zs, d, which: ref.at[zs * CORES + d, pl.ds(2 * which, 2)]),
        Item((CORES, D_ROWS, BLOCK), facts.dtype, lambda refs, z, d: refs[1],
             lambda ref, zs, d: ref.at[d], lambda ref, zs, d, which: ref.at[d, pl.ds(which * BLOCK, BLOCK)], True),
        Item((4, BLOCK, BLOCK), facts.dtype, lambda refs, z, d: refs[2],
             lambda ref, zs, d: ref.at[:, pl.ds(d * STRIP, STRIP)], lambda ref, zs, d, which: ref.at[pl.ds(2 * which, 2), pl.ds(d * STRIP, STRIP)], True),
    ]
    return gather_call((facts, u_half, blocks), items, (1, 2, 0), 3, 'results')


def add_into(dst, src, rows):
    step = max(n for n in range(CORES, 65, CORES) if rows % n == 0)

    def body(i, carry):
        span = pl.ds(pl.multiple_of(i * step, CORES), step)
        dst[span, :] = dst[span, :] + src[span, :]
        return carry

    lax.fori_loop(0, rows // step, body, 0)


def scatter_kernel(rows, parts_ref, ends_ref, share_ref, eshare_ref, grad_ref, own, mate, one_x, one_y, two_x, two_y, up_buf, dn_buf,
                   eown, emate, eone, etwo, gland, e_sem, emate_sem, eone_sem, etwo_sem, g_sem, out2_sem,
                   own_sem, mate_send, mate_recv, x1_send, x1_recv, y1_send, y1_recv, x2_send, x2_recv, y2_send, y2_recv,
                   up_send, up_recv, dn_send, dn_recv, out_sem):
    z, y, x, c, near = torus_place()
    sub = rows // (2 * PIECES)
    eload = pltpu.make_async_copy(ends_ref.at[:, :, :, c], eown, e_sem.at[0])
    eload.start()
    loads = {}
    for k, (zd, h) in enumerate(CHUNK_ORDER):
        loads[k] = []
        for col in range(2):
            span = pl.ds(col * PIECES * sub + h * sub, sub)
            load = pltpu.make_async_copy(parts_ref.at[zd, :, :, c, span], own.at[zd, :, :, span], own_sem.at[k, col])
            load.start()
            loads[k].append(load)
    meet_neighbours(z, near)
    ematec = remote(ends_ref.at[:, :, :, 1 - c], emate, emate_sem.at[0], emate_sem.at[1], near['c'])
    ematec.start()
    eones = (remote(eown.at[0, :, 1 - x], eone.at[0], eone_sem.at[0], eone_sem.at[1], near['x']),
             remote(eown.at[1, 1 - y], eone.at[1], eone_sem.at[2], eone_sem.at[3], near['y']))
    etwos = (remote(eown.at[0, 1 - y, x], etwo.at[0], etwo_sem.at[0], etwo_sem.at[1], near['y']),
             remote(eown.at[1, y, 1 - x], etwo.at[1], etwo_sem.at[2], etwo_sem.at[3], near['x']))
    mates = {}
    for k, (zd, h) in enumerate(CHUNK_ORDER):
        mates[k] = []
        for col in range(2):
            span = pl.ds(col * PIECES * sub + h * sub, sub)
            copy = remote(parts_ref.at[zd, :, :, 1 - c, span], mate.at[zd, :, :, span], mate_send.at[k, col], mate_recv.at[k, col], near['c'])
            copy.start()
            mates[k].append(copy)

    def spans(h):
        return pl.ds(h * sub, sub), pl.ds(PIECES * sub + h * sub, sub)

    def one_copies(k):
        zd, h = CHUNK_ORDER[k]
        first, second = spans(h)
        piece = pl.ds(h * sub, sub)
        return (remote(own.at[zd, :, 1 - x, first], one_x.at[zd, :, piece], x1_send.at[k], x1_recv.at[k], near['x']),
                remote(own.at[zd, 1 - y, :, second], one_y.at[zd, :, piece], y1_send.at[k], y1_recv.at[k], near['y']))

    def two_copies(k):
        zd, h = CHUNK_ORDER[k]
        first, second = spans(h)
        piece = pl.ds(h * sub, sub)
        return (remote(own.at[zd, 1 - y, x, first], two_y.at[zd, piece], y2_send.at[k], y2_recv.at[k], near['y']),
                remote(own.at[zd, y, 1 - x, second], two_x.at[zd, piece], x2_send.at[k], x2_recv.at[k], near['x']))

    def z_copies(k):
        zd, h = CHUNK_ORDER[k]
        out = []
        for col, span in enumerate(spans(h)):
            out.append((remote(own.at[zd, y, x, span], up_buf.at[zd, span], dn_send.at[k, col], up_recv.at[k, col], near['dn']),
                        remote(own.at[zd, y, x, span], dn_buf.at[zd, span], up_send.at[k, col], dn_recv.at[k, col], near['up'])))
        return out

    def step_a(k):
        zd, h = CHUNK_ORDER[k]
        first, second = spans(h)
        ones = one_copies(k)
        loads[k][0].wait()
        mates[k][0].wait_recv()
        for yy in range(2):
            add_into(own.at[zd, yy, 1 - x, first], mate.at[zd, yy, 1 - x, first], sub)
        ones[0].start()
        loads[k][1].wait()
        mates[k][1].wait_recv()
        for xx in range(2):
            add_into(own.at[zd, 1 - y, xx, second], mate.at[zd, 1 - y, xx, second], sub)
        ones[1].start()
        for yy in range(2):
            add_into(own.at[zd, yy, x, first], mate.at[zd, yy, x, first], sub)
        for xx in range(2):
            add_into(own.at[zd, y, xx, second], mate.at[zd, y, xx, second], sub)

    def step_b(k):
        zd, h = CHUNK_ORDER[k]
        first, second = spans(h)
        piece = pl.ds(h * sub, sub)
        ones, twos = one_copies(k), two_copies(k)
        ones[0].wait_recv()
        add_into(own.at[zd, 1 - y, x, first], one_x.at[zd, 1 - y, piece], sub)
        twos[0].start()
        ones[1].wait_recv()
        add_into(own.at[zd, y, 1 - x, second], one_y.at[zd, 1 - x, piece], sub)
        twos[1].start()
        add_into(own.at[zd, y, x, first], one_x.at[zd, y, piece], sub)
        add_into(own.at[zd, y, x, second], one_y.at[zd, x, piece], sub)

    def step_c(k):
        zd, h = CHUNK_ORDER[k]
        first, second = spans(h)
        piece = pl.ds(h * sub, sub)
        twos = two_copies(k)
        zcs = z_copies(k)
        for col, (copy, buf, span) in enumerate(((twos[0], two_y, first), (twos[1], two_x, second))):
            copy.wait_recv()
            add_into(own.at[zd, y, x, span], buf.at[zd, piece], sub)

            @pl.when((z < 3) & (z >= zd))
            def _(col=col, span=span):
                zcs[col][0].wait_recv()
                add_into(own.at[zd, y, x, span], up_buf.at[zd, span], sub)

            @pl.when((z > 0) & (z <= zd))
            def _(col=col, span=span):
                zcs[col][1].wait_recv()
                add_into(own.at[zd, y, x, span], dn_buf.at[zd, span], sub)
            pl.when(z > zd)(lambda: zcs[col][0].start())
            pl.when(z < zd)(lambda: zcs[col][1].start())

            @pl.when(z == zd)
            def _(col=col, span=span):
                pltpu.make_async_copy(own.at[zd, y, x, span], share_ref.at[span], out_sem.at[h, col]).start()

    def ends_a():
        eload.wait()
        ematec.wait_recv()
        for mat in range(2):
            for yy in range(2):
                for xx in range(2):
                    add_into(eown.at[mat, yy, xx], emate.at[mat, yy, xx], SYM_ROWS)
            eones[mat].start()

    def ends_b():
        eones[0].wait_recv()
        for yy in range(2):
            add_into(eown.at[0, yy, x], eone.at[0, yy], SYM_ROWS)
        etwos[0].start()
        eones[1].wait_recv()
        for xx in range(2):
            add_into(eown.at[1, y, xx], eone.at[1, xx], SYM_ROWS)
        etwos[1].start()

    def ends_c():
        for mat in range(2):
            etwos[mat].wait_recv()
            add_into(eown.at[mat, y, x], etwo.at[mat], SYM_ROWS)
            pltpu.make_async_copy(eown.at[mat, y, x], eshare_ref.at[mat], out2_sem.at[mat]).start()

    n = len(CHUNK_ORDER)
    ends_a()
    for step in range(n + 3):
        if step == 1:
            ends_b()
        if step == 2:
            ends_c()
        if step < n:
            step_a(step)
        if 0 <= step - 1 < n:
            step_b(step - 1)
        if 0 <= step - 3 < n:
            step_c(step - 3)
    mine = own.at[z, y, x, pl.ds(0, D_ROWS)]
    gcopy = remote(mine, gland, g_sem.at[0], g_sem.at[1], near['c'])
    gcopy.start()
    gout = pltpu.make_async_copy(mine, grad_ref.at[c], out2_sem.at[2])
    gout.start()
    gcopy.wait_recv()
    gmate = pltpu.make_async_copy(gland, grad_ref.at[1 - c], out2_sem.at[3])
    gmate.start()
    for copy in (ematec, gcopy) + eones + etwos:
        copy.wait_send()
    for k, (zd, h) in enumerate(CHUNK_ORDER):
        for copy in mates[k] + list(one_copies(k)) + list(two_copies(k)):
            copy.wait_send()
        for col, (down, up) in enumerate(z_copies(k)):
            pl.when(z > zd)(lambda: down.wait_send())
            pl.when(z < zd)(lambda: up.wait_send())
    for h in range(PIECES):
        for col in range(2):
            span = spans(h)[col]
            pltpu.make_async_copy(own.at[0, y, x, span], share_ref.at[span], out_sem.at[h, col]).wait()
    for mat in range(2):
        pltpu.make_async_copy(eown.at[mat, y, x], eshare_ref.at[mat], out2_sem.at[mat]).wait()
    gout.wait()
    gmate.wait()


def scatter_call(parts, ends, collective_id, name):
    rows = parts.shape[-2]
    half = rows // 2
    f32 = jnp.float32
    dma = pltpu.SemaphoreType.DMA
    n = len(CHUNK_ORDER)
    whole = pltpu.VMEM((4, 2, 2, rows, BLOCK), f32)
    one_buf = pltpu.VMEM((4, 2, half, BLOCK), f32)
    two_buf = pltpu.VMEM((4, half, BLOCK), f32)
    z_buf = pltpu.VMEM((4, rows, BLOCK), f32)
    e_buf = pltpu.VMEM((2, 2, 2, SYM_ROWS, BLOCK), f32)
    hbm = pl.BlockSpec(memory_space=pltpu.HBM)
    return pl.pallas_call(
        functools.partial(scatter_kernel, rows),
        out_shape=[jax.ShapeDtypeStruct((rows, BLOCK), f32), jax.ShapeDtypeStruct((2, SYM_ROWS, BLOCK), f32), jax.ShapeDtypeStruct((2, D_ROWS, BLOCK), f32)],
        in_specs=[hbm] * 2,
        out_specs=[hbm] * 3,
        scratch_shapes=[whole, whole, one_buf, one_buf, two_buf, two_buf, z_buf, z_buf,
                        e_buf, e_buf, pltpu.VMEM((2, 2, SYM_ROWS, BLOCK), f32), pltpu.VMEM((2, SYM_ROWS, BLOCK), f32), pltpu.VMEM((D_ROWS, BLOCK), f32),
                        dma((1,)), dma((2,)), dma((4,)), dma((4,)), dma((2,)), dma((4,))]
        + [dma((n, 2))] * 3 + [dma((n,))] * CORES + [dma((n, 2))] * 4 + [dma((PIECES, 2))],
        compiler_params=pltpu.CompilerParams(collective_id=collective_id, has_side_effects=True, vmem_limit_bytes=60 * MIB),
        cost_estimate=pl.CostEstimate(flops=120_000_000_000, bytes_accessed=60 * MIB, transcendentals=0),
        name=name,
    )(parts.reshape(4, 2, 2, 2, rows, BLOCK), ends.reshape(2, 2, 2, 2, SYM_ROWS, BLOCK))


def mirror_kernel(in_ref, a_ref, s_ref):
    def block(i, j, mat):
        def take(plane, at, size):
            return in_ref[plane, :, mat, pl.ds(at, size)].reshape(CORES * size, BLOCK)

        if i == j:
            return take(j, 0, STRIP)
        if i == (j + 1) % 4:
            return take(j, STRIP, STRIP)
        if j == (i + 1) % 4:
            return take(i, STRIP, STRIP).T
        low = min(i, j)
        both = jnp.concatenate([take(low, 64, HALF_STRIP), take(low + 2, 64, HALF_STRIP)], axis=0)
        return both if i > j else both.T

    for i in range(4):
        @pl.when(pl.program_id(1) == i)
        def _(i=i):
            for mat, out in enumerate((a_ref, s_ref)):
                for j in range(4):
                    out[0, :, pl.ds(j * BLOCK, BLOCK)] = block(i, j, mat)


def mirror_call(facts):
    full = jax.ShapeDtypeStruct((2, HIDDEN, HIDDEN), facts.dtype)
    out_spec = pl.BlockSpec((1, BLOCK, HIDDEN), lambda k, i: (k, i, 0))
    return pl.pallas_call(
        mirror_kernel,
        grid=(2, 4),
        out_shape=[full, full],
        in_specs=[pl.BlockSpec((4, CORES, 2, SYM_ROWS, BLOCK), lambda k, i: (0, 0, k, 0, 0))],
        out_specs=[out_spec, out_spec],
        compiler_params=pltpu.CompilerParams(vmem_limit_bytes=STRIP * MIB),
        cost_estimate=pl.CostEstimate(flops=10_000_000_000, bytes_accessed=26 * MIB, transcendentals=0),
        name='mirror',
    )(facts.reshape(4, CORES, 4, SYM_ROWS, BLOCK))


def solution(mesh):
    data_ways = mesh.shape['data']
    model_ways = mesh.shape['model']

    def shard_body(x_tokens, dy_tokens, w_col, w_row, a_old_col, s_old_col, a_old_row, s_old_row, a_inv_col, s_inv_col, a_inv_row, s_inv_row):
        model_id = lax.axis_index('model')
        data_id = lax.axis_index('data')
        inv_rows = 1.0 / (x_tokens.shape[0] * data_ways)
        w_one, w_three, w_two, w_four, ends = gather_weights(w_col, w_row, x_tokens, dy_tokens)
        rows_dev = x_tokens.shape[0] // model_ways
        x_loc = lax.dynamic_slice(x_tokens, (rows_dev * model_id, 0), (rows_dev, HIDDEN))
        dy_loc = lax.dynamic_slice(dy_tokens, (rows_dev * model_id, 0), (rows_dev, HIDDEN))
        z_one = matmul(x_loc, w_one).astype(jnp.bfloat16)
        h_one = activate(z_one)
        z_two = matmul(h_one, w_two).astype(jnp.bfloat16)
        h_two = activate(z_two)
        z_three = matmul(h_two, w_three).astype(jnp.bfloat16)
        h_three = activate(z_three)
        g_three = back_gate(matmul_nt(dy_loc, w_four).astype(jnp.bfloat16), z_three)
        g_two = back_gate(matmul_nt(g_three, w_three).astype(jnp.bfloat16), z_two)
        g_one = back_gate(matmul_nt(g_two, w_two).astype(jnp.bfloat16), z_one)
        parts = gram_call(x_loc, g_one, g_two, h_one, h_two, g_three, dy_loc, h_three)
        share, eshare, grad_mat = scatter_call(parts, ends, 2, 'sums')
        keep = 1.0 - FACTOR_DECAY
        low = lax.rem(model_id, 2)
        spots = ((model_id * BLOCK + STRIP * data_id, model_id * BLOCK, STRIP),
                 (lax.rem(model_id + 1, 4) * BLOCK + STRIP * data_id, model_id * BLOCK, STRIP),
                 ((low + 2) * BLOCK + model_id // 2 * LANES + HALF_STRIP * data_id, low * BLOCK, HALF_STRIP))
        olds = [jnp.concatenate([lax.dynamic_slice(old, (0, at, col), (2, size, BLOCK)) for at, col, size in spots], axis=1) for old in (a_old_col, s_old_row)]
        mids = share[FULL_BASE:BLOCK_BASE].reshape(2, SYM_ROWS, BLOCK)
        sums = jnp.stack([eshare[0], mids[1], mids[0], eshare[1]])
        facts = FACTOR_DECAY * jnp.stack(olds, axis=1).reshape(4, SYM_ROWS, BLOCK) + keep * inv_rows * sums
        grad_mat = grad_mat.reshape(HIDDEN, BLOCK) * inv_rows
        layer_id = data_id // 2
        stack_id = layer_id // 2
        is_col = lax.rem(layer_id, 2) == 0
        half_at = lax.rem(data_id, 2) * D_ROWS
        full_inv = jnp.where(is_col, *[lax.dynamic_slice(inv, (stack_id, half_at, 0), (1, D_ROWS, HIDDEN))[0] for inv in (a_inv_col, s_inv_row)])
        block_inv = jnp.where(is_col, *[lax.dynamic_slice(inv, (stack_id, 0, 0), (1, BLOCK, BLOCK))[0] for inv in (s_inv_col, a_inv_row)])
        u_half = exact_dot(exact_dot(full_inv, grad_mat), block_inv)
        old_blocks = jnp.concatenate([lax.dynamic_slice(old, (0, STRIP * data_id, 0), (2, STRIP, BLOCK)) for old in (s_old_col, a_old_row)])
        new_blocks = jnp.swapaxes(share[BLOCK_BASE:].reshape(2, 2, STRIP, BLOCK), 0, 1).reshape(4, STRIP, BLOCK)
        blocks = FACTOR_DECAY * old_blocks + keep * inv_rows * new_blocks
        fact_all, u_all, blk_all = gather_results(facts, u_half, blocks)
        a_new_col, s_new_row = mirror_call(fact_all)
        u_all = u_all.reshape(2, 2, HIDDEN, BLOCK)
        u_col = u_all[:, 0]
        u_row = jnp.swapaxes(u_all[:, 1], 1, 2)
        return (u_col, u_row, a_new_col, blk_all[:2], blk_all[2:], s_new_row)

    batch_split = P('data', None)
    col_split = P(None, None, 'model')
    row_split = P(None, 'model', None)
    replicated = P()
    return jax.shard_map(
        shard_body,
        mesh=mesh,
        in_specs=(batch_split, batch_split, col_split, row_split, replicated, row_split, row_split, replicated, replicated, row_split, row_split, replicated),
        out_specs=(col_split, row_split, replicated, row_split, row_split, replicated),
        check_vma=False,
    )
```

```python
import functools
import math
import jax
import jax.numpy as jnp
from jax import lax
from jax.sharding import PartitionSpec as P
from jax.experimental import pallas as pl
from jax.experimental.pallas import tpu as pltpu

FACTOR_DECAY = 0.8
GELU_SCALE = math.sqrt(2.0 / math.pi)
GELU_CUBIC = 0.044715
EXACT = lax.Precision.HIGHEST
TN_DIMS = (((0,), (0,)), ((), ()))
NT_DIMS = (((1,), (1,)), ((), ()))
BOTH = ('model', 'data')


def gelu_value(pre_act):
    tanh_arg = GELU_SCALE * (pre_act + GELU_CUBIC * pre_act * pre_act * pre_act)
    return 0.5 * pre_act * (1.0 + jnp.tanh(tanh_arg))


def gelu_slope(pre_act):
    tanh_arg = GELU_SCALE * (pre_act + GELU_CUBIC * pre_act * pre_act * pre_act)
    tanh_val = jnp.tanh(tanh_arg)
    return 0.5 * (1.0 + tanh_val) + 0.5 * pre_act * (1.0 - tanh_val * tanh_val) * GELU_SCALE * (1.0 + 3.0 * GELU_CUBIC * pre_act * pre_act)


def activate(pre_act):
    return gelu_value(pre_act.astype(jnp.float32)).astype(jnp.bfloat16)


def back_gate(grad_act, pre_act):
    return (grad_act.astype(jnp.float32) * gelu_slope(pre_act.astype(jnp.float32))).astype(jnp.bfloat16)


def matmul(left_mat, right_mat):
    return jnp.dot(left_mat, right_mat, preferred_element_type=jnp.float32)


def matmul_tn(left_mat, right_mat):
    return lax.dot_general(left_mat, right_mat, TN_DIMS, preferred_element_type=jnp.float32)


def matmul_nt(left_mat, right_mat):
    return lax.dot_general(left_mat, right_mat, NT_DIMS, preferred_element_type=jnp.float32)


def exact_dot(left_mat, right_mat):
    return jnp.dot(left_mat, right_mat, precision=EXACT, preferred_element_type=jnp.float32)


MIB = 1024 * 1024
BLOCK = 256
HIDDEN = 1024
D_ROWS = 512
SYM_ROWS = 80
FULL_BASE = 512
BLOCK_BASE = 672
SHARE_ROWS = 800
LANES = 128
STRIP = 32
HALF_STRIP = 16
CORES = 8


def gram_kernel(x_ref, g1_ref, g2_ref, h1_ref, h2_ref, g3_ref, dy_ref, h3_ref, out_ref,
                act, stage, bstage, fstage, in_sem, out_sem, b_sem, f_sem):
    sources = [dy_ref, h3_ref, h2_ref, g3_ref, g2_ref, h1_ref, x_ref, g1_ref]
    slots = [3, 7, 2, 6, 1, 5, 0, 4]
    loads = [pltpu.make_async_copy(src, act.at[slot], in_sem.at[slot]) for src, slot in zip(sources, slots)]
    for load in loads:
        load.start()

    def out_copy(slot, dst):
        return pltpu.make_async_copy(stage.at[slot], dst, out_sem.at[slot])

    def f_copy(slot, n, which):
        return pltpu.make_async_copy(fstage.at[slot], out_ref.at[pl.ds(n * CORES, CORES), pl.ds(FULL_BASE + which * SYM_ROWS, SYM_ROWS)], f_sem.at[slot])

    for layer in (3, 2, 1, 0):
        pltpu.make_async_copy(x_ref, act.at[layer], in_sem.at[layer]).wait()
        pltpu.make_async_copy(x_ref, act.at[4 + layer], in_sem.at[4 + layer]).wait()

        def d_body(m, carry, layer=layer):
            slot = lax.rem(m, 2)
            cols = pl.ds(pl.multiple_of(m * BLOCK, BLOCK), BLOCK)
            right = act[4 + layer, :, cols]
            dst = out_ref.at[pl.ds(m * CORES + 2 * layer, 2), pl.ds(0, D_ROWS)]

            if layer == 3:
                @pl.when(m >= 2)
                def _():
                    out_copy(slot, dst).wait()
                    pltpu.make_async_copy(bstage.at[slot], out_ref.at[pl.ds(0, CORES), pl.ds(BLOCK_BASE, STRIP)], b_sem.at[slot]).wait()
            else:
                out_copy(slot, dst).wait()
                pltpu.make_async_copy(bstage.at[slot], out_ref.at[pl.ds(0, CORES), pl.ds(BLOCK_BASE, STRIP)], b_sem.at[slot]).wait()
            prod = lax.dot_general(act[layer], right, TN_DIMS, preferred_element_type=jnp.float32)
            stage[slot] = prod.reshape(2, D_ROWS, BLOCK)
            out_copy(slot, dst).start()
            blk = lax.dot_general(right, right, TN_DIMS, preferred_element_type=jnp.float32)
            bstage[slot] = blk.reshape(CORES, STRIP, BLOCK)
            pltpu.make_async_copy(bstage.at[slot], out_ref.at[pl.ds(m * CORES, CORES), pl.ds(BLOCK_BASE + STRIP * layer, STRIP)], b_sem.at[slot]).start()
            return carry

        lax.fori_loop(0, 4, d_body, 0)

        if layer in (2, 1):
            which = 0 if layer == 2 else 1

            def f_body(n, carry, layer=layer, which=which):
                slot = lax.rem(n, 2)
                if which == 0:
                    pl.when(n >= 2)(lambda: f_copy(slot, n, which).wait())
                else:
                    f_copy(slot, n, which).wait()
                put_sym(fstage.at[slot], sym_blocks(act.at[layer], n), False)
                f_copy(slot, n, which).start()
                return carry

            lax.fori_loop(0, 4, f_body, 0)
    for slot in range(2):
        f_copy(slot, 0, 0).wait()
        pltpu.make_async_copy(stage.at[slot], out_ref.at[pl.ds(0, 2), pl.ds(0, D_ROWS)], out_sem.at[slot]).wait()
        pltpu.make_async_copy(bstage.at[slot], out_ref.at[pl.ds(0, CORES), pl.ds(BLOCK_BASE, STRIP)], b_sem.at[slot]).wait()


def gram_call(x_loc, g_one, g_two, h_one, h_two, g_three, dy_loc, h_three):
    any_spec = pl.BlockSpec(memory_space=pl.ANY)
    return pl.pallas_call(
        gram_kernel,
        out_shape=jax.ShapeDtypeStruct((STRIP, SHARE_ROWS, BLOCK), jnp.float32),
        in_specs=[any_spec] * CORES,
        out_specs=any_spec,
        scratch_shapes=[
            pltpu.VMEM((CORES, HIDDEN, HIDDEN), jnp.bfloat16),
            pltpu.VMEM((2, 2, D_ROWS, BLOCK), jnp.float32),
            pltpu.VMEM((2, CORES, STRIP, BLOCK), jnp.float32),
            pltpu.VMEM((2, CORES, SYM_ROWS, BLOCK), jnp.float32),
            pltpu.SemaphoreType.DMA((CORES,)),
            pltpu.SemaphoreType.DMA((2,)),
            pltpu.SemaphoreType.DMA((2,)),
            pltpu.SemaphoreType.DMA((2,)),
        ],
        compiler_params=pltpu.CompilerParams(vmem_limit_bytes=48 * HIDDEN * HIDDEN),
        cost_estimate=pl.CostEstimate(flops=15_000_000_000, bytes_accessed=46_000_000, transcendentals=0),
        name='gram',
    )(x_loc, g_one, g_two, h_one, h_two, g_three, dy_loc, h_three)


MESH_ID = pl.DeviceIdType.MESH
PIECES = 5
FAR = 3
CHUNK_ORDER = tuple((zd, h) for pair in ((0, 3), (1, 2)) for h in range(PIECES) for zd in pair)


def torus_place():
    z = lax.axis_index('model')
    d = lax.axis_index('data')
    y = d // 4
    x = (d // 2) % 2
    c = d % 2
    near = {'x': (z, d + 2 - 4 * x), 'y': (z, d + 4 - CORES * y), 'c': (z, d + 1 - 2 * c), 'up': (z + 1, d), 'dn': (z - 1, d)}
    return z, y, x, c, near


def meet_neighbours(z, near):
    barrier = pltpu.get_barrier_semaphore()
    for side in ('x', 'y', 'c'):
        pl.semaphore_signal(barrier, inc=1, device_id=near[side], device_id_type=MESH_ID)

    @pl.when(z < 3)
    def _():
        pl.semaphore_signal(barrier, inc=1, device_id=near['up'], device_id_type=MESH_ID)

    @pl.when(z > 0)
    def _():
        pl.semaphore_signal(barrier, inc=1, device_id=near['dn'], device_id_type=MESH_ID)
    pl.semaphore_wait(barrier, 3 + (z + 3) // 4 + (6 - z) // 4)


def remote(src, dst, send_sem, recv_sem, where):
    return pltpu.make_async_remote_copy(src_ref=src, dst_ref=dst, send_sem=send_sem, recv_sem=recv_sem, device_id=where, device_id_type=MESH_ID)


def sym_blocks(left, n):
    def cols(at, size):
        return left[:, pl.ds(pl.multiple_of(at, LANES), size)]

    low = n % 2
    right = cols(n * BLOCK, BLOCK)
    pairs = ((right, right, STRIP), (cols((n + 1) % 4 * BLOCK, BLOCK), right, STRIP),
             (cols((low + 2) * BLOCK + n // 2 * LANES, LANES), cols(low * BLOCK, BLOCK), HALF_STRIP))
    return [lax.dot_general(a, b, TN_DIMS, preferred_element_type=jnp.float32).reshape(CORES, rows, BLOCK) for a, b, rows in pairs]


def put_sym(dst, blocks, more):
    at = 0
    for blk in blocks:
        span = pl.ds(at, blk.shape[1])
        dst[:, span] = dst[:, span] + blk if more else blk
        at += blk.shape[1]


def gather_kernel(plan, *refs):
    n = len(plan.items)
    pieces, refs = refs[:plan.n_in], refs[plan.n_in:]
    outs, refs = refs[:n], refs[n:]
    ends = len(plan.tokens) > 0
    if ends:
        ends_ref, refs = refs[0], refs[1:]
    lands, refs = refs[:n], refs[n:]
    if ends:
        tok, acc, tok_sem, acc_sem, *refs = refs
    load_sem, z_recv, x_recv, y_recv, d_recv, c_recv, up_send, dn_send, x_send, y_send, dy_send, dx_send, c_send, flush_sem = refs
    z, y, x, c, near = torus_place()

    def slot(ref, j, zs, yy, xx, cc):
        return plan.items[j].slot(ref, zs, 4 * yy + 2 * xx + cc)

    def view(j, zs, yy, xx, cc):
        return slot(lands[j], j, zs, yy, xx, cc)

    def half(j, zs, yy, xx, cc, which):
        return plan.items[j].half(lands[j], zs, 4 * yy + 2 * xx + cc, which)

    def flush(j, zs, yy, xx, cc, index):
        return pltpu.make_async_copy(view(j, zs, yy, xx, cc), slot(outs[j], j, zs, yy, xx, cc), flush_sem.at[j, zs, index])

    loads = [pltpu.make_async_copy(item.piece(pieces, z, 4 * y + 2 * x + c), view(j, z, y, x, c), load_sem.at[j]) for j, item in enumerate(plan.items)]
    for load in loads:
        load.start()

    def tok_load(t):
        src = pieces[plan.tokens[t // 4]].at[pl.ds(t % 4 * HIDDEN, HIDDEN)]
        return pltpu.make_async_copy(src, tok.at[t % 2], tok_sem.at[t % 2])

    def ends_out(mat):
        return pltpu.make_async_copy(acc.at[mat], ends_ref.at[mat], acc_sem.at[mat])

    def ends_step(t):
        tok_load(t).wait()
        put_sym(acc.at[t // 4], sym_blocks(tok.at[t % 2], z), t % 4 > 0)
        if t + 2 < CORES:
            tok_load(t + 2).start()
        if t % 4 == 3:
            ends_out(t // 4).start()

    todo = list(range(CORES)) if ends else []
    if ends:
        tok_load(0).start()
        tok_load(1).start()
    meet_neighbours(z, near)

    def side_copy(j, zs, side):
        send, recv = {'x': (x_send, x_recv), 'y': (y_send, y_recv), 'up': (up_send, z_recv), 'dn': (dn_send, z_recv)}[side]
        return remote(view(j, zs, y, x, c), view(j, zs, y, x, c), send.at[j, zs], recv.at[j, zs], near[side])

    def from_side(j, zs, side):
        yy, xx = (y, 1 - x) if side == 'x' else (1 - y, x)
        send, recv = {'x': (x_send, x_recv), 'y': (y_send, y_recv)}[side]
        return remote(view(j, zs, yy, xx, c), view(j, zs, yy, xx, c), send.at[j, zs], recv.at[j, zs], near[side])

    def dy_copy(j, zs):
        return remote(half(j, zs, y, 1 - x, c, 0), half(j, zs, y, 1 - x, c, 0), dy_send.at[j, zs], d_recv.at[j, zs, 0], near['y'])

    def dx_copy(j, zs):
        return remote(half(j, zs, 1 - y, x, c, 1), half(j, zs, 1 - y, x, c, 1), dx_send.at[j, zs], d_recv.at[j, zs, 1], near['x'])

    def kind_place(kind):
        return (y if kind < 2 else 1 - y), (x if kind % 2 == 0 else 1 - x)

    def c_copy(j, zs, kind):
        yy, xx = kind_place(kind)
        return remote(view(j, zs, yy, xx, c), view(j, zs, yy, xx, c), c_send.at[j, zs, kind], c_recv.at[j, zs, kind], near['c'])

    def share_core(j, zs, kind):
        yy, xx = kind_place(kind)
        c_copy(j, zs, kind).start()
        flush(j, zs, yy, xx, c, kind).start()

    def guard(off, body):
        if off == 0:
            body(z)
        elif off < 0:
            pl.when(z >= -off)(lambda: body(z + off))
        else:
            pl.when(z <= 3 - off)(lambda: body(z + off))

    def z_step(j, off):
        def body(zs):
            if off == 0:
                loads[j].wait()
            else:
                side_copy(j, zs, 'up').wait_recv()
            if off <= 0 and not plan.items[j].plane:
                pl.when(z < 3)(lambda: side_copy(j, zs, 'up').start())
            if off >= 0 and not plan.items[j].plane:
                pl.when(z > 0)(lambda: side_copy(j, zs, 'dn').start())
            side_copy(j, zs, 'x').start()
            side_copy(j, zs, 'y').start()
            share_core(j, zs, 0)
        guard(off, body)

    def xy_step(j, off):
        def body(zs):
            from_side(j, zs, 'x').wait_recv()
            dy_copy(j, zs).start()
            share_core(j, zs, 1)
            from_side(j, zs, 'y').wait_recv()
            dx_copy(j, zs).start()
            share_core(j, zs, 2)
        guard(off, body)

    def diag_step(j, off):
        def body(zs):
            for which in range(2):
                remote(half(j, zs, 1 - y, 1 - x, c, which), half(j, zs, 1 - y, 1 - x, c, which), dy_send.at[j, zs], d_recv.at[j, zs, which], near['y']).wait_recv()
            share_core(j, zs, 3)
        guard(off, body)

    def core_step(j, off):
        def body(zs):
            for kind in range(4):
                yy, xx = kind_place(kind)
                remote(view(j, zs, yy, xx, 1 - c), view(j, zs, yy, xx, 1 - c), c_send.at[j, zs, kind], c_recv.at[j, zs, kind], near['c']).wait_recv()
                flush(j, zs, yy, xx, 1 - c, 4 + kind).start()
        guard(off, body)

    def last_step(j, off):
        def body(zs):
            for kind in range(4):
                yy, xx = kind_place(kind)
                c_copy(j, zs, kind).wait_send()
                flush(j, zs, yy, xx, c, kind).wait()
                flush(j, zs, yy, xx, 1 - c, 4 + kind).wait()
            side_copy(j, zs, 'x').wait_send()
            side_copy(j, zs, 'y').wait_send()
            dy_copy(j, zs).wait_send()
            dx_copy(j, zs).wait_send()
            if off <= 0 and not plan.items[j].plane:
                pl.when(z < 3)(lambda: side_copy(j, zs, 'up').wait_send())
            if off >= 0 and not plan.items[j].plane:
                pl.when(z > 0)(lambda: side_copy(j, zs, 'dn').wait_send())
        guard(off, body)

    waves = [[(j, 0) for j in plan.order]]
    for far in range(1, 4):
        waves.append([(j, sign * far) for j in plan.order if not plan.items[j].plane for sign in (-1, 1)])
    for step in range(7):
        for func, lag in ((z_step, 0), (xy_step, 1), (diag_step, 2), (core_step, 3)):
            if 0 <= step - lag < 4:
                for j, off in waves[step - lag]:
                    func(j, off)
                if todo and step >= 3 and lag:
                    ends_step(todo.pop(0))
    for t in todo:
        ends_step(t)
    if ends:
        ends_out(0).wait()
        ends_out(1).wait()
    for wave in waves:
        for j, off in wave:
            last_step(j, off)


class Item:
    def __init__(self, shape, dtype, piece, slot, half, plane=False):
        self.shape, self.dtype, self.piece, self.slot, self.half, self.plane = shape, dtype, piece, slot, half, plane


class Plan:
    def __init__(self, n_in, items, order, tokens):
        self.n_in, self.items, self.order, self.tokens = n_in, items, order, tokens


def gather_call(args, items, order, collective_id, name, tokens=()):
    n = len(items)
    dma = pltpu.SemaphoreType.DMA
    size = sum(math.prod(item.shape) * jnp.dtype(item.dtype).itemsize for item in items)
    hbm = pl.BlockSpec(memory_space=pltpu.HBM)
    flat = dma((n, 4))
    shapes = [jax.ShapeDtypeStruct(item.shape, item.dtype) for item in items]
    extra = []
    if tokens:
        part = (2, CORES, SYM_ROWS, BLOCK)
        shapes.append(jax.ShapeDtypeStruct(part, jnp.float32))
        extra = [pltpu.VMEM((2, HIDDEN, HIDDEN), jnp.bfloat16), pltpu.VMEM(part, jnp.float32), dma((2,)), dma((2,))]
    return pl.pallas_call(
        functools.partial(gather_kernel, Plan(len(args), items, order, tokens)),
        out_shape=shapes,
        in_specs=[hbm] * len(args),
        out_specs=[hbm] * len(shapes),
        scratch_shapes=[pltpu.VMEM(item.shape, item.dtype) for item in items] + extra
        + [dma((n,)), flat, flat, flat, dma((n, 4, 2)), dma((n, 4, 4)), flat, flat, flat, flat, flat, flat, dma((n, 4, 4)), dma((n, 4, CORES))],
        compiler_params=pltpu.CompilerParams(collective_id=collective_id, has_side_effects=True, vmem_limit_bytes=60 * MIB if tokens else size + CORES * MIB),
        cost_estimate=pl.CostEstimate(flops=50_000_000_000, bytes_accessed=size, transcendentals=0),
        name=name,
    )(*args)


def col_slot(ref, zs, d):
    return ref.at[pl.ds(d * LANES, LANES), pl.ds(zs * BLOCK, BLOCK)]


def col_half(ref, zs, d, which):
    return ref.at[pl.ds(d * LANES + which * 64, 64), pl.ds(zs * BLOCK, BLOCK)]


def row_slot(ref, zs, d):
    return ref.at[pl.ds((zs * CORES + d) * STRIP, STRIP)]


def row_half(ref, zs, d, which):
    return ref.at[pl.ds((zs * CORES + d) * STRIP + which * HALF_STRIP, HALF_STRIP)]


def gather_weights(w_col, w_row, x_tokens, dy_tokens):
    shape = (HIDDEN, HIDDEN)
    items = [Item(shape, w_col.dtype, lambda refs, z, d, i=i: refs[0].at[i, pl.ds(d * LANES, LANES)], col_slot, col_half) for i in range(2)]
    items += [Item(shape, w_row.dtype, lambda refs, z, d, i=i: refs[1].at[i, pl.ds(d * STRIP, STRIP)], row_slot, row_half) for i in range(2)]
    return gather_call((w_col, w_row, x_tokens, dy_tokens), items, (0, 3, 2, 1), 1, 'weights', (2, 3))


def gather_results(facts, u_half, blocks):
    items = [
        Item((STRIP, 4, SYM_ROWS, BLOCK), facts.dtype, lambda refs, z, d: refs[0],
             lambda ref, zs, d: ref.at[zs * CORES + d], lambda ref, zs, d, which: ref.at[zs * CORES + d, pl.ds(2 * which, 2)]),
        Item((CORES, D_ROWS, BLOCK), facts.dtype, lambda refs, z, d: refs[1],
             lambda ref, zs, d: ref.at[d], lambda ref, zs, d, which: ref.at[d, pl.ds(which * BLOCK, BLOCK)], True),
        Item((4, BLOCK, BLOCK), facts.dtype, lambda refs, z, d: refs[2],
             lambda ref, zs, d: ref.at[:, pl.ds(d * STRIP, STRIP)], lambda ref, zs, d, which: ref.at[pl.ds(2 * which, 2), pl.ds(d * STRIP, STRIP)], True),
    ]
    return gather_call((facts, u_half, blocks), items, (1, 2, 0), 3, 'results')


def add_into(dst, src, rows):
    step = max(n for n in range(CORES, 65, CORES) if rows % n == 0)

    def body(i, carry):
        span = pl.ds(pl.multiple_of(i * step, CORES), step)
        dst[span, :] = dst[span, :] + src[span, :]
        return carry

    lax.fori_loop(0, rows // step, body, 0)


def scatter_kernel(rows, parts_ref, ends_ref, share_ref, eshare_ref, grad_ref, own, mate, one_x, one_y, two_x, two_y, up_buf, dn_buf,
                   eown, emate, eone, etwo, gland, e_sem, emate_sem, eone_sem, etwo_sem, g_sem, out2_sem,
                   own_sem, mate_send, mate_recv, x1_send, x1_recv, y1_send, y1_recv, x2_send, x2_recv, y2_send, y2_recv,
                   up_send, up_recv, dn_send, dn_recv, out_sem):
    z, y, x, c, near = torus_place()
    sub = rows // (2 * PIECES)
    eload = pltpu.make_async_copy(ends_ref.at[:, :, :, c], eown, e_sem.at[0])
    eload.start()
    loads = {}
    for k, (zd, h) in enumerate(CHUNK_ORDER):
        loads[k] = []
        for col in range(2):
            span = pl.ds(col * PIECES * sub + h * sub, sub)
            load = pltpu.make_async_copy(parts_ref.at[zd, :, :, c, span], own.at[zd, :, :, span], own_sem.at[k, col])
            load.start()
            loads[k].append(load)
    meet_neighbours(z, near)
    ematec = remote(ends_ref.at[:, :, :, 1 - c], emate, emate_sem.at[0], emate_sem.at[1], near['c'])
    ematec.start()
    eones = (remote(eown.at[0, :, 1 - x], eone.at[0], eone_sem.at[0], eone_sem.at[1], near['x']),
             remote(eown.at[1, 1 - y], eone.at[1], eone_sem.at[2], eone_sem.at[3], near['y']))
    etwos = (remote(eown.at[0, 1 - y, x], etwo.at[0], etwo_sem.at[0], etwo_sem.at[1], near['y']),
             remote(eown.at[1, y, 1 - x], etwo.at[1], etwo_sem.at[2], etwo_sem.at[3], near['x']))
    mates = {}
    for k, (zd, h) in enumerate(CHUNK_ORDER):
        mates[k] = []
        for col in range(2):
            span = pl.ds(col * PIECES * sub + h * sub, sub)
            copy = remote(parts_ref.at[zd, :, :, 1 - c, span], mate.at[zd, :, :, span], mate_send.at[k, col], mate_recv.at[k, col], near['c'])
            copy.start()
            mates[k].append(copy)

    def spans(h):
        return pl.ds(h * sub, sub), pl.ds(PIECES * sub + h * sub, sub)

    def one_copies(k):
        zd, h = CHUNK_ORDER[k]
        first, second = spans(h)
        piece = pl.ds(h * sub, sub)
        return (remote(own.at[zd, :, 1 - x, first], one_x.at[zd, :, piece], x1_send.at[k], x1_recv.at[k], near['x']),
                remote(own.at[zd, 1 - y, :, second], one_y.at[zd, :, piece], y1_send.at[k], y1_recv.at[k], near['y']))

    def two_copies(k):
        zd, h = CHUNK_ORDER[k]
        first, second = spans(h)
        piece = pl.ds(h * sub, sub)
        return (remote(own.at[zd, 1 - y, x, first], two_y.at[zd, piece], y2_send.at[k], y2_recv.at[k], near['y']),
                remote(own.at[zd, y, 1 - x, second], two_x.at[zd, piece], x2_send.at[k], x2_recv.at[k], near['x']))

    def z_copies(k):
        zd, h = CHUNK_ORDER[k]
        out = []
        for col, span in enumerate(spans(h)):
            out.append((remote(own.at[zd, y, x, span], up_buf.at[zd, span], dn_send.at[k, col], up_recv.at[k, col], near['dn']),
                        remote(own.at[zd, y, x, span], dn_buf.at[zd, span], up_send.at[k, col], dn_recv.at[k, col], near['up'])))
        return out

    def step_a(k):
        zd, h = CHUNK_ORDER[k]
        first, second = spans(h)
        ones = one_copies(k)
        loads[k][0].wait()
        mates[k][0].wait_recv()
        for yy in range(2):
            add_into(own.at[zd, yy, 1 - x, first], mate.at[zd, yy, 1 - x, first], sub)
        ones[0].start()
        loads[k][1].wait()
        mates[k][1].wait_recv()
        for xx in range(2):
            add_into(own.at[zd, 1 - y, xx, second], mate.at[zd, 1 - y, xx, second], sub)
        ones[1].start()
        for yy in range(2):
            add_into(own.at[zd, yy, x, first], mate.at[zd, yy, x, first], sub)
        for xx in range(2):
            add_into(own.at[zd, y, xx, second], mate.at[zd, y, xx, second], sub)

    def step_b(k):
        zd, h = CHUNK_ORDER[k]
        first, second = spans(h)
        piece = pl.ds(h * sub, sub)
        ones, twos = one_copies(k), two_copies(k)
        ones[0].wait_recv()
        add_into(own.at[zd, 1 - y, x, first], one_x.at[zd, 1 - y, piece], sub)
        twos[0].start()
        ones[1].wait_recv()
        add_into(own.at[zd, y, 1 - x, second], one_y.at[zd, 1 - x, piece], sub)
        twos[1].start()
        add_into(own.at[zd, y, x, first], one_x.at[zd, y, piece], sub)
        add_into(own.at[zd, y, x, second], one_y.at[zd, x, piece], sub)

    def step_c(k):
        zd, h = CHUNK_ORDER[k]
        first, second = spans(h)
        piece = pl.ds(h * sub, sub)
        twos = two_copies(k)
        for copy, buf, span in ((twos[0], two_y, first), (twos[1], two_x, second)):
            copy.wait_recv()
            add_into(own.at[zd, y, x, span], buf.at[zd, piece], sub)

    def z_add(k, side, buf):
        zd, h = CHUNK_ORDER[k]
        for col, span in enumerate(spans(h)):
            z_copies(k)[col][side].wait_recv()
            add_into(own.at[zd, y, x, span], buf.at[zd, span], sub)

    def z_hop(k, hop):
        zd, h = CHUNK_ORDER[k]
        for place, side, far in ((3 - hop, 0, hop), (hop, 1, hop)):
            if (place > zd, place < zd)[side]:
                @pl.when(z == place)
                def _(side=side, far=far):
                    if far:
                        z_add(k, side, (up_buf, dn_buf)[side])
                    for pair in z_copies(k):
                        pair[side].start()
        if hop == 3:
            @pl.when(z == zd)
            def _():
                if zd < 3:
                    z_add(k, 0, up_buf)
                if zd:
                    z_add(k, 1, dn_buf)
                for col, span in enumerate(spans(h)):
                    pltpu.make_async_copy(own.at[zd, y, x, span], share_ref.at[span], out_sem.at[h, col]).start()

    def ends_a():
        eload.wait()
        ematec.wait_recv()
        for mat in range(2):
            for yy in range(2):
                for xx in range(2):
                    add_into(eown.at[mat, yy, xx], emate.at[mat, yy, xx], SYM_ROWS)
            eones[mat].start()

    def ends_b():
        eones[0].wait_recv()
        for yy in range(2):
            add_into(eown.at[0, yy, x], eone.at[0, yy], SYM_ROWS)
        etwos[0].start()
        eones[1].wait_recv()
        for xx in range(2):
            add_into(eown.at[1, y, xx], eone.at[1, xx], SYM_ROWS)
        etwos[1].start()

    def ends_c():
        for mat in range(2):
            etwos[mat].wait_recv()
            add_into(eown.at[mat, y, x], etwo.at[mat], SYM_ROWS)
            pltpu.make_async_copy(eown.at[mat, y, x], eshare_ref.at[mat], out2_sem.at[mat]).start()

    n = len(CHUNK_ORDER)
    ends_a()
    for step in range(n + 2 * FAR + 4):
        for func, lag in ((step_a, 0), (step_b, FAR), (step_c, 2 * FAR)):
            if 0 <= step - lag < n:
                func(step - lag)
        for hop in range(4):
            if 0 <= step - 2 * FAR - hop < n:
                z_hop(step - 2 * FAR - hop, hop)
        if step == 2:
            ends_b()
        if step == 4:
            ends_c()
    mine = own.at[z, y, x, pl.ds(0, D_ROWS)]
    gcopy = remote(mine, gland, g_sem.at[0], g_sem.at[1], near['c'])
    gcopy.start()
    gout = pltpu.make_async_copy(mine, grad_ref.at[c], out2_sem.at[2])
    gout.start()
    gcopy.wait_recv()
    gmate = pltpu.make_async_copy(gland, grad_ref.at[1 - c], out2_sem.at[3])
    gmate.start()
    for copy in (ematec, gcopy) + eones + etwos:
        copy.wait_send()
    for k, (zd, h) in enumerate(CHUNK_ORDER):
        for copy in mates[k] + list(one_copies(k)) + list(two_copies(k)):
            copy.wait_send()
        for col, (down, up) in enumerate(z_copies(k)):
            pl.when(z > zd)(lambda: down.wait_send())
            pl.when(z < zd)(lambda: up.wait_send())
    for h in range(PIECES):
        for col in range(2):
            span = spans(h)[col]
            pltpu.make_async_copy(own.at[0, y, x, span], share_ref.at[span], out_sem.at[h, col]).wait()
    for mat in range(2):
        pltpu.make_async_copy(eown.at[mat, y, x], eshare_ref.at[mat], out2_sem.at[mat]).wait()
    gout.wait()
    gmate.wait()


def scatter_call(parts, ends, collective_id, name):
    rows = parts.shape[-2]
    half = rows // 2
    f32 = jnp.float32
    dma = pltpu.SemaphoreType.DMA
    n = len(CHUNK_ORDER)
    whole = pltpu.VMEM((4, 2, 2, rows, BLOCK), f32)
    one_buf = pltpu.VMEM((4, 2, half, BLOCK), f32)
    two_buf = pltpu.VMEM((4, half, BLOCK), f32)
    z_buf = pltpu.VMEM((4, rows, BLOCK), f32)
    e_buf = pltpu.VMEM((2, 2, 2, SYM_ROWS, BLOCK), f32)
    hbm = pl.BlockSpec(memory_space=pltpu.HBM)
    return pl.pallas_call(
        functools.partial(scatter_kernel, rows),
        out_shape=[jax.ShapeDtypeStruct((rows, BLOCK), f32), jax.ShapeDtypeStruct((2, SYM_ROWS, BLOCK), f32), jax.ShapeDtypeStruct((2, D_ROWS, BLOCK), f32)],
        in_specs=[hbm] * 2,
        out_specs=[hbm] * 3,
        scratch_shapes=[whole, whole, one_buf, one_buf, two_buf, two_buf, z_buf, z_buf,
                        e_buf, e_buf, pltpu.VMEM((2, 2, SYM_ROWS, BLOCK), f32), pltpu.VMEM((2, SYM_ROWS, BLOCK), f32), pltpu.VMEM((D_ROWS, BLOCK), f32),
                        dma((1,)), dma((2,)), dma((4,)), dma((4,)), dma((2,)), dma((4,))]
        + [dma((n, 2))] * 3 + [dma((n,))] * CORES + [dma((n, 2))] * 4 + [dma((PIECES, 2))],
        compiler_params=pltpu.CompilerParams(collective_id=collective_id, has_side_effects=True, vmem_limit_bytes=60 * MIB),
        cost_estimate=pl.CostEstimate(flops=120_000_000_000, bytes_accessed=60 * MIB, transcendentals=0),
        name=name,
    )(parts.reshape(4, 2, 2, 2, rows, BLOCK), ends.reshape(2, 2, 2, 2, SYM_ROWS, BLOCK))


def mirror_kernel(in_ref, a_ref, s_ref):
    def block(i, j, mat):
        def take(plane, at, size):
            return in_ref[plane, :, mat, pl.ds(at, size)].reshape(CORES * size, BLOCK)

        if i == j:
            return take(j, 0, STRIP)
        if i == (j + 1) % 4:
            return take(j, STRIP, STRIP)
        if j == (i + 1) % 4:
            return take(i, STRIP, STRIP).T
        low = min(i, j)
        both = jnp.concatenate([take(low, 64, HALF_STRIP), take(low + 2, 64, HALF_STRIP)], axis=0)
        return both if i > j else both.T

    for i in range(4):
        @pl.when(pl.program_id(1) == i)
        def _(i=i):
            for mat, out in enumerate((a_ref, s_ref)):
                for j in range(4):
                    out[0, :, pl.ds(j * BLOCK, BLOCK)] = block(i, j, mat)


def mirror_call(facts):
    full = jax.ShapeDtypeStruct((2, HIDDEN, HIDDEN), facts.dtype)
    out_spec = pl.BlockSpec((1, BLOCK, HIDDEN), lambda k, i: (k, i, 0))
    return pl.pallas_call(
        mirror_kernel,
        grid=(2, 4),
        out_shape=[full, full],
        in_specs=[pl.BlockSpec((4, CORES, 2, SYM_ROWS, BLOCK), lambda k, i: (0, 0, k, 0, 0))],
        out_specs=[out_spec, out_spec],
        compiler_params=pltpu.CompilerParams(vmem_limit_bytes=STRIP * MIB),
        cost_estimate=pl.CostEstimate(flops=10_000_000_000, bytes_accessed=26 * MIB, transcendentals=0),
        name='mirror',
    )(facts.reshape(4, CORES, 4, SYM_ROWS, BLOCK))


def solution(mesh):
    data_ways = mesh.shape['data']
    model_ways = mesh.shape['model']

    def shard_body(x_tokens, dy_tokens, w_col, w_row, a_old_col, s_old_col, a_old_row, s_old_row, a_inv_col, s_inv_col, a_inv_row, s_inv_row):
        model_id = lax.axis_index('model')
        data_id = lax.axis_index('data')
        inv_rows = 1.0 / (x_tokens.shape[0] * data_ways)
        w_one, w_three, w_two, w_four, ends = gather_weights(w_col, w_row, x_tokens, dy_tokens)
        rows_dev = x_tokens.shape[0] // model_ways
        x_loc = lax.dynamic_slice(x_tokens, (rows_dev * model_id, 0), (rows_dev, HIDDEN))
        dy_loc = lax.dynamic_slice(dy_tokens, (rows_dev * model_id, 0), (rows_dev, HIDDEN))
        z_one = matmul(x_loc, w_one).astype(jnp.bfloat16)
        h_one = activate(z_one)
        z_two = matmul(h_one, w_two).astype(jnp.bfloat16)
        h_two = activate(z_two)
        z_three = matmul(h_two, w_three).astype(jnp.bfloat16)
        h_three = activate(z_three)
        g_three = back_gate(matmul_nt(dy_loc, w_four).astype(jnp.bfloat16), z_three)
        g_two = back_gate(matmul_nt(g_three, w_three).astype(jnp.bfloat16), z_two)
        g_one = back_gate(matmul_nt(g_two, w_two).astype(jnp.bfloat16), z_one)
        parts = gram_call(x_loc, g_one, g_two, h_one, h_two, g_three, dy_loc, h_three)
        share, eshare, grad_mat = scatter_call(parts, ends, 2, 'sums')
        keep = 1.0 - FACTOR_DECAY
        low = lax.rem(model_id, 2)
        spots = ((model_id * BLOCK + STRIP * data_id, model_id * BLOCK, STRIP),
                 (lax.rem(model_id + 1, 4) * BLOCK + STRIP * data_id, model_id * BLOCK, STRIP),
                 ((low + 2) * BLOCK + model_id // 2 * LANES + HALF_STRIP * data_id, low * BLOCK, HALF_STRIP))
        olds = [jnp.concatenate([lax.dynamic_slice(old, (0, at, col), (2, size, BLOCK)) for at, col, size in spots], axis=1) for old in (a_old_col, s_old_row)]
        mids = share[FULL_BASE:BLOCK_BASE].reshape(2, SYM_ROWS, BLOCK)
        sums = jnp.stack([eshare[0], mids[1], mids[0], eshare[1]])
        facts = FACTOR_DECAY * jnp.stack(olds, axis=1).reshape(4, SYM_ROWS, BLOCK) + keep * inv_rows * sums
        grad_mat = grad_mat.reshape(HIDDEN, BLOCK) * inv_rows
        layer_id = data_id // 2
        stack_id = layer_id // 2
        is_col = lax.rem(layer_id, 2) == 0
        half_at = lax.rem(data_id, 2) * D_ROWS
        full_inv = jnp.where(is_col, *[lax.dynamic_slice(inv, (stack_id, half_at, 0), (1, D_ROWS, HIDDEN))[0] for inv in (a_inv_col, s_inv_row)])
        block_inv = jnp.where(is_col, *[lax.dynamic_slice(inv, (stack_id, 0, 0), (1, BLOCK, BLOCK))[0] for inv in (s_inv_col, a_inv_row)])
        u_half = exact_dot(exact_dot(full_inv, grad_mat), block_inv)
        old_blocks = jnp.concatenate([lax.dynamic_slice(old, (0, STRIP * data_id, 0), (2, STRIP, BLOCK)) for old in (s_old_col, a_old_row)])
        new_blocks = jnp.swapaxes(share[BLOCK_BASE:].reshape(2, 2, STRIP, BLOCK), 0, 1).reshape(4, STRIP, BLOCK)
        blocks = FACTOR_DECAY * old_blocks + keep * inv_rows * new_blocks
        fact_all, u_all, blk_all = gather_results(facts, u_half, blocks)
        a_new_col, s_new_row = mirror_call(fact_all)
        u_all = u_all.reshape(2, 2, HIDDEN, BLOCK)
        u_col = u_all[:, 0]
        u_row = jnp.swapaxes(u_all[:, 1], 1, 2)
        return (u_col, u_row, a_new_col, blk_all[:2], blk_all[2:], s_new_row)

    batch_split = P('data', None)
    col_split = P(None, None, 'model')
    row_split = P(None, 'model', None)
    replicated = P()
    return jax.shard_map(
        shard_body,
        mesh=mesh,
        in_specs=(batch_split, batch_split, col_split, row_split, replicated, row_split, row_split, replicated, replicated, row_split, row_split, replicated),
        out_specs=(col_split, row_split, replicated, row_split, row_split, replicated),
        check_vma=False,
    )
```

```python
import functools
import math
import jax
import jax.numpy as jnp
from jax import lax
from jax.sharding import PartitionSpec as P
from jax.experimental import pallas as pl
from jax.experimental.pallas import tpu as pltpu

FACTOR_DECAY = 0.8
GELU_SCALE = math.sqrt(2.0 / math.pi)
GELU_CUBIC = 0.044715
EXACT = lax.Precision.HIGHEST
TN_DIMS = (((0,), (0,)), ((), ()))
NT_DIMS = (((1,), (1,)), ((), ()))
BOTH = ('model', 'data')


def gelu_value(pre_act):
    tanh_arg = GELU_SCALE * (pre_act + GELU_CUBIC * pre_act * pre_act * pre_act)
    return 0.5 * pre_act * (1.0 + jnp.tanh(tanh_arg))


def gelu_slope(pre_act):
    tanh_arg = GELU_SCALE * (pre_act + GELU_CUBIC * pre_act * pre_act * pre_act)
    tanh_val = jnp.tanh(tanh_arg)
    return 0.5 * (1.0 + tanh_val) + 0.5 * pre_act * (1.0 - tanh_val * tanh_val) * GELU_SCALE * (1.0 + 3.0 * GELU_CUBIC * pre_act * pre_act)


def activate(pre_act):
    return gelu_value(pre_act.astype(jnp.float32)).astype(jnp.bfloat16)


def back_gate(grad_act, pre_act):
    return (grad_act.astype(jnp.float32) * gelu_slope(pre_act.astype(jnp.float32))).astype(jnp.bfloat16)


def matmul(left_mat, right_mat):
    return jnp.dot(left_mat, right_mat, preferred_element_type=jnp.float32)


def matmul_tn(left_mat, right_mat):
    return lax.dot_general(left_mat, right_mat, TN_DIMS, preferred_element_type=jnp.float32)


def matmul_nt(left_mat, right_mat):
    return lax.dot_general(left_mat, right_mat, NT_DIMS, preferred_element_type=jnp.float32)


def exact_dot(left_mat, right_mat):
    return jnp.dot(left_mat, right_mat, precision=EXACT, preferred_element_type=jnp.float32)


MIB = 1024 * 1024
BLOCK = 256
HIDDEN = 1024
D_ROWS = 512
SYM_ROWS = 80
FULL_BASE = 512
BLOCK_BASE = 672
SHARE_ROWS = 800
LANES = 128
STRIP = 32
HALF_STRIP = 16
CORES = 8


def gram_kernel(x_ref, g1_ref, g2_ref, h1_ref, h2_ref, g3_ref, dy_ref, h3_ref, out_ref,
                act, stage, bstage, fstage, in_sem, out_sem, b_sem, f_sem):
    sources = [dy_ref, h3_ref, h2_ref, g3_ref, g2_ref, h1_ref, x_ref, g1_ref]
    slots = [3, 7, 2, 6, 1, 5, 0, 4]
    rows = pl.ds(lax.axis_index('model') * HIDDEN, HIDDEN)
    loads = [pltpu.make_async_copy(src.at[rows] if slot in (0, 3) else src, act.at[slot], in_sem.at[slot]) for src, slot in zip(sources, slots)]
    for load in loads:
        load.start()

    def out_copy(slot, dst):
        return pltpu.make_async_copy(stage.at[slot], dst, out_sem.at[slot])

    def f_copy(slot, n, which):
        return pltpu.make_async_copy(fstage.at[slot], out_ref.at[pl.ds(n * CORES, CORES), pl.ds(FULL_BASE + which * SYM_ROWS, SYM_ROWS)], f_sem.at[slot])

    for layer in (3, 2, 1, 0):
        pltpu.make_async_copy(g1_ref, act.at[layer], in_sem.at[layer]).wait()
        pltpu.make_async_copy(g1_ref, act.at[4 + layer], in_sem.at[4 + layer]).wait()

        def d_body(m, carry, layer=layer):
            slot = lax.rem(m, 2)
            cols = pl.ds(pl.multiple_of(m * BLOCK, BLOCK), BLOCK)
            right = act[4 + layer, :, cols]
            dst = out_ref.at[pl.ds(m * CORES + 2 * layer, 2), pl.ds(0, D_ROWS)]

            if layer == 3:
                @pl.when(m >= 2)
                def _():
                    out_copy(slot, dst).wait()
                    pltpu.make_async_copy(bstage.at[slot], out_ref.at[pl.ds(0, CORES), pl.ds(BLOCK_BASE, STRIP)], b_sem.at[slot]).wait()
            else:
                out_copy(slot, dst).wait()
                pltpu.make_async_copy(bstage.at[slot], out_ref.at[pl.ds(0, CORES), pl.ds(BLOCK_BASE, STRIP)], b_sem.at[slot]).wait()
            prod = lax.dot_general(act[layer], right, TN_DIMS, preferred_element_type=jnp.float32)
            stage[slot] = prod.reshape(2, D_ROWS, BLOCK)
            out_copy(slot, dst).start()
            blk = lax.dot_general(right, right, TN_DIMS, preferred_element_type=jnp.float32)
            bstage[slot] = blk.reshape(CORES, STRIP, BLOCK)
            pltpu.make_async_copy(bstage.at[slot], out_ref.at[pl.ds(m * CORES, CORES), pl.ds(BLOCK_BASE + STRIP * layer, STRIP)], b_sem.at[slot]).start()
            return carry

        lax.fori_loop(0, 4, d_body, 0)

        if layer in (2, 1):
            which = 0 if layer == 2 else 1

            def f_body(n, carry, layer=layer, which=which):
                slot = lax.rem(n, 2)
                if which == 0:
                    pl.when(n >= 2)(lambda: f_copy(slot, n, which).wait())
                else:
                    f_copy(slot, n, which).wait()
                put_sym(fstage.at[slot], sym_blocks(act.at[layer], n), False)
                f_copy(slot, n, which).start()
                return carry

            lax.fori_loop(0, 4, f_body, 0)
    for slot in range(2):
        f_copy(slot, 0, 0).wait()
        pltpu.make_async_copy(stage.at[slot], out_ref.at[pl.ds(0, 2), pl.ds(0, D_ROWS)], out_sem.at[slot]).wait()
        pltpu.make_async_copy(bstage.at[slot], out_ref.at[pl.ds(0, CORES), pl.ds(BLOCK_BASE, STRIP)], b_sem.at[slot]).wait()


def gram_call(x_tokens, g_one, g_two, h_one, h_two, g_three, dy_tokens, h_three):
    any_spec = pl.BlockSpec(memory_space=pl.ANY)
    return pl.pallas_call(
        gram_kernel,
        out_shape=jax.ShapeDtypeStruct((STRIP, SHARE_ROWS, BLOCK), jnp.float32),
        in_specs=[any_spec] * CORES,
        out_specs=any_spec,
        scratch_shapes=[
            pltpu.VMEM((CORES, HIDDEN, HIDDEN), jnp.bfloat16),
            pltpu.VMEM((2, 2, D_ROWS, BLOCK), jnp.float32),
            pltpu.VMEM((2, CORES, STRIP, BLOCK), jnp.float32),
            pltpu.VMEM((2, CORES, SYM_ROWS, BLOCK), jnp.float32),
            pltpu.SemaphoreType.DMA((CORES,)),
            pltpu.SemaphoreType.DMA((2,)),
            pltpu.SemaphoreType.DMA((2,)),
            pltpu.SemaphoreType.DMA((2,)),
        ],
        compiler_params=pltpu.CompilerParams(vmem_limit_bytes=48 * HIDDEN * HIDDEN),
        cost_estimate=pl.CostEstimate(flops=15_000_000_000, bytes_accessed=46_000_000, transcendentals=0),
        name='gram',
    )(x_tokens, g_one, g_two, h_one, h_two, g_three, dy_tokens, h_three)


MESH_ID = pl.DeviceIdType.MESH
PIECES = 5
FAR = 3
CHUNK_ORDER = tuple((zd, h) for pair in ((0, 3), (1, 2)) for h in range(PIECES) for zd in pair)


def torus_place():
    z = lax.axis_index('model')
    d = lax.axis_index('data')
    y = d // 4
    x = (d // 2) % 2
    c = d % 2
    near = {'x': (z, d + 2 - 4 * x), 'y': (z, d + 4 - CORES * y), 'c': (z, d + 1 - 2 * c), 'up': (z + 1, d), 'dn': (z - 1, d)}
    return z, y, x, c, near


def meet_neighbours(z, near):
    barrier = pltpu.get_barrier_semaphore()
    for side in ('x', 'y', 'c'):
        pl.semaphore_signal(barrier, inc=1, device_id=near[side], device_id_type=MESH_ID)

    @pl.when(z < 3)
    def _():
        pl.semaphore_signal(barrier, inc=1, device_id=near['up'], device_id_type=MESH_ID)

    @pl.when(z > 0)
    def _():
        pl.semaphore_signal(barrier, inc=1, device_id=near['dn'], device_id_type=MESH_ID)
    pl.semaphore_wait(barrier, 3 + (z + 3) // 4 + (6 - z) // 4)


def remote(src, dst, send_sem, recv_sem, where):
    return pltpu.make_async_remote_copy(src_ref=src, dst_ref=dst, send_sem=send_sem, recv_sem=recv_sem, device_id=where, device_id_type=MESH_ID)


def sym_blocks(left, n):
    def cols(at, size):
        return left[:, pl.ds(pl.multiple_of(at, LANES), size)]

    low = n % 2
    right = cols(n * BLOCK, BLOCK)
    pairs = ((right, right, STRIP), (cols((n + 1) % 4 * BLOCK, BLOCK), right, STRIP),
             (cols((low + 2) * BLOCK + n // 2 * LANES, LANES), cols(low * BLOCK, BLOCK), HALF_STRIP))
    return [lax.dot_general(a, b, TN_DIMS, preferred_element_type=jnp.float32).reshape(CORES, rows, BLOCK) for a, b, rows in pairs]


def put_sym(dst, blocks, more):
    at = 0
    for blk in blocks:
        span = pl.ds(at, blk.shape[1])
        dst[:, span] = dst[:, span] + blk if more else blk
        at += blk.shape[1]


def gather_kernel(plan, *refs):
    n = len(plan.items)
    pieces, refs = refs[:plan.n_in], refs[plan.n_in:]
    outs, refs = refs[:n], refs[n:]
    ends = len(plan.tokens) > 0
    if ends:
        ends_ref, refs = refs[0], refs[1:]
    lands, refs = refs[:n], refs[n:]
    if ends:
        tok, acc, tok_sem, acc_sem, *refs = refs
    load_sem, z_recv, x_recv, y_recv, d_recv, c_recv, up_send, dn_send, x_send, y_send, dy_send, dx_send, c_send, flush_sem = refs
    z, y, x, c, near = torus_place()

    def slot(ref, j, zs, yy, xx, cc):
        return plan.items[j].slot(ref, zs, 4 * yy + 2 * xx + cc)

    def view(j, zs, yy, xx, cc):
        return slot(lands[j], j, zs, yy, xx, cc)

    def half(j, zs, yy, xx, cc, which):
        return plan.items[j].half(lands[j], zs, 4 * yy + 2 * xx + cc, which)

    def flush(j, zs, yy, xx, cc, index):
        return pltpu.make_async_copy(view(j, zs, yy, xx, cc), slot(outs[j], j, zs, yy, xx, cc), flush_sem.at[j, zs, index])

    loads = [pltpu.make_async_copy(item.piece(pieces, z, 4 * y + 2 * x + c), view(j, z, y, x, c), load_sem.at[j]) for j, item in enumerate(plan.items)]
    for load in loads:
        load.start()

    def tok_load(t):
        src = pieces[plan.tokens[t // 4]].at[pl.ds(t % 4 * HIDDEN, HIDDEN)]
        return pltpu.make_async_copy(src, tok.at[t % 2], tok_sem.at[t % 2])

    def ends_out(mat):
        return pltpu.make_async_copy(acc.at[mat], ends_ref.at[mat], acc_sem.at[mat])

    def ends_step(t):
        tok_load(t).wait()
        put_sym(acc.at[t // 4], sym_blocks(tok.at[t % 2], z), t % 4 > 0)
        if t + 2 < CORES:
            tok_load(t + 2).start()
        if t % 4 == 3:
            ends_out(t // 4).start()

    todo = list(range(CORES)) if ends else []
    if ends:
        tok_load(0).start()
        tok_load(1).start()
    meet_neighbours(z, near)

    def side_copy(j, zs, side):
        send, recv = {'x': (x_send, x_recv), 'y': (y_send, y_recv), 'up': (up_send, z_recv), 'dn': (dn_send, z_recv)}[side]
        return remote(view(j, zs, y, x, c), view(j, zs, y, x, c), send.at[j, zs], recv.at[j, zs], near[side])

    def from_side(j, zs, side):
        yy, xx = (y, 1 - x) if side == 'x' else (1 - y, x)
        send, recv = {'x': (x_send, x_recv), 'y': (y_send, y_recv)}[side]
        return remote(view(j, zs, yy, xx, c), view(j, zs, yy, xx, c), send.at[j, zs], recv.at[j, zs], near[side])

    def dy_copy(j, zs):
        return remote(half(j, zs, y, 1 - x, c, 0), half(j, zs, y, 1 - x, c, 0), dy_send.at[j, zs], d_recv.at[j, zs, 0], near['y'])

    def dx_copy(j, zs):
        return remote(half(j, zs, 1 - y, x, c, 1), half(j, zs, 1 - y, x, c, 1), dx_send.at[j, zs], d_recv.at[j, zs, 1], near['x'])

    def kind_place(kind):
        return (y if kind < 2 else 1 - y), (x if kind % 2 == 0 else 1 - x)

    def c_copy(j, zs, kind):
        yy, xx = kind_place(kind)
        return remote(view(j, zs, yy, xx, c), view(j, zs, yy, xx, c), c_send.at[j, zs, kind], c_recv.at[j, zs, kind], near['c'])

    def share_core(j, zs, kind):
        yy, xx = kind_place(kind)
        c_copy(j, zs, kind).start()
        flush(j, zs, yy, xx, c, kind).start()

    def guard(off, body):
        if off == 0:
            body(z)
        elif off < 0:
            pl.when(z >= -off)(lambda: body(z + off))
        else:
            pl.when(z <= 3 - off)(lambda: body(z + off))

    def z_step(j, off):
        def body(zs):
            if off == 0:
                loads[j].wait()
            else:
                side_copy(j, zs, 'up').wait_recv()
            if off <= 0 and not plan.items[j].plane:
                pl.when(z < 3)(lambda: side_copy(j, zs, 'up').start())
            if off >= 0 and not plan.items[j].plane:
                pl.when(z > 0)(lambda: side_copy(j, zs, 'dn').start())
            side_copy(j, zs, 'x').start()
            side_copy(j, zs, 'y').start()
            share_core(j, zs, 0)
        guard(off, body)

    def xy_step(j, off):
        def body(zs):
            from_side(j, zs, 'x').wait_recv()
            dy_copy(j, zs).start()
            share_core(j, zs, 1)
            from_side(j, zs, 'y').wait_recv()
            dx_copy(j, zs).start()
            share_core(j, zs, 2)
        guard(off, body)

    def diag_step(j, off):
        def body(zs):
            for which in range(2):
                remote(half(j, zs, 1 - y, 1 - x, c, which), half(j, zs, 1 - y, 1 - x, c, which), dy_send.at[j, zs], d_recv.at[j, zs, which], near['y']).wait_recv()
            share_core(j, zs, 3)
        guard(off, body)

    def core_step(j, off):
        def body(zs):
            for kind in range(4):
                yy, xx = kind_place(kind)
                remote(view(j, zs, yy, xx, 1 - c), view(j, zs, yy, xx, 1 - c), c_send.at[j, zs, kind], c_recv.at[j, zs, kind], near['c']).wait_recv()
                flush(j, zs, yy, xx, 1 - c, 4 + kind).start()
        guard(off, body)

    def last_step(j, off):
        def body(zs):
            for kind in range(4):
                yy, xx = kind_place(kind)
                c_copy(j, zs, kind).wait_send()
                flush(j, zs, yy, xx, c, kind).wait()
                flush(j, zs, yy, xx, 1 - c, 4 + kind).wait()
            side_copy(j, zs, 'x').wait_send()
            side_copy(j, zs, 'y').wait_send()
            dy_copy(j, zs).wait_send()
            dx_copy(j, zs).wait_send()
            if off <= 0 and not plan.items[j].plane:
                pl.when(z < 3)(lambda: side_copy(j, zs, 'up').wait_send())
            if off >= 0 and not plan.items[j].plane:
                pl.when(z > 0)(lambda: side_copy(j, zs, 'dn').wait_send())
        guard(off, body)

    waves = [[(j, 0) for j in plan.order]]
    for far in range(1, 4):
        waves.append([(j, sign * far) for j in plan.order if not plan.items[j].plane for sign in (-1, 1)])
    for step in range(7):
        for func, lag in ((z_step, 0), (xy_step, 1), (diag_step, 2), (core_step, 3)):
            if 0 <= step - lag < 4:
                for j, off in waves[step - lag]:
                    func(j, off)
                if todo and step >= 3 and lag:
                    ends_step(todo.pop(0))
    for t in todo:
        ends_step(t)
    if ends:
        ends_out(0).wait()
        ends_out(1).wait()
    for wave in waves:
        for j, off in wave:
            last_step(j, off)


class Item:
    def __init__(self, shape, dtype, piece, slot, half, plane=False):
        self.shape, self.dtype, self.piece, self.slot, self.half, self.plane = shape, dtype, piece, slot, half, plane


class Plan:
    def __init__(self, n_in, items, order, tokens):
        self.n_in, self.items, self.order, self.tokens = n_in, items, order, tokens


def gather_call(args, items, order, collective_id, name, tokens=()):
    n = len(items)
    dma = pltpu.SemaphoreType.DMA
    size = sum(math.prod(item.shape) * jnp.dtype(item.dtype).itemsize for item in items)
    hbm = pl.BlockSpec(memory_space=pltpu.HBM)
    flat = dma((n, 4))
    shapes = [jax.ShapeDtypeStruct(item.shape, item.dtype) for item in items]
    extra = []
    if tokens:
        part = (2, CORES, SYM_ROWS, BLOCK)
        shapes.append(jax.ShapeDtypeStruct(part, jnp.float32))
        extra = [pltpu.VMEM((2, HIDDEN, HIDDEN), jnp.bfloat16), pltpu.VMEM(part, jnp.float32), dma((2,)), dma((2,))]
    return pl.pallas_call(
        functools.partial(gather_kernel, Plan(len(args), items, order, tokens)),
        out_shape=shapes,
        in_specs=[hbm] * len(args),
        out_specs=[hbm] * len(shapes),
        scratch_shapes=[pltpu.VMEM(item.shape, item.dtype) for item in items] + extra
        + [dma((n,)), flat, flat, flat, dma((n, 4, 2)), dma((n, 4, 4)), flat, flat, flat, flat, flat, flat, dma((n, 4, 4)), dma((n, 4, CORES))],
        compiler_params=pltpu.CompilerParams(collective_id=collective_id, has_side_effects=True, vmem_limit_bytes=60 * MIB if tokens else size + CORES * MIB),
        cost_estimate=pl.CostEstimate(flops=50_000_000_000, bytes_accessed=size, transcendentals=0),
        name=name,
    )(*args)


def col_slot(ref, zs, d):
    return ref.at[pl.ds(d * LANES, LANES), pl.ds(zs * BLOCK, BLOCK)]


def col_half(ref, zs, d, which):
    return ref.at[pl.ds(d * LANES + which * 64, 64), pl.ds(zs * BLOCK, BLOCK)]


def row_slot(ref, zs, d):
    return ref.at[pl.ds((zs * CORES + d) * STRIP, STRIP)]


def row_half(ref, zs, d, which):
    return ref.at[pl.ds((zs * CORES + d) * STRIP + which * HALF_STRIP, HALF_STRIP)]


def gather_weights(w_col, w_row, x_tokens, dy_tokens):
    shape = (HIDDEN, HIDDEN)
    items = [Item(shape, w_col.dtype, lambda refs, z, d, i=i: refs[0].at[i, pl.ds(d * LANES, LANES)], col_slot, col_half) for i in range(2)]
    items += [Item(shape, w_row.dtype, lambda refs, z, d, i=i: refs[1].at[i, pl.ds(d * STRIP, STRIP)], row_slot, row_half) for i in range(2)]
    return gather_call((w_col, w_row, x_tokens, dy_tokens), items, (0, 3, 2, 1), 1, 'weights', (2, 3))


def gather_results(facts, u_half, blocks):
    items = [
        Item((STRIP, 4, SYM_ROWS, BLOCK), facts.dtype, lambda refs, z, d: refs[0],
             lambda ref, zs, d: ref.at[zs * CORES + d], lambda ref, zs, d, which: ref.at[zs * CORES + d, pl.ds(2 * which, 2)]),
        Item((CORES, D_ROWS, BLOCK), facts.dtype, lambda refs, z, d: refs[1],
             lambda ref, zs, d: ref.at[d], lambda ref, zs, d, which: ref.at[d, pl.ds(which * BLOCK, BLOCK)], True),
        Item((4, BLOCK, BLOCK), facts.dtype, lambda refs, z, d: refs[2],
             lambda ref, zs, d: ref.at[:, pl.ds(d * STRIP, STRIP)], lambda ref, zs, d, which: ref.at[pl.ds(2 * which, 2), pl.ds(d * STRIP, STRIP)], True),
    ]
    return gather_call((facts, u_half, blocks), items, (1, 2, 0), 3, 'results')


def add_into(dst, src, rows):
    step = max(n for n in range(CORES, 65, CORES) if rows % n == 0)

    def body(i, carry):
        span = pl.ds(pl.multiple_of(i * step, CORES), step)
        dst[span, :] = dst[span, :] + src[span, :]
        return carry

    lax.fori_loop(0, rows // step, body, 0)


def scatter_kernel(rows, parts_ref, ends_ref, share_ref, eshare_ref, grad_ref, own, mate, one_x, one_y, two_x, two_y, up_buf, dn_buf,
                   eown, emate, eone, etwo, gland, e_sem, emate_sem, eone_sem, etwo_sem, g_sem, out2_sem,
                   own_sem, mate_send, mate_recv, x1_send, x1_recv, y1_send, y1_recv, x2_send, x2_recv, y2_send, y2_recv,
                   up_send, up_recv, dn_send, dn_recv, out_sem):
    z, y, x, c, near = torus_place()
    sub = rows // (2 * PIECES)
    eload = pltpu.make_async_copy(ends_ref.at[:, :, :, c], eown, e_sem.at[0])
    eload.start()
    loads = {}
    for k, (zd, h) in enumerate(CHUNK_ORDER):
        loads[k] = []
        for col in range(2):
            span = pl.ds(col * PIECES * sub + h * sub, sub)
            load = pltpu.make_async_copy(parts_ref.at[zd, :, :, c, span], own.at[zd, :, :, span], own_sem.at[k, col])
            load.start()
            loads[k].append(load)
    meet_neighbours(z, near)
    ematec = remote(ends_ref.at[:, :, :, 1 - c], emate, emate_sem.at[0], emate_sem.at[1], near['c'])
    ematec.start()
    eones = (remote(eown.at[0, :, 1 - x], eone.at[0], eone_sem.at[0], eone_sem.at[1], near['x']),
             remote(eown.at[1, 1 - y], eone.at[1], eone_sem.at[2], eone_sem.at[3], near['y']))
    etwos = (remote(eown.at[0, 1 - y, x], etwo.at[0], etwo_sem.at[0], etwo_sem.at[1], near['y']),
             remote(eown.at[1, y, 1 - x], etwo.at[1], etwo_sem.at[2], etwo_sem.at[3], near['x']))
    mates = {}
    for k, (zd, h) in enumerate(CHUNK_ORDER):
        mates[k] = []
        for col in range(2):
            span = pl.ds(col * PIECES * sub + h * sub, sub)
            copy = remote(parts_ref.at[zd, :, :, 1 - c, span], mate.at[zd, :, :, span], mate_send.at[k, col], mate_recv.at[k, col], near['c'])
            copy.start()
            mates[k].append(copy)

    def spans(h):
        return pl.ds(h * sub, sub), pl.ds(PIECES * sub + h * sub, sub)

    def one_copies(k):
        zd, h = CHUNK_ORDER[k]
        first, second = spans(h)
        piece = pl.ds(h * sub, sub)
        return (remote(own.at[zd, :, 1 - x, first], one_x.at[zd, :, piece], x1_send.at[k], x1_recv.at[k], near['x']),
                remote(own.at[zd, 1 - y, :, second], one_y.at[zd, :, piece], y1_send.at[k], y1_recv.at[k], near['y']))

    def two_copies(k):
        zd, h = CHUNK_ORDER[k]
        first, second = spans(h)
        piece = pl.ds(h * sub, sub)
        return (remote(own.at[zd, 1 - y, x, first], two_y.at[zd, piece], y2_send.at[k], y2_recv.at[k], near['y']),
                remote(own.at[zd, y, 1 - x, second], two_x.at[zd, piece], x2_send.at[k], x2_recv.at[k], near['x']))

    def z_copies(k):
        zd, h = CHUNK_ORDER[k]
        out = []
        for col, span in enumerate(spans(h)):
            out.append((remote(own.at[zd, y, x, span], up_buf.at[zd, span], dn_send.at[k, col], up_recv.at[k, col], near['dn']),
                        remote(own.at[zd, y, x, span], dn_buf.at[zd, span], up_send.at[k, col], dn_recv.at[k, col], near['up'])))
        return out

    def step_a(k):
        zd, h = CHUNK_ORDER[k]
        first, second = spans(h)
        ones = one_copies(k)
        loads[k][0].wait()
        mates[k][0].wait_recv()
        for yy in range(2):
            add_into(own.at[zd, yy, 1 - x, first], mate.at[zd, yy, 1 - x, first], sub)
        ones[0].start()
        loads[k][1].wait()
        mates[k][1].wait_recv()
        for xx in range(2):
            add_into(own.at[zd, 1 - y, xx, second], mate.at[zd, 1 - y, xx, second], sub)
        ones[1].start()
        for yy in range(2):
            add_into(own.at[zd, yy, x, first], mate.at[zd, yy, x, first], sub)
        for xx in range(2):
            add_into(own.at[zd, y, xx, second], mate.at[zd, y, xx, second], sub)

    def step_b(k):
        zd, h = CHUNK_ORDER[k]
        first, second = spans(h)
        piece = pl.ds(h * sub, sub)
        ones, twos = one_copies(k), two_copies(k)
        ones[0].wait_recv()
        add_into(own.at[zd, 1 - y, x, first], one_x.at[zd, 1 - y, piece], sub)
        twos[0].start()
        ones[1].wait_recv()
        add_into(own.at[zd, y, 1 - x, second], one_y.at[zd, 1 - x, piece], sub)
        twos[1].start()
        add_into(own.at[zd, y, x, first], one_x.at[zd, y, piece], sub)
        add_into(own.at[zd, y, x, second], one_y.at[zd, x, piece], sub)

    def step_c(k):
        zd, h = CHUNK_ORDER[k]
        first, second = spans(h)
        piece = pl.ds(h * sub, sub)
        twos = two_copies(k)
        for copy, buf, span in ((twos[0], two_y, first), (twos[1], two_x, second)):
            copy.wait_recv()
            add_into(own.at[zd, y, x, span], buf.at[zd, piece], sub)

    def z_add(k, side, buf):
        zd, h = CHUNK_ORDER[k]
        for col, span in enumerate(spans(h)):
            z_copies(k)[col][side].wait_recv()
            add_into(own.at[zd, y, x, span], buf.at[zd, span], sub)

    def z_hop(k, hop):
        zd, h = CHUNK_ORDER[k]
        for place, side, far in ((3 - hop, 0, hop), (hop, 1, hop)):
            if (place > zd, place < zd)[side]:
                @pl.when(z == place)
                def _(side=side, far=far):
                    if far:
                        z_add(k, side, (up_buf, dn_buf)[side])
                    for pair in z_copies(k):
                        pair[side].start()
        if hop == 3:
            @pl.when(z == zd)
            def _():
                if zd < 3:
                    z_add(k, 0, up_buf)
                if zd:
                    z_add(k, 1, dn_buf)
                for col, span in enumerate(spans(h)):
                    pltpu.make_async_copy(own.at[zd, y, x, span], share_ref.at[span], out_sem.at[h, col]).start()

    def ends_a():
        eload.wait()
        ematec.wait_recv()
        for mat in range(2):
            for yy in range(2):
                for xx in range(2):
                    add_into(eown.at[mat, yy, xx], emate.at[mat, yy, xx], SYM_ROWS)
            eones[mat].start()

    def ends_b():
        eones[0].wait_recv()
        for yy in range(2):
            add_into(eown.at[0, yy, x], eone.at[0, yy], SYM_ROWS)
        etwos[0].start()
        eones[1].wait_recv()
        for xx in range(2):
            add_into(eown.at[1, y, xx], eone.at[1, xx], SYM_ROWS)
        etwos[1].start()

    def ends_c():
        for mat in range(2):
            etwos[mat].wait_recv()
            add_into(eown.at[mat, y, x], etwo.at[mat], SYM_ROWS)
            pltpu.make_async_copy(eown.at[mat, y, x], eshare_ref.at[mat], out2_sem.at[mat]).start()

    n = len(CHUNK_ORDER)
    ends_a()
    for step in range(n + 2 * FAR + 4):
        for func, lag in ((step_a, 0), (step_b, FAR), (step_c, 2 * FAR)):
            if 0 <= step - lag < n:
                func(step - lag)
        for hop in range(4):
            if 0 <= step - 2 * FAR - hop < n:
                z_hop(step - 2 * FAR - hop, hop)
        if step == 2:
            ends_b()
        if step == 4:
            ends_c()
    mine = own.at[z, y, x, pl.ds(0, D_ROWS)]
    gcopy = remote(mine, gland, g_sem.at[0], g_sem.at[1], near['c'])
    gcopy.start()
    gout = pltpu.make_async_copy(mine, grad_ref.at[c], out2_sem.at[2])
    gout.start()
    gcopy.wait_recv()
    gmate = pltpu.make_async_copy(gland, grad_ref.at[1 - c], out2_sem.at[3])
    gmate.start()
    for copy in (ematec, gcopy) + eones + etwos:
        copy.wait_send()
    for k, (zd, h) in enumerate(CHUNK_ORDER):
        for copy in mates[k] + list(one_copies(k)) + list(two_copies(k)):
            copy.wait_send()
        for col, (down, up) in enumerate(z_copies(k)):
            pl.when(z > zd)(lambda: down.wait_send())
            pl.when(z < zd)(lambda: up.wait_send())
    for h in range(PIECES):
        for col in range(2):
            span = spans(h)[col]
            pltpu.make_async_copy(own.at[0, y, x, span], share_ref.at[span], out_sem.at[h, col]).wait()
    for mat in range(2):
        pltpu.make_async_copy(eown.at[mat, y, x], eshare_ref.at[mat], out2_sem.at[mat]).wait()
    gout.wait()
    gmate.wait()


def scatter_call(parts, ends, collective_id, name):
    rows = parts.shape[-2]
    half = rows // 2
    f32 = jnp.float32
    dma = pltpu.SemaphoreType.DMA
    n = len(CHUNK_ORDER)
    whole = pltpu.VMEM((4, 2, 2, rows, BLOCK), f32)
    one_buf = pltpu.VMEM((4, 2, half, BLOCK), f32)
    two_buf = pltpu.VMEM((4, half, BLOCK), f32)
    z_buf = pltpu.VMEM((4, rows, BLOCK), f32)
    e_buf = pltpu.VMEM((2, 2, 2, SYM_ROWS, BLOCK), f32)
    hbm = pl.BlockSpec(memory_space=pltpu.HBM)
    return pl.pallas_call(
        functools.partial(scatter_kernel, rows),
        out_shape=[jax.ShapeDtypeStruct((rows, BLOCK), f32), jax.ShapeDtypeStruct((2, SYM_ROWS, BLOCK), f32), jax.ShapeDtypeStruct((2, D_ROWS, BLOCK), f32)],
        in_specs=[hbm] * 2,
        out_specs=[hbm] * 3,
        scratch_shapes=[whole, whole, one_buf, one_buf, two_buf, two_buf, z_buf, z_buf,
                        e_buf, e_buf, pltpu.VMEM((2, 2, SYM_ROWS, BLOCK), f32), pltpu.VMEM((2, SYM_ROWS, BLOCK), f32), pltpu.VMEM((D_ROWS, BLOCK), f32),
                        dma((1,)), dma((2,)), dma((4,)), dma((4,)), dma((2,)), dma((4,))]
        + [dma((n, 2))] * 3 + [dma((n,))] * CORES + [dma((n, 2))] * 4 + [dma((PIECES, 2))],
        compiler_params=pltpu.CompilerParams(collective_id=collective_id, has_side_effects=True, vmem_limit_bytes=60 * MIB),
        cost_estimate=pl.CostEstimate(flops=120_000_000_000, bytes_accessed=60 * MIB, transcendentals=0),
        name=name,
    )(parts.reshape(4, 2, 2, 2, rows, BLOCK), ends.reshape(2, 2, 2, 2, SYM_ROWS, BLOCK))


def mirror_kernel(in_ref, a_ref, s_ref):
    def block(i, j, mat):
        def take(plane, at, size):
            return in_ref[plane, :, mat, pl.ds(at, size)].reshape(CORES * size, BLOCK)

        if i == j:
            return take(j, 0, STRIP)
        if i == (j + 1) % 4:
            return take(j, STRIP, STRIP)
        if j == (i + 1) % 4:
            return take(i, STRIP, STRIP).T
        low = min(i, j)
        both = jnp.concatenate([take(low, 64, HALF_STRIP), take(low + 2, 64, HALF_STRIP)], axis=0)
        return both if i > j else both.T

    for i in range(4):
        @pl.when(pl.program_id(1) == i)
        def _(i=i):
            for mat, out in enumerate((a_ref, s_ref)):
                for j in range(4):
                    out[0, :, pl.ds(j * BLOCK, BLOCK)] = block(i, j, mat)


def mirror_call(facts):
    full = jax.ShapeDtypeStruct((2, HIDDEN, HIDDEN), facts.dtype)
    out_spec = pl.BlockSpec((1, BLOCK, HIDDEN), lambda k, i: (k, i, 0))
    return pl.pallas_call(
        mirror_kernel,
        grid=(2, 4),
        out_shape=[full, full],
        in_specs=[pl.BlockSpec((4, CORES, 2, SYM_ROWS, BLOCK), lambda k, i: (0, 0, k, 0, 0))],
        out_specs=[out_spec, out_spec],
        compiler_params=pltpu.CompilerParams(vmem_limit_bytes=STRIP * MIB),
        cost_estimate=pl.CostEstimate(flops=10_000_000_000, bytes_accessed=26 * MIB, transcendentals=0),
        name='mirror',
    )(facts.reshape(4, CORES, 4, SYM_ROWS, BLOCK))


def solution(mesh):
    data_ways = mesh.shape['data']
    model_ways = mesh.shape['model']

    def shard_body(x_tokens, dy_tokens, w_col, w_row, a_old_col, s_old_col, a_old_row, s_old_row, a_inv_col, s_inv_col, a_inv_row, s_inv_row):
        model_id = lax.axis_index('model')
        data_id = lax.axis_index('data')
        inv_rows = 1.0 / (x_tokens.shape[0] * data_ways)
        w_one, w_three, w_two, w_four, ends = gather_weights(w_col, w_row, x_tokens, dy_tokens)
        rows_dev = x_tokens.shape[0] // model_ways
        x_loc = lax.dynamic_slice(x_tokens, (rows_dev * model_id, 0), (rows_dev, HIDDEN))
        dy_loc = lax.dynamic_slice(dy_tokens, (rows_dev * model_id, 0), (rows_dev, HIDDEN))
        z_one = matmul(x_loc, w_one).astype(jnp.bfloat16)
        h_one = activate(z_one)
        z_two = matmul(h_one, w_two).astype(jnp.bfloat16)
        h_two = activate(z_two)
        z_three = matmul(h_two, w_three).astype(jnp.bfloat16)
        h_three = activate(z_three)
        g_three = back_gate(matmul_nt(dy_loc, w_four).astype(jnp.bfloat16), z_three)
        g_two = back_gate(matmul_nt(g_three, w_three).astype(jnp.bfloat16), z_two)
        g_one = back_gate(matmul_nt(g_two, w_two).astype(jnp.bfloat16), z_one)
        parts = gram_call(x_tokens, g_one, g_two, h_one, h_two, g_three, dy_tokens, h_three)
        share, eshare, grad_mat = scatter_call(parts, ends, 2, 'sums')
        keep = 1.0 - FACTOR_DECAY
        low = lax.rem(model_id, 2)
        spots = ((model_id * BLOCK + STRIP * data_id, model_id * BLOCK, STRIP),
                 (lax.rem(model_id + 1, 4) * BLOCK + STRIP * data_id, model_id * BLOCK, STRIP),
                 ((low + 2) * BLOCK + model_id // 2 * LANES + HALF_STRIP * data_id, low * BLOCK, HALF_STRIP))
        olds = [jnp.concatenate([lax.dynamic_slice(old, (0, at, col), (2, size, BLOCK)) for at, col, size in spots], axis=1) for old in (a_old_col, s_old_row)]
        mids = share[FULL_BASE:BLOCK_BASE].reshape(2, SYM_ROWS, BLOCK)
        sums = jnp.stack([eshare[0], mids[1], mids[0], eshare[1]])
        facts = FACTOR_DECAY * jnp.stack(olds, axis=1).reshape(4, SYM_ROWS, BLOCK) + keep * inv_rows * sums
        grad_mat = grad_mat.reshape(HIDDEN, BLOCK) * inv_rows
        layer_id = data_id // 2
        stack_id = layer_id // 2
        is_col = lax.rem(layer_id, 2) == 0
        half_at = lax.rem(data_id, 2) * D_ROWS
        full_inv = jnp.where(is_col, *[lax.dynamic_slice(inv, (stack_id, half_at, 0), (1, D_ROWS, HIDDEN))[0] for inv in (a_inv_col, s_inv_row)])
        block_inv = jnp.where(is_col, *[lax.dynamic_slice(inv, (stack_id, 0, 0), (1, BLOCK, BLOCK))[0] for inv in (s_inv_col, a_inv_row)])
        u_half = exact_dot(exact_dot(full_inv, grad_mat), block_inv)
        old_blocks = jnp.concatenate([lax.dynamic_slice(old, (0, STRIP * data_id, 0), (2, STRIP, BLOCK)) for old in (s_old_col, a_old_row)])
        new_blocks = jnp.swapaxes(share[BLOCK_BASE:].reshape(2, 2, STRIP, BLOCK), 0, 1).reshape(4, STRIP, BLOCK)
        blocks = FACTOR_DECAY * old_blocks + keep * inv_rows * new_blocks
        fact_all, u_all, blk_all = gather_results(facts, u_half, blocks)
        a_new_col, s_new_row = mirror_call(fact_all)
        u_all = u_all.reshape(2, 2, HIDDEN, BLOCK)
        u_col = u_all[:, 0]
        u_row = jnp.swapaxes(u_all[:, 1], 1, 2)
        return (u_col, u_row, a_new_col, blk_all[:2], blk_all[2:], s_new_row)

    batch_split = P('data', None)
    col_split = P(None, None, 'model')
    row_split = P(None, 'model', None)
    replicated = P()
    return jax.shard_map(
        shard_body,
        mesh=mesh,
        in_specs=(batch_split, batch_split, col_split, row_split, replicated, row_split, row_split, replicated, replicated, row_split, row_split, replicated),
        out_specs=(col_split, row_split, replicated, row_split, row_split, replicated),
        check_vma=False,
    )
```
